32 devices in a mesh: dp: 16 (over z, x, core), tensor: 2 (over y).
Axes of the slice: x: 2, y: 2, z: 4, core: 2. Of those that a mesh axis runs over, the one named last changes fastest.
Arguments:
- tokens: bfloat16 [63040, 384], P(('dp', 'tensor')), may hold values from -6 to 6
- query_key_value: bfloat16 [384, 3, 384], P('dp', None, 'tensor'), may hold values from -0.3125 to 0.3125
- attention_out: bfloat16 [384, 384], P('tensor', 'dp'), may hold values from -1.25 to 1.25
- first_gain: bfloat16 [384], P('dp'), may hold values from 0.099609375 to 1.8984375
- first_shift: bfloat16 [384], P('dp'), may hold values from -3 to 3
- second_gain: bfloat16 [384], P('dp'), may hold values from 0.099609375 to 1.8984375
- second_shift: bfloat16 [384], P('dp'), may hold values from -3 to 3
- expert_in: bfloat16 [8, 384, 1536], P(None, None, ('dp', 'tensor')), may hold values from -0.3125 to 0.3125
- expert_out: bfloat16 [8, 1536, 384], P(None, ('dp', 'tensor')), may hold values from -0.15625 to 0.15625
- expert_ids: int32 [63040, 2], P('dp'), may hold values from 0 to 7, all different within a row; in each aligned block of 3940 rows (0 to 3939, 3940 to 7879, ...) at most 1232 rows name the same one
- gate_weights: float32 [63040, 2], P('dp'), may hold values from 0.1 to 0.9
- cotangent: bfloat16 [63040, 384], P(('dp', 'tensor')), may hold values from -6 to 6
Outputs:
- output: bfloat16 [63040, 384], P(('dp', 'tensor'))
- grad_tokens: float32 [63040, 384], P(('dp', 'tensor'))
- grad_query_key_value: float32 [384, 3, 384], P('dp', None, 'tensor')
- grad_attention_out: float32 [384, 384], P('tensor', 'dp')
- grad_first_gain: float32 [384], P('dp')
- grad_first_shift: float32 [384], P('dp')
- grad_second_gain: float32 [384], P('dp')
- grad_second_shift: float32 [384], P('dp')
- grad_expert_in: float32 [8, 384, 1536], P(None, None, ('dp', 'tensor'))
- grad_expert_out: float32 [8, 1536, 384], P(None, ('dp', 'tensor'))
The draws below stay inside these ranges and needn't reach their ends.
Inputs may be any that keep to these rules, and one draw needn't show every extreme that they name: `expert_ids`: each row names 2 different experts; within the rows of one index of dp (aligned blocks of 3940 rows) no expert is named by more than 1232 rows, and in some such block one is named by exactly 1232.
All inputs are finite; a program needn't handle non-finite values.
Results may differ from the reference program's by a relative error of at most 0.015.
Values may be sent and summed in bfloat16 or wider, within the bound.
A program may use at most 192 MiB of HBM per device.

```python
import math
import jax
import jax.numpy as jnp
import numpy as np
from jax import lax

D = 384
HEADS = 6
HEAD_DIM = 64
FF = 1536
EXPERTS = 8
TOP = 2
SEQ = 197
IMGS = 20
GROUP_ROWS = 3940
TOKENS = 63040
CAP = 1232
N_DP = 16


def steps_of(stream_key, extent, split, smallest, top_value):
    def one(dim, blocks):
        heights = jax.random.uniform(jax.random.fold_in(jax.random.fold_in(stream_key, 6), dim), (blocks,), jnp.float32, smallest / len(split), top_value / len(split))
        return jnp.repeat(jnp.exp(heights), extent[dim] // blocks).reshape((-1,) + (1,) * (len(extent) - dim - 1))

    level = one(*split[0])
    for cut in split[1:]:
        level = level * one(*cut)
    return level


def assign_block(rng, own, number, rows, number_of, top, limit, slope):
    ranking = jax.random.permutation(rng, number_of)
    heavy_load, common = shares(number_of, rows * top, limit, slope, True), shares(number_of, rows * top, limit, slope, False)
    places = jnp.arange(number_of)

    def named(sizes, turn):
        used = int((sizes > 0).sum())
        fixed = max(1, used // 4)
        shifted = fixed + (places - fixed + turn * (used - fixed)) % max(1, number_of - fixed)
        return jnp.zeros((number_of,), jnp.int32).at[ranking[jnp.where(places < fixed, places, shifted)]].set(jnp.asarray(sizes, jnp.int32))

    sizes = jnp.where(number % 4 == 0, named(heavy_load, number // 4), named(common, number - number // 4 - 1))
    mixed = jax.random.permutation(jax.random.fold_in(own, 3), number_of)
    giver, taker = mixed[0:number_of // 2 * 2:2], mixed[1:number_of // 2 * 2:2]
    margin = jnp.minimum(sizes[giver] - 1, limit - sizes[taker]) // 2
    margin = jnp.where((giver == ranking[0]) | (taker == ranking[0]) | (sizes[taker] == 0), 0, jnp.maximum(margin, 0))
    shifted = jax.random.randint(jax.random.fold_in(own, 4), (number_of // 2,), 0, 1 << 20) % (margin + 1)
    sizes = sizes.at[giver].add(-shifted).at[taker].add(shifted)
    labels = jnp.searchsorted(jnp.cumsum(sizes), jnp.arange(rows * top), side="right").astype(jnp.int32)
    listing = labels.reshape(top, rows).T
    listing = listing[jax.random.permutation(jax.random.fold_in(own, 1), rows)]
    turn = jax.random.randint(jax.random.fold_in(own, 2), (rows, 1), 0, top)
    return jnp.take_along_axis(listing, (jnp.arange(top)[None, :] + turn) % top, axis=1)


def shares(number_of, total, most, skew, full):
    portions = [(1 << 20) // math.isqrt(grade ** skew) + 1 for grade in range(1, number_of + 1)]
    largest = most if full else min(most, max(-(-total // number_of), total * portions[0] // sum(portions)))
    least = 1 if total - largest >= number_of - 1 else 0
    holding, spare = [largest] + [least] * (number_of - 1), total - largest - least * (number_of - 1)
    while spare > 0:
        free = [i for i in range(1, number_of) if holding[i] < largest] or [i for i in range(1, number_of) if holding[i] < most]
        whole, left = sum([portions[i] for i in free]), spare
        for i in free:
            extra = min(most - holding[i], max(1, left * portions[i] // whole), spare)
            holding[i] = holding[i] + extra
            spare = spare - extra
    return np.array(holding)


def bell_draw(key, dims, width, bound, cuts=(), kind=jnp.bfloat16):
    level = steps_of(key, dims, cuts, -0.22, 0.18) if cuts else 1.0
    drawn = jax.random.normal(key, dims, jnp.float32) * width * level
    return jnp.minimum(jnp.maximum(drawn, -bound), bound).astype(kind)


def setup_inputs(seed: int = 0) -> dict:
    arg_keys = jax.random.split(jax.random.key(seed), 13)
    tokens = bell_draw(arg_keys[0], (TOKENS, D), 1.0, 6.0, ((0, 32),))
    query_key_value = bell_draw(arg_keys[1], (D, 3, D), D ** -0.5, 0.3125, ((0, 16), (2, 2)))
    attention_out = bell_draw(arg_keys[2], (D, D), (D // 16) ** -0.5, 1.25, ((0, 2), (1, 16)))
    first_gain = jnp.clip(1.0 + 0.18 * jax.random.normal(arg_keys[3], (D,), jnp.float32), 0.099609375, 1.8984375).astype(jnp.bfloat16)
    first_shift = bell_draw(arg_keys[4], (D,), 0.5, 3.0, ((0, 16),))
    second_gain = jnp.clip(1.0 + 0.18 * jax.random.normal(arg_keys[5], (D,), jnp.float32), 0.099609375, 1.8984375).astype(jnp.bfloat16)
    second_shift = bell_draw(arg_keys[6], (D,), 0.5, 3.0, ((0, 16),))
    expert_in = bell_draw(arg_keys[7], (EXPERTS, D, FF), D ** -0.5, 0.3125, ((2, 32),))
    expert_out = bell_draw(arg_keys[8], (EXPERTS, FF, D), FF ** -0.5, 0.15625, ((1, 32),))
    expert_ids_keys = jax.random.split(jax.random.fold_in(arg_keys[9], 1), TOKENS // GROUP_ROWS)
    expert_ids_turns = jax.random.permutation(jax.random.fold_in(arg_keys[9], 3), TOKENS // GROUP_ROWS)
    expert_ids = jax.vmap(lambda own, number: assign_block(jax.random.fold_in(arg_keys[9], 2), own, number, GROUP_ROWS, EXPERTS, TOP, CAP, 1))(expert_ids_keys, expert_ids_turns).reshape((TOKENS, TOP))
    gate_weights = jnp.clip(0.1 + 0.79999997 * jax.random.uniform(arg_keys[10], (TOKENS, TOP), jnp.float32) ** steps_of(arg_keys[10], (TOKENS, TOP), ((0, 16),), -0.2, 0.2), 0.1, 0.9)
    cotangent = bell_draw(arg_keys[11], (TOKENS, D), 1.0, 6.0, ((0, 32),))
    return {"tokens": tokens, "query_key_value": query_key_value, "attention_out": attention_out, "first_gain": first_gain, "first_shift": first_shift, "second_gain": second_gain, "second_shift": second_shift, "expert_in": expert_in, "expert_out": expert_out, "expert_ids": expert_ids, "gate_weights": gate_weights, "cotangent": cotangent}


@jax.custom_vjp
def low(v):
    return lax.optimization_barrier(v.astype(jnp.bfloat16)).astype(jnp.float32)

@jax.custom_vjp
def low_back(v):
    return v

def low_keep(v):
    return (low(v), None)

def low_pass(kept, grad):
    return (grad,)

def back_keep(v):
    return (v, None)

def back_low(kept, grad):
    return (low(grad),)
low.defvjp(low_keep, low_pass)
low_back.defvjp(back_keep, back_low)
HIGHEST = lax.Precision.HIGHEST
EPSILON = 1e-06

def layer_norm(matrix, scaling, offset):
    centre = matrix - lax.optimization_barrier(jnp.mean(matrix, -1, keepdims=True))
    variance = lax.optimization_barrier(jnp.mean(centre * centre, -1, keepdims=True))
    return centre * lax.rsqrt(variance + EPSILON) * scaling + offset

def place_pairs(routes, number, capacity):
    flattened = routes.reshape(-1)
    matches = (flattened[:, None] == jnp.arange(number, dtype=jnp.int32)[None, :]).astype(jnp.int32)
    earlier = jnp.cumsum(matches, axis=0) - matches
    return (flattened * capacity + lax.optimization_barrier(jnp.sum(earlier * matches, axis=1))).astype(jnp.int32)

def attend_group(packed):
    pieces = packed.reshape(IMGS, SEQ, 3, HEADS, HEAD_DIM)
    queries = pieces[:, :, 0]
    key_rows = pieces[:, :, 1]
    values = pieces[:, :, 2]
    scores = low_back(jnp.einsum('bqhd,bkhd->bhqk', queries, key_rows, precision=HIGHEST) * HEAD_DIM ** (-0.5))
    softened = low(jax.nn.softmax(scores, axis=-1))
    blended = jnp.einsum('bhqk,bkhd->bqhd', softened, values, precision=HIGHEST)
    return low(low_back(blended)).reshape(GROUP_ROWS, D)

def expert_group(normed, routes, weights, first_layer, second_layer):
    position = place_pairs(routes, EXPERTS, CAP)
    owners = jnp.full((EXPERTS * CAP,), GROUP_ROWS, jnp.int32).at[position].set(jnp.arange(GROUP_ROWS * TOP, dtype=jnp.int32) // TOP)
    padded = jnp.concatenate([normed, jnp.zeros((1, D), normed.dtype)], 0)
    loaded = padded[owners].reshape(EXPERTS, CAP, D)
    before_act = low_back(jnp.einsum('ecd,edf->ecf', loaded, first_layer, precision=HIGHEST))
    active = low(jax.nn.gelu(before_act, approximate=False))
    results = low_back(jnp.einsum('ecf,efd->ecd', active, second_layer, precision=HIGHEST)).reshape(EXPERTS * CAP, D)
    chosen = results[position].reshape(GROUP_ROWS, TOP, D)
    return lax.optimization_barrier(jnp.sum(chosen * weights[:, :, None], axis=1))

def reference(tokens, query_key_value, attention_out, first_gain, first_shift, second_gain, second_shift, expert_in, expert_out, expert_ids, gate_weights, cotangent):
    grouped_ids = expert_ids.reshape(N_DP, GROUP_ROWS, TOP)
    grouped_gates = gate_weights.astype(jnp.float32).reshape(N_DP, GROUP_ROWS, TOP)

    def forward(inputs, joint_matrix, out_matrix, gain_one, offset_one, gain_two, offset_two, first_layer, second_layer):
        normed_one = low(layer_norm(inputs, gain_one, offset_one))
        packed = low(low_back(jnp.dot(normed_one, joint_matrix.reshape(D, 3 * D), precision=HIGHEST)))
        blended = lax.map(jax.checkpoint(attend_group), packed.reshape(N_DP, GROUP_ROWS, 3, D)).reshape(TOKENS, D)
        hidden = inputs + low_back(jnp.dot(blended, out_matrix, precision=HIGHEST))
        normed_two = low(layer_norm(hidden, gain_two, offset_two))

        def per_group(members):
            return expert_group(members[0], members[1], members[2], first_layer, second_layer)
        branch = lax.map(jax.checkpoint(per_group), (normed_two.reshape(N_DP, GROUP_ROWS, D), grouped_ids, grouped_gates))
        return hidden + branch.reshape(TOKENS, D)
    result, pullback = jax.vjp(forward, tokens.astype(jnp.float32), query_key_value.astype(jnp.float32), attention_out.astype(jnp.float32), first_gain.astype(jnp.float32), first_shift.astype(jnp.float32), second_gain.astype(jnp.float32), second_shift.astype(jnp.float32), expert_in.astype(jnp.float32), expert_out.astype(jnp.float32))
    gradients = pullback(cotangent.astype(jnp.float32))
    return (result.astype(jnp.bfloat16), gradients[0], gradients[1], gradients[2], gradients[3], gradients[4], gradients[5], gradients[6], gradients[7], gradients[8])
```

```python
import functools

import jax
import jax.numpy as jnp
from jax import lax
from jax.experimental import pallas as pl
from jax.experimental.pallas import tpu as pltpu
from jax.sharding import Mesh
from jax.sharding import PartitionSpec as P

HEAD_DIM = 64
SEQ = 197
EPSILON = 1e-06
ALIGN = 16
WIN = 224
CHUNK = 256
BLOCKS = 4
NEG = -1e30
F32 = jnp.float32
BF16 = jnp.bfloat16
INV_ROOT_TAU = 0.3989422804014327
ALL = ("chip", "core", "tensor")
DP = ("chip", "core")
RING = ("chip", "tensor")
SWAP = [(0, 1), (1, 0)]
VMEM_LIMIT = 60 * 1024 * 1024


def nn(a, b):
    return lax.dot_general(a, b, (((1,), (0,)), ((), ())), preferred_element_type=F32)


def nt(a, b):
    return lax.dot_general(a, b, (((1,), (1,)), ((), ())), preferred_element_type=F32)


def tn(a, b):
    return lax.dot_general(a, b, (((0,), (0,)), ((), ())), preferred_element_type=F32)


def standardize(matrix):
    centre = matrix - jnp.mean(matrix, -1, keepdims=True)
    variance = jnp.mean(centre * centre, -1, keepdims=True)
    inverse = lax.rsqrt(variance + EPSILON)
    return centre * inverse, inverse


def norm_back(weighted, scaled, inverse):
    return inverse * (
        weighted
        - jnp.mean(weighted, -1, keepdims=True)
        - scaled * jnp.mean(weighted * scaled, -1, keepdims=True)
    )


def window(i):
    first = i * SEQ
    start = pl.multiple_of((first // ALIGN) * ALIGN, ALIGN)
    return start, first - start


def put(ref, start, keep, value):
    head = pl.ds(start, ALIGN)
    ref[head, :] = jnp.where(keep, value[:ALIGN], ref[head, :])
    ref[pl.ds(start + ALIGN, WIN - ALIGN), :] = value[ALIGN:]


def fill(dst, src, rows):
    padded = dst.shape[0]
    dst[padded - ALIGN :, :] = jnp.zeros((ALIGN, dst.shape[1]), dst.dtype)
    dst[0:rows, :] = src[...]


def masks(offset):
    row = lax.broadcasted_iota(jnp.int32, (WIN, 1), 0)
    col = lax.broadcasted_iota(jnp.int32, (1, WIN), 1)
    valid = (row >= offset) & (row < offset + SEQ)
    bias = jnp.where((col >= offset) & (col < offset + SEQ), 0.0, NEG).astype(F32)
    keep = lax.broadcasted_iota(jnp.int32, (ALIGN, 1), 0) >= offset
    return valid, bias, keep


def attention_forward(tok, wqkv, wout, par, normed_o, hidden_o, packed_o, mixed_o, lse_o, xs):
    rows, width = tok.shape
    fill(xs, tok, rows)
    lane = lax.broadcasted_iota(jnp.int32, (1, 128), 1)
    low = lane < HEAD_DIM
    gain1, shift1, gain2, shift2 = (par[k : k + 1, :] for k in range(4))

    def image(i, carry):
        start, offset = window(i)
        valid, bias, keep = masks(offset)
        x = xs[pl.ds(start, WIN), :].astype(F32)
        scaled1, _ = standardize(x)
        normed1 = (scaled1 * gain1 + shift1).astype(BF16)
        packed = nn(normed1, wqkv[...]).astype(BF16)
        pieces = []
        lse = jnp.zeros((WIN, 128), F32)
        for pair in range(width // 128):
            at = 128 * pair
            q2 = packed[:, at : at + 128]
            k2 = packed[:, width + at : width + at + 128]
            v2 = packed[:, 2 * width + at : 2 * width + at + 128]
            halves = []
            for half in range(2):
                mine = low if half == 0 else ~low
                qm = jnp.where(mine, q2, jnp.zeros_like(q2)) * jnp.asarray(0.125, BF16)
                s = nt(qm, k2) + bias
                top = jnp.max(s, -1, keepdims=True)
                e = jnp.exp(s - top)
                total = jnp.sum(e, -1, keepdims=True)
                halves.append(nn(e.astype(BF16), v2) * (1.0 / total))
                lse = jnp.where(lane == 2 * pair + half, top + jnp.log(total), lse)
            pieces.append(jnp.where(low, halves[0], halves[1]).astype(BF16))
        mixed = jnp.concatenate(pieces, -1)
        hidden = x + nn(mixed, wout[...])
        scaled2, _ = standardize(hidden)
        put(normed_o, start, keep, (scaled2 * gain2 + shift2).astype(BF16))
        put(hidden_o, start, keep, hidden)
        put(packed_o, start, keep, packed)
        put(mixed_o, start, keep, mixed)
        put(lse_o, start, keep, lse)
        return carry

    lax.fori_loop(0, rows // SEQ, image, 0)


def attention_backward(
    tok, cot, hidden_r, packed_r, mixed_r, lse_r, own, other, wqkv, wout, par,
    out_o, gtok_o, gqkv_o, gout_o, gpar_o, xs, cs, outs, gtoks,
):
    rows, width = tok.shape
    fill(xs, tok, rows)
    fill(cs, cot, rows)
    gqkv_o[...] = jnp.zeros_like(gqkv_o)
    gout_o[...] = jnp.zeros_like(gout_o)
    gpar_o[...] = jnp.zeros_like(gpar_o)
    lane = lax.broadcasted_iota(jnp.int32, (1, 128), 1)
    low = lane < HEAD_DIM
    gain1, shift1, gain2 = (par[k : k + 1, :] for k in range(3))
    eighth = jnp.asarray(0.125, BF16)

    def image(i, carry):
        start, offset = window(i)
        valid, bias, keep = masks(offset)
        here = pl.ds(start, WIN)
        hidden = hidden_r[here, :]
        put(
            outs, start, keep,
            (hidden + own[here, 0:width].astype(F32) + other[here, 0:width].astype(F32)).astype(BF16),
        )
        scaled2, inverse2 = standardize(hidden)
        g2 = own[here, width:].astype(F32) + other[here, width:].astype(F32)
        g2 = jnp.where(valid, g2, 0.0)
        gpar_o[2:3, :] += jnp.sum(g2 * scaled2, 0, keepdims=True)
        gpar_o[3:4, :] += jnp.sum(g2, 0, keepdims=True)
        ghid = cs[here, :].astype(F32) + norm_back(g2 * gain2, scaled2, inverse2)
        branch = jnp.where(valid, ghid, 0.0).astype(BF16)
        gout_o[...] += tn(mixed_r[here, :], branch)
        gmix = nt(branch, wout[...]).astype(BF16)
        gq, gk, gv = [], [], []
        for pair in range(width // 128):
            at = 128 * pair
            q2 = packed_r[here, at : at + 128]
            k2 = packed_r[here, width + at : width + at + 128]
            v2 = packed_r[here, 2 * width + at : 2 * width + at + 128]
            gm2 = gmix[:, at : at + 128]
            sums = [0.0, 0.0, 0.0]
            for half in range(2):
                mine = low if half == 0 else ~low
                qm = jnp.where(mine, q2, jnp.zeros_like(q2)) * eighth
                km = jnp.where(mine, k2, jnp.zeros_like(k2)) * eighth
                gm = jnp.where(mine, gm2, jnp.zeros_like(gm2))
                head = 2 * pair + half
                lse = jnp.where(valid, lse_r[here, head : head + 1], -NEG)
                p = jnp.exp(nt(qm, k2) + bias - lse)
                gp = nt(gm, v2)
                inner = jnp.sum(gp * p, -1, keepdims=True)
                gs = (p * (gp - inner)).astype(BF16)
                sums[0] += nn(gs, km)
                sums[1] += tn(gs, qm)
                sums[2] += tn(p.astype(BF16), gm)
            for store, total in zip((gq, gk, gv), sums):
                store.append(total.astype(BF16))
        gpacked = jnp.concatenate(gq + gk + gv, -1)
        scaled1, inverse1 = standardize(xs[here, :].astype(F32))
        normed1 = (scaled1 * gain1 + shift1).astype(BF16)
        gqkv_o[...] += tn(normed1, gpacked)
        g1 = nt(gpacked, wqkv[...])
        gpar_o[0:1, :] += jnp.sum(g1 * scaled1, 0, keepdims=True)
        gpar_o[1:2, :] += jnp.sum(g1, 0, keepdims=True)
        put(gtoks, start, keep, ghid + norm_back(g1 * gain1, scaled1, inverse1))
        return carry

    lax.fori_loop(0, rows // SEQ, image, 0)
    out_o[...] = outs[0:rows, :]
    gtok_o[...] = gtoks[0:rows, :]


def gelu_parts(v):
    e = jnp.exp(v * v * -0.5)
    t = 1.0 / (1.0 + jnp.abs(v) * (0.3275911 * 0.7071067811865476))
    q = 0.5 * 1.061405429
    for c in (-1.453152027, 1.421413741, -0.284496736, 0.254829592):
        q = q * t + 0.5 * c
    q = q * t * e
    return jnp.where(v < 0, q, 1.0 - q), e * INV_ROOT_TAU


def experts(
    cnt, rown, rsib, cown, csib, town, tsib, w_ref,
    pown, psib, g_ref, xb, gb, tmpx, tmpg, acc1, acc2, off, dst, base, tot,
):
    number = pl.num_programs(0)
    e_now = pl.program_id(0)
    depth = town.shape[2]
    width = rown.shape[1]
    slots = tmpx.shape[0]
    step = slots // 3

    def blocks(fn):
        for side, (table, r, c, out) in enumerate(((town, rown, cown, pown), (tsib, rsib, csib, psib))):
            def body(j, carry, side=side, table=table, r=r, c=c, out=out):
                fn(side * BLOCKS + j, table[j], r, c, out, pl.ds(pl.multiple_of(j * depth, ALIGN), depth))
                return carry

            lax.fori_loop(0, BLOCKS, body, 0)

    def onehot(table, at):
        slot = (lax.broadcasted_iota(jnp.int32, (step, 1), 0) + at).astype(F32)
        first = table[0:1, :] == slot
        second = table[1:2, :] == slot
        gate = jnp.where(first, table[2:3, :], jnp.where(second, table[3:4, :], 0.0))
        pick = jnp.where(first | second, 1.0, 0.0).astype(BF16)
        return pick, jnp.sum(gate, -1, keepdims=True)

    def segments(b, move):
        def per(e, carry):
            k = b * number + e
            o, d = off[k], dst[k]

            def tile(t, carry):
                move(
                    pl.ds(pl.multiple_of(o + t * ALIGN, ALIGN), ALIGN),
                    pl.ds(pl.multiple_of(d + t * ALIGN, ALIGN), ALIGN),
                )
                return carry

            return lax.fori_loop(0, (cnt[k] + (ALIGN - 1)) // ALIGN, tile, carry)

        lax.fori_loop(0, number, per, 0)

    @pl.when(e_now == 0)
    def _():
        def plan_expert(e, at):
            base[e] = at

            def plan_block(b, run):
                dst[b * number + e] = at + run
                return run + (cnt[b * number + e] + (ALIGN - 1)) // ALIGN * ALIGN

            total = lax.fori_loop(0, 2 * BLOCKS, plan_block, 0)
            tot[e] = total
            return at + (total + (CHUNK - 1)) // CHUNK * CHUNK

        lax.fori_loop(0, number, plan_expert, 0)

        def plan_off(b, carry):
            def one(e, run):
                off[b * number + e] = run
                return run + (cnt[b * number + e] + (ALIGN - 1)) // ALIGN * ALIGN

            lax.fori_loop(0, number, one, 0)
            return carry

        lax.fori_loop(0, 2 * BLOCKS, plan_off, 0)

        def dispatch(b, table, r, c, out, here):
            rows, cots = r[here, :], c[here, :]
            for k in range(3):
                pick, gate = onehot(table, k * step)
                tmpx[k * step : (k + 1) * step, :] = nn(pick, rows).astype(BF16)
                tmpg[k * step : (k + 1) * step, :] = (nn(pick, cots) * gate).astype(BF16)

            def move(local, far):
                xb[far, :] = tmpx[local, :]
                gb[far, :] = tmpg[local, :]

            segments(b, move)

        blocks(dispatch)

        def clear(e, carry):
            total = tot[e]
            end = base[e] + total

            def tile(t, carry):
                far = pl.ds(pl.multiple_of(end + t * ALIGN, ALIGN), ALIGN)
                xb[far, :] = jnp.zeros((ALIGN, width), BF16)
                gb[far, :] = jnp.zeros((ALIGN, width), BF16)
                return carry

            rest = (total + (CHUNK - 1)) // CHUNK * CHUNK - total
            return lax.fori_loop(0, rest // ALIGN, tile, carry)

        lax.fori_loop(0, number, clear, 0)

    shards, _, _, units, _ = w_ref.shape
    hidden = shards * units
    acc1[...] = jnp.zeros_like(acc1)
    acc2[...] = jnp.zeros_like(acc2)

    def chunk(t, carry):
        here = pl.ds(pl.multiple_of(base[e_now] + t * CHUNK, ALIGN), CHUNK)
        first = w_ref[:, 0, 0].reshape(hidden, width)
        second = w_ref[:, 0, 1].reshape(hidden, width)
        x, g = xb[here, :], gb[here, :]
        v = nt(x, first)
        big, small = gelu_parts(v)
        act = (v * big).astype(BF16)
        gpre = (nt(g, second) * (big + v * small)).astype(BF16)
        acc1[...] += tn(gpre, x)
        acc2[...] += tn(act, g)
        xb[here, :] = nn(act, second).astype(BF16)
        gb[here, :] = nn(gpre, first).astype(BF16)
        return carry

    lax.fori_loop(0, (tot[e_now] + (CHUNK - 1)) // CHUNK, chunk, 0)
    g_ref[:, 0, 0] = acc1[...].reshape(shards, units, width).astype(BF16)
    g_ref[:, 0, 1] = acc2[...].reshape(shards, units, width).astype(BF16)

    @pl.when(e_now == number - 1)
    def _():
        def combine(b, table, r, c, out, here):
            def move(local, far):
                tmpx[local, :] = xb[far, :]
                tmpg[local, :] = gb[far, :]

            segments(b, move)
            forward, back = 0.0, 0.0
            for k in range(3):
                pick, gate = onehot(table, k * step)
                part = slice(k * step, (k + 1) * step)
                forward += tn(pick, (tmpx[part, :].astype(F32) * gate).astype(BF16))
                back += tn(pick, tmpg[part, :])
            out[here, 0:width] = forward.astype(BF16)
            out[here, width:] = back.astype(BF16)

        blocks(combine)


def route(ids, gates, number, padded):
    rows = ids.shape[1]
    depth = padded // BLOCKS
    ids = jnp.pad(ids, ((0, 0), (0, padded - rows)), constant_values=-1)
    gates = jnp.pad(gates, ((0, 0), (0, padded - rows)))
    ids = ids.reshape(2, BLOCKS, 1, depth)
    gates = gates.reshape(2, BLOCKS, 1, depth)
    match = ids == jnp.arange(number, dtype=jnp.int32)[None, None, :, None]
    named = (match[0] | match[1]).astype(BF16)
    order = jnp.arange(depth)
    earlier = (order[:, None] < order[None, :]).astype(BF16)
    rank = jnp.einsum("ber,rs->bes", named, earlier, preferred_element_type=F32)
    count = jnp.sum(named.astype(F32), -1)
    room = jnp.ceil(count * (1.0 / ALIGN)) * ALIGN
    before = jnp.arange(number)
    off = jnp.sum(jnp.where(before[None, :, None] < before[None, None, :], room[:, :, None], 0.0), 1)
    place = off[:, :, None] + rank
    slot = jnp.sum(jnp.where(match, place[None], 0.0), 2)
    slot = jnp.where(ids[:, :, 0] >= 0, slot, -1.0)
    table = jnp.stack([slot[0], slot[1], gates[0, :, 0], gates[1, :, 0]], 1)
    lanes = jnp.pad(count, ((0, 0), (0, depth - number)))
    return jnp.concatenate([table, lanes[:, None, :], jnp.zeros((BLOCKS, 3, depth), F32)], 1)


def whole(shape, dtype):
    return jax.ShapeDtypeStruct(shape, dtype)


IN_VMEM = pl.BlockSpec(memory_space=pltpu.VMEM)


def on_device(
    tokens, query_key_value, attention_out, first_gain, first_shift, second_gain, second_shift,
    expert_in, expert_out, expert_ids, gate_weights, cotangent,
):
    rows, width = tokens.shape
    padded = -(-rows // (ALIGN * BLOCKS)) * (ALIGN * BLOCKS)
    number = expert_in.shape[0]
    groups, span = lax.axis_size(DP), lax.axis_size("tensor")
    part = width // groups
    wide = width // span
    half = lax.axis_index("tensor")

    small = jnp.concatenate(
        [query_key_value.reshape(-1), attention_out.reshape(-1), first_gain, first_shift, second_gain, second_shift]
    )
    length = small.shape[0]
    rounded = -(-length // 1024) * 1024
    gathered = lax.all_gather(jnp.pad(small, (0, rounded - length)), ALL, axis=0, tiled=False)
    sizes = (query_key_value.size, attention_out.size)
    wqkv = (
        gathered[:, : sizes[0]]
        .reshape(groups, span, part, 3, wide)
        .transpose(0, 2, 3, 1, 4)
        .reshape(width, 3 * width)
    )
    wout = (
        gathered[:, sizes[0] : sizes[0] + sizes[1]]
        .reshape(groups, span, wide, part)
        .transpose(1, 2, 0, 3)
        .reshape(width, width)
    )
    par = (
        gathered.reshape(groups, span, rounded)[:, 0, sizes[0] + sizes[1] : length]
        .reshape(groups, 4, part)
        .transpose(1, 0, 2)
        .reshape(4, width)
        .astype(F32)
    )
    shard = jnp.stack([expert_in.transpose(0, 2, 1), expert_out], 1)
    weights = lax.all_gather(shard, RING, axis=0, tiled=False)
    shards, units = weights.shape[0], weights.shape[3]
    regroup = units % ALIGN != 0
    if regroup:
        weights = weights.transpose(1, 2, 0, 3, 4).reshape(1, number, 2, shards * units, width)

    ids = lax.dynamic_slice_in_dim(expert_ids.T, half * rows, rows, 1)
    gates = lax.dynamic_slice_in_dim(gate_weights.T, half * rows, rows, 1)
    table = route(ids, gates, number, padded)
    table_sib = lax.ppermute(table, "core", SWAP)
    cot_own = jnp.pad(cotangent, ((0, padded - rows), (0, 0)))
    cot_sib = lax.ppermute(cot_own, "core", SWAP)

    normed, hidden, packed, mixed, lse = pl.pallas_call(
        attention_forward,
        out_shape=(
            whole((padded, width), BF16),
            whole((padded, width), F32),
            whole((padded, 3 * width), BF16),
            whole((padded, width), BF16),
            whole((padded, 128), F32),
        ),
        in_specs=[IN_VMEM] * 4,
        out_specs=(IN_VMEM,) * 5,
        scratch_shapes=[pltpu.VMEM((padded, width), BF16)],
        compiler_params=pltpu.CompilerParams(vmem_limit_bytes=VMEM_LIMIT),
        cost_estimate=pl.CostEstimate(flops=6 * 10**9, bytes_accessed=14 * 10**6, transcendentals=3 * 10**6),
        name="attention_forward",
    )(tokens, wqkv, wout, par)
    normed_sib = lax.ppermute(normed, "core", SWAP)

    counts = jnp.concatenate([table[:, 4, :number], table_sib[:, 4, :number]], 0).astype(jnp.int32).reshape(-1)
    n_blocks = 2 * BLOCKS
    room = -(-(4 * rows + n_blocks * number * (ALIGN - 1) + number * (CHUNK - ALIGN)) // CHUNK) * CHUNK
    depth = padded // BLOCKS
    slots = -(-(2 * depth + number * (ALIGN - 1)) // (3 * ALIGN)) * (3 * ALIGN)
    held = weights.shape[0] * weights.shape[3]

    def full(*shape):
        return pl.BlockSpec(shape, lambda e, *_: (0,) * len(shape), pipeline_mode=pl.Buffered(1))

    by_expert = pl.BlockSpec(
        (weights.shape[0], 1, 2, weights.shape[3], width), lambda e, *_: (0, e, 0, 0, 0)
    )
    part_own, part_sib, grads = pl.pallas_call(
        experts,
        out_shape=(
            whole((padded, 2 * width), BF16),
            whole((padded, 2 * width), BF16),
            whole(weights.shape, BF16),
        ),
        grid_spec=pltpu.PrefetchScalarGridSpec(
            num_scalar_prefetch=1,
            grid=(number,),
            in_specs=[full(padded, width)] * 4 + [full(*table.shape)] * 2 + [by_expert],
            out_specs=(full(padded, 2 * width), full(padded, 2 * width), by_expert),
            scratch_shapes=[
                pltpu.VMEM((room, width), BF16),
                pltpu.VMEM((room, width), BF16),
                pltpu.VMEM((slots, width), BF16),
                pltpu.VMEM((slots, width), BF16),
                pltpu.VMEM((held, width), F32),
                pltpu.VMEM((held, width), F32),
                pltpu.SMEM((n_blocks * number,), jnp.int32),
                pltpu.SMEM((n_blocks * number,), jnp.int32),
                pltpu.SMEM((number,), jnp.int32),
                pltpu.SMEM((number,), jnp.int32),
            ],
        ),
        compiler_params=pltpu.CompilerParams(
            vmem_limit_bytes=VMEM_LIMIT, dimension_semantics=("arbitrary",)
        ),
        cost_estimate=pl.CostEstimate(flops=50 * 10**9, bytes_accessed=40 * 10**6, transcendentals=12 * 10**6),
        name="experts",
    )(counts, normed, normed_sib, cot_own, cot_sib, table, table_sib, weights)
    part_other = lax.ppermute(part_sib, "core", SWAP)
    if regroup:
        grads = grads.reshape(number, 2, shards, units, width).transpose(2, 0, 1, 3, 4)
    grad_shard = lax.psum_scatter(grads, RING, scatter_dimension=0, tiled=False).astype(F32)

    output, grad_tokens, gqkv, gout, gpar = pl.pallas_call(
        attention_backward,
        out_shape=(
            whole((rows, width), BF16),
            whole((rows, width), F32),
            whole((width, 3 * width), F32),
            whole((width, width), F32),
            whole((8, width), F32),
        ),
        in_specs=[IN_VMEM] * 11,
        out_specs=(IN_VMEM,) * 5,
        scratch_shapes=[
            pltpu.VMEM((padded, width), BF16),
            pltpu.VMEM((padded, width), BF16),
            pltpu.VMEM((padded, width), BF16),
            pltpu.VMEM((padded, width), F32),
        ],
        compiler_params=pltpu.CompilerParams(vmem_limit_bytes=VMEM_LIMIT),
        cost_estimate=pl.CostEstimate(flops=15 * 10**9, bytes_accessed=25 * 10**6, transcendentals=3 * 10**6),
        name="attention_backward",
    )(tokens, cotangent, hidden, packed, mixed, lse, part_own, part_other, wqkv, wout, par)

    owed = jnp.concatenate(
        [
            gqkv.reshape(groups, part, 3, span, wide).transpose(0, 3, 1, 2, 4).reshape(groups * span, -1),
            gout.reshape(span, wide, groups, part).transpose(2, 0, 1, 3).reshape(groups * span, -1),
            jnp.repeat(gpar[:4].reshape(4, groups, part).transpose(1, 0, 2).reshape(groups, -1), span, axis=0),
        ],
        1,
    )
    owed = jnp.pad(owed, ((0, 0), (0, rounded - length)))
    mine = lax.psum_scatter(owed, ALL, scatter_dimension=0, tiled=False)
    vectors = mine[sizes[0] + sizes[1] : length].reshape(4, part)
    return (
        output,
        grad_tokens,
        mine[: sizes[0]].reshape(part, 3, wide),
        mine[sizes[0] : sizes[0] + sizes[1]].reshape(wide, part),
        vectors[0],
        vectors[1],
        vectors[2],
        vectors[3],
        grad_shard[:, 0].transpose(0, 2, 1),
        grad_shard[:, 1],
    )


def solution(mesh):
    groups, span = mesh.devices.shape
    split = Mesh(mesh.devices.reshape(groups // 2, 2, span), ALL)
    return jax.shard_map(
        on_device,
        mesh=split,
        in_specs=(
            P(ALL, None),
            P(DP, None, "tensor"),
            P("tensor", DP),
            P(DP),
            P(DP),
            P(DP),
            P(DP),
            P(None, None, ALL),
            P(None, ALL, None),
            P(DP, None),
            P(DP, None),
            P(ALL, None),
        ),
        out_specs=(
            P(ALL, None),
            P(ALL, None),
            P(DP, None, "tensor"),
            P("tensor", DP),
            P(DP),
            P(DP),
            P(DP),
            P(DP),
            P(None, None, ALL),
            P(None, ALL, None),
        ),
        check_vma=False,
    )
```

```python
import functools

import jax
import jax.numpy as jnp
from jax import lax
from jax.experimental import pallas as pl
from jax.experimental.pallas import tpu as pltpu
from jax.sharding import Mesh
from jax.sharding import PartitionSpec as P

HEAD_DIM = 64
SEQ = 197
EPSILON = 1e-06
ALIGN = 16
WIN = 224
CHUNK = 256
BLOCKS = 4
NEG = -1e30
F32 = jnp.float32
BF16 = jnp.bfloat16
INV_ROOT_TAU = 0.3989422804014327
ALL = ("chip", "core", "tensor")
DP = ("chip", "core")
RING = ("chip", "tensor")
SWAP = [(0, 1), (1, 0)]
VMEM_LIMIT = 60 * 1024 * 1024


def nn(a, b):
    return lax.dot_general(a, b, (((1,), (0,)), ((), ())), preferred_element_type=F32)


def nt(a, b):
    return lax.dot_general(a, b, (((1,), (1,)), ((), ())), preferred_element_type=F32)


def tn(a, b):
    return lax.dot_general(a, b, (((0,), (0,)), ((), ())), preferred_element_type=F32)


def standardize(matrix):
    centre = matrix - jnp.mean(matrix, -1, keepdims=True)
    variance = jnp.mean(centre * centre, -1, keepdims=True)
    inverse = lax.rsqrt(variance + EPSILON)
    return centre * inverse, inverse


def norm_back(weighted, scaled, inverse):
    return inverse * (
        weighted
        - jnp.mean(weighted, -1, keepdims=True)
        - scaled * jnp.mean(weighted * scaled, -1, keepdims=True)
    )


def window(i):
    first = i * SEQ
    start = pl.multiple_of((first // ALIGN) * ALIGN, ALIGN)
    return start, first - start


def put(ref, start, keep, value):
    head = pl.ds(start, ALIGN)
    ref[head, :] = jnp.where(keep, value[:ALIGN], ref[head, :])
    ref[pl.ds(start + ALIGN, WIN - ALIGN), :] = value[ALIGN:]


def fill(dst, src, rows):
    padded = dst.shape[0]
    dst[padded - ALIGN :, :] = jnp.zeros((ALIGN, dst.shape[1]), dst.dtype)
    dst[0:rows, :] = src[...]


def masks(offset):
    row = lax.broadcasted_iota(jnp.int32, (WIN, 1), 0)
    col = lax.broadcasted_iota(jnp.int32, (1, WIN), 1)
    valid = (row >= offset) & (row < offset + SEQ)
    bias = jnp.where((col >= offset) & (col < offset + SEQ), 0.0, NEG).astype(F32)
    keep = lax.broadcasted_iota(jnp.int32, (ALIGN, 1), 0) >= offset
    return valid, bias, keep


class Spread:
    def __init__(self, src, dst, send, recv, own_sem):
        self.src, self.dst, self.send, self.recv, self.own_sem = src, dst, send, recv, own_sem
        self.chips, self.span = lax.axis_size("chip"), lax.axis_size("tensor")
        self.length = self.chips // 2
        chip = lax.axis_index("chip")
        self.z, self.x, self.y = chip // 2, chip % 2, lax.axis_index("tensor")
        self.sends = []

    def slot(self, z, x, y):
        return (z * 2 + x) * self.span + y

    def links(self):
        return (
            (self.z > 0, {"chip": (self.z - 1) * 2 + self.x}),
            (self.z < self.length - 1, {"chip": (self.z + 1) * 2 + self.x}),
            (None, {"chip": self.z * 2 + 1 - self.x}),
            (None, {"tensor": 1 - self.y}),
        )

    def greet(self, extra=()):
        barrier = pltpu.get_barrier_semaphore()
        for guard, device in self.links() + tuple(extra):
            run(guard, lambda device=device: pl.semaphore_signal(
                barrier, inc=1, device_id=device, device_id_type=pl.DeviceIdType.MESH))
        edge = jnp.where(self.z > 0, 1, 0) + jnp.where(self.z < self.length - 1, 1, 0)
        pl.semaphore_wait(barrier, 2 + len(extra) + edge)

    def copy(self, half, place, device, own, index):
        to = self.dst.at[self.slot(*place), half]
        return pltpu.make_async_remote_copy(
            src_ref=self.src.at[half] if own else to,
            dst_ref=to,
            send_sem=self.send.at[index],
            recv_sem=self.recv.at[self.slot(*place), half],
            device_id=device,
            device_id_type=pl.DeviceIdType.MESH,
        )

    def start(self, guard, half, place, link, own=False):
        index = len(self.sends)
        edge, device = self.links()[link]
        guard = both(guard, edge)
        make = functools.partial(self.copy, half, place, device, own, index)
        self.sends.append((guard, make))
        run(guard, lambda: make().start())

    def arrive(self, guard, half, place):
        make = functools.partial(self.copy, half, place, self.links()[2][1], False, 0)
        run(guard, lambda: make().wait_recv())

    def enter(self, guard, z, own=False):
        for half, link in ((0, 2), (1, 3), (0, 3), (1, 2)):
            self.start(guard, half, (z, self.x, self.y), link, own)

    def cross(self, guard, z):
        for half, place, link in (
            (0, (z, 1 - self.x, self.y), 3),
            (1, (z, self.x, 1 - self.y), 2),
        ):
            self.arrive(guard, half, place)
            self.start(guard, half, place, link)

    def steps(self):
        def first():
            own = pltpu.make_async_copy(self.src, self.dst.at[self.slot(self.z, self.x, self.y)], self.own_sem)
            own.start()
            for link in (0, 1):
                for half in range(2):
                    self.start(None, half, (self.z, self.x, self.y), link, True)
            self.enter(None, self.z, True)

        def hop(d):
            for side, onward in ((-1, 1), (1, 0)):
                z = self.z + side * d
                guard = z >= 0 if side < 0 else z < self.length
                for half in range(2):
                    self.arrive(guard, half, (z, self.x, self.y))
                    self.start(guard, half, (z, self.x, self.y), onward)
                self.enter(guard, z)
            self.crossing(d - 1)

        def last():
            self.crossing(self.length - 1)
            for z in range(self.length):
                for half, place in (
                    (0, (z, self.x, 1 - self.y)),
                    (0, (z, 1 - self.x, 1 - self.y)),
                    (1, (z, 1 - self.x, self.y)),
                    (1, (z, 1 - self.x, 1 - self.y)),
                ):
                    self.arrive(None, half, place)
            for guard, make in self.sends:
                run(guard, lambda make=make: make().wait_send())
            pltpu.make_async_copy(self.src, self.dst.at[self.slot(self.z, self.x, self.y)], self.own_sem).wait()

        return [first] + [functools.partial(hop, d) for d in range(1, self.length)] + [last]

    def crossing(self, d):
        if d == 0:
            self.cross(None, self.z)
        else:
            self.cross(self.z - d >= 0, self.z - d)
            self.cross(self.z + d < self.length, self.z + d)


def both(a, b):
    if a is None or b is None:
        return b if a is None else a
    return a & b


def run(guard, body):
    if guard is None:
        body()
    else:
        pl.when(guard)(body)


def spread_sems(chips, span):
    length = chips // 2
    return [
        pltpu.SemaphoreType.DMA((8 + (2 * length - 2) * 6 + (2 * length - 1) * 2 + 8,)),
        pltpu.SemaphoreType.DMA((chips * span, 2)),
        pltpu.SemaphoreType.DMA,
    ]


def gather_small(src, dst, send, recv, own_sem, core_sem):
    core = lax.axis_index("core")
    spread = Spread(src, dst.at[core], send, recv, own_sem)
    spread.greet(((None, {"core": 1 - core}),))
    for step in spread.steps():
        step()
    across = pltpu.make_async_remote_copy(
        src_ref=dst.at[core],
        dst_ref=dst.at[core],
        send_sem=core_sem.at[0],
        recv_sem=core_sem.at[1],
        device_id={"core": 1 - core},
        device_id_type=pl.DeviceIdType.MESH,
    )
    across.start()
    across.wait_send()
    pltpu.make_async_remote_copy(
        src_ref=dst.at[1 - core],
        dst_ref=dst.at[1 - core],
        send_sem=core_sem.at[0],
        recv_sem=core_sem.at[1],
        device_id={"core": 1 - core},
        device_id_type=pl.DeviceIdType.MESH,
    ).wait_recv()


def attention_forward(
    tok, wqkv, wout, par, shard, normed_o, hidden_o, packed_o, mixed_o, lse_o, all_o, xs, send, recv, own_sem
):
    rows, width = tok.shape
    spread = Spread(shard, all_o, send, recv, own_sem)
    spread.greet()
    first, *rest = spread.steps()
    first()
    fill(xs, tok, rows)
    lane = lax.broadcasted_iota(jnp.int32, (1, 128), 1)
    low = lane < HEAD_DIM
    gain1, shift1, gain2, shift2 = (par[k : k + 1, :] for k in range(4))

    def image(i, carry):
        start, offset = window(i)
        valid, bias, keep = masks(offset)
        x = xs[pl.ds(start, WIN), :].astype(F32)
        scaled1, _ = standardize(x)
        normed1 = (scaled1 * gain1 + shift1).astype(BF16)
        packed = nn(normed1, wqkv[...]).astype(BF16)
        pieces = []
        lse = jnp.zeros((WIN, 128), F32)
        for pair in range(width // 128):
            at = 128 * pair
            q2 = packed[:, at : at + 128]
            k2 = packed[:, width + at : width + at + 128]
            v2 = packed[:, 2 * width + at : 2 * width + at + 128]
            halves = []
            for half in range(2):
                mine = low if half == 0 else ~low
                qm = jnp.where(mine, q2, jnp.zeros_like(q2)) * jnp.asarray(0.125, BF16)
                s = nt(qm, k2) + bias
                top = jnp.max(s, -1, keepdims=True)
                e = jnp.exp(s - top)
                total = jnp.sum(e, -1, keepdims=True)
                halves.append(nn(e.astype(BF16), v2) * (1.0 / total))
                lse = jnp.where(lane == 2 * pair + half, top + jnp.log(total), lse)
            pieces.append(jnp.where(low, halves[0], halves[1]).astype(BF16))
        mixed = jnp.concatenate(pieces, -1)
        hidden = x + nn(mixed, wout[...])
        scaled2, _ = standardize(hidden)
        put(normed_o, start, keep, (scaled2 * gain2 + shift2).astype(BF16))
        put(hidden_o, start, keep, hidden)
        put(packed_o, start, keep, packed)
        put(mixed_o, start, keep, mixed)
        put(lse_o, start, keep, lse)
        return carry

    images = rows // SEQ
    lax.fori_loop(0, images // 2, image, 0)
    rest[0]()
    lax.fori_loop(images // 2, images, image, 0)
    for step in rest[1:]:
        step()


def attention_backward(
    tok, cot, hidden_r, packed_r, mixed_r, lse_r, own, other, wqkv, wout, par,
    out_o, gtok_o, gqkv_o, gout_o, gpar_o, xs, cs, outs, gtoks,
):
    rows, width = tok.shape
    fill(xs, tok, rows)
    fill(cs, cot, rows)
    gqkv_o[...] = jnp.zeros_like(gqkv_o)
    gout_o[...] = jnp.zeros_like(gout_o)
    gpar_o[...] = jnp.zeros_like(gpar_o)
    lane = lax.broadcasted_iota(jnp.int32, (1, 128), 1)
    low = lane < HEAD_DIM
    gain1, shift1, gain2 = (par[k : k + 1, :] for k in range(3))
    eighth = jnp.asarray(0.125, BF16)

    def image(i, carry):
        start, offset = window(i)
        valid, bias, keep = masks(offset)
        here = pl.ds(start, WIN)
        hidden = hidden_r[here, :]
        put(
            outs, start, keep,
            (hidden + own[here, 0:width].astype(F32) + other[here, 0:width].astype(F32)).astype(BF16),
        )
        scaled2, inverse2 = standardize(hidden)
        g2 = own[here, width:].astype(F32) + other[here, width:].astype(F32)
        g2 = jnp.where(valid, g2, 0.0)
        gpar_o[2:3, :] += jnp.sum(g2 * scaled2, 0, keepdims=True)
        gpar_o[3:4, :] += jnp.sum(g2, 0, keepdims=True)
        ghid = cs[here, :].astype(F32) + norm_back(g2 * gain2, scaled2, inverse2)
        branch = jnp.where(valid, ghid, 0.0).astype(BF16)
        gout_o[...] += tn(mixed_r[here, :], branch)
        gmix = nt(branch, wout[...]).astype(BF16)
        gq, gk, gv = [], [], []
        for pair in range(width // 128):
            at = 128 * pair
            q2 = packed_r[here, at : at + 128]
            k2 = packed_r[here, width + at : width + at + 128]
            v2 = packed_r[here, 2 * width + at : 2 * width + at + 128]
            gm2 = gmix[:, at : at + 128]
            sums = [0.0, 0.0, 0.0]
            for half in range(2):
                mine = low if half == 0 else ~low
                qm = jnp.where(mine, q2, jnp.zeros_like(q2)) * eighth
                km = jnp.where(mine, k2, jnp.zeros_like(k2)) * eighth
                gm = jnp.where(mine, gm2, jnp.zeros_like(gm2))
                head = 2 * pair + half
                lse = jnp.where(valid, lse_r[here, head : head + 1], -NEG)
                p = jnp.exp(nt(qm, k2) + bias - lse)
                gp = nt(gm, v2)
                inner = jnp.sum(gp * p, -1, keepdims=True)
                gs = (p * (gp - inner)).astype(BF16)
                sums[0] += nn(gs, km)
                sums[1] += tn(gs, qm)
                sums[2] += tn(p.astype(BF16), gm)
            for store, total in zip((gq, gk, gv), sums):
                store.append(total.astype(BF16))
        gpacked = jnp.concatenate(gq + gk + gv, -1)
        scaled1, inverse1 = standardize(xs[here, :].astype(F32))
        normed1 = (scaled1 * gain1 + shift1).astype(BF16)
        gqkv_o[...] += tn(normed1, gpacked)
        g1 = nt(gpacked, wqkv[...])
        gpar_o[0:1, :] += jnp.sum(g1 * scaled1, 0, keepdims=True)
        gpar_o[1:2, :] += jnp.sum(g1, 0, keepdims=True)
        put(gtoks, start, keep, ghid + norm_back(g1 * gain1, scaled1, inverse1))
        return carry

    lax.fori_loop(0, rows // SEQ, image, 0)
    out_o[...] = outs[0:rows, :]
    gtok_o[...] = gtoks[0:rows, :]


def gelu_parts(v):
    e = jnp.exp(v * v * -0.5)
    t = 1.0 / (1.0 + jnp.abs(v) * (0.3275911 * 0.7071067811865476))
    q = 0.5 * 1.061405429
    for c in (-1.453152027, 1.421413741, -0.284496736, 0.254829592):
        q = q * t + 0.5 * c
    q = q * t * e
    return jnp.where(v < 0, q, 1.0 - q), e * INV_ROOT_TAU


def experts(
    cnt, rown, rsib, cown, csib, town, tsib, w_ref,
    pown, psib, g_ref, xb, gb, tmpx, tmpg, acc1, acc2, off, dst, base, tot,
):
    number = pl.num_programs(0)
    e_now = pl.program_id(0)
    depth = town.shape[2]
    width = rown.shape[1]
    slots = tmpx.shape[0]
    step = slots // 3

    def blocks(fn):
        for side, (table, r, c, out) in enumerate(((town, rown, cown, pown), (tsib, rsib, csib, psib))):
            def body(j, carry, side=side, table=table, r=r, c=c, out=out):
                fn(side * BLOCKS + j, table[j], r, c, out, pl.ds(pl.multiple_of(j * depth, ALIGN), depth))
                return carry

            lax.fori_loop(0, BLOCKS, body, 0)

    def onehot(table, at):
        slot = (lax.broadcasted_iota(jnp.int32, (step, 1), 0) + at).astype(F32)
        first = table[0:1, :] == slot
        second = table[1:2, :] == slot
        gate = jnp.where(first, table[2:3, :], jnp.where(second, table[3:4, :], 0.0))
        pick = jnp.where(first | second, 1.0, 0.0).astype(BF16)
        return pick, jnp.sum(gate, -1, keepdims=True)

    def segments(b, move):
        def per(e, carry):
            k = b * number + e
            o, d = off[k], dst[k]

            def tile(t, carry):
                move(
                    pl.ds(pl.multiple_of(o + t * ALIGN, ALIGN), ALIGN),
                    pl.ds(pl.multiple_of(d + t * ALIGN, ALIGN), ALIGN),
                )
                return carry

            return lax.fori_loop(0, (cnt[k] + (ALIGN - 1)) // ALIGN, tile, carry)

        lax.fori_loop(0, number, per, 0)

    @pl.when(e_now == 0)
    def _():
        def plan_expert(e, at):
            base[e] = at

            def plan_block(b, run):
                dst[b * number + e] = at + run
                return run + (cnt[b * number + e] + (ALIGN - 1)) // ALIGN * ALIGN

            total = lax.fori_loop(0, 2 * BLOCKS, plan_block, 0)
            tot[e] = total
            return at + (total + (CHUNK - 1)) // CHUNK * CHUNK

        lax.fori_loop(0, number, plan_expert, 0)

        def plan_off(b, carry):
            def one(e, run):
                off[b * number + e] = run
                return run + (cnt[b * number + e] + (ALIGN - 1)) // ALIGN * ALIGN

            lax.fori_loop(0, number, one, 0)
            return carry

        lax.fori_loop(0, 2 * BLOCKS, plan_off, 0)

        def dispatch(b, table, r, c, out, here):
            rows, cots = r[here, :], c[here, :]
            for k in range(3):
                pick, gate = onehot(table, k * step)
                tmpx[k * step : (k + 1) * step, :] = nn(pick, rows).astype(BF16)
                tmpg[k * step : (k + 1) * step, :] = (nn(pick, cots) * gate).astype(BF16)

            def move(local, far):
                xb[far, :] = tmpx[local, :]
                gb[far, :] = tmpg[local, :]

            segments(b, move)

        blocks(dispatch)

        def clear(e, carry):
            total = tot[e]
            end = base[e] + total

            def tile(t, carry):
                far = pl.ds(pl.multiple_of(end + t * ALIGN, ALIGN), ALIGN)
                xb[far, :] = jnp.zeros((ALIGN, width), BF16)
                gb[far, :] = jnp.zeros((ALIGN, width), BF16)
                return carry

            rest = (total + (CHUNK - 1)) // CHUNK * CHUNK - total
            return lax.fori_loop(0, rest // ALIGN, tile, carry)

        lax.fori_loop(0, number, clear, 0)

    shards, _, _, units, _ = w_ref.shape
    hidden = shards * units
    acc1[...] = jnp.zeros_like(acc1)
    acc2[...] = jnp.zeros_like(acc2)

    def chunk(t, carry):
        here = pl.ds(pl.multiple_of(base[e_now] + t * CHUNK, ALIGN), CHUNK)
        first = w_ref[:, 0, 0].reshape(hidden, width)
        second = w_ref[:, 0, 1].reshape(hidden, width)
        x, g = xb[here, :], gb[here, :]
        v = nt(x, first)
        big, small = gelu_parts(v)
        act = (v * big).astype(BF16)
        gpre = (nt(g, second) * (big + v * small)).astype(BF16)
        acc1[...] += tn(gpre, x)
        acc2[...] += tn(act, g)
        xb[here, :] = nn(act, second).astype(BF16)
        gb[here, :] = nn(gpre, first).astype(BF16)
        return carry

    lax.fori_loop(0, (tot[e_now] + (CHUNK - 1)) // CHUNK, chunk, 0)
    g_ref[:, 0, 0] = acc1[...].reshape(shards, units, width).astype(BF16)
    g_ref[:, 0, 1] = acc2[...].reshape(shards, units, width).astype(BF16)

    @pl.when(e_now == number - 1)
    def _():
        def combine(b, table, r, c, out, here):
            def move(local, far):
                tmpx[local, :] = xb[far, :]
                tmpg[local, :] = gb[far, :]

            segments(b, move)
            forward, back = 0.0, 0.0
            for k in range(3):
                pick, gate = onehot(table, k * step)
                part = slice(k * step, (k + 1) * step)
                forward += tn(pick, (tmpx[part, :].astype(F32) * gate).astype(BF16))
                back += tn(pick, tmpg[part, :])
            out[here, 0:width] = forward.astype(BF16)
            out[here, width:] = back.astype(BF16)

        blocks(combine)


def route(ids, gates, number, padded):
    rows = ids.shape[1]
    depth = padded // BLOCKS
    ids = jnp.pad(ids, ((0, 0), (0, padded - rows)), constant_values=-1)
    gates = jnp.pad(gates, ((0, 0), (0, padded - rows)))
    ids = ids.reshape(2, BLOCKS, 1, depth)
    gates = gates.reshape(2, BLOCKS, 1, depth)
    match = ids == jnp.arange(number, dtype=jnp.int32)[None, None, :, None]
    named = (match[0] | match[1]).astype(BF16)
    order = jnp.arange(depth)
    earlier = (order[:, None] < order[None, :]).astype(BF16)
    rank = jnp.einsum("ber,rs->bes", named, earlier, preferred_element_type=F32)
    count = jnp.sum(named.astype(F32), -1)
    room = jnp.ceil(count * (1.0 / ALIGN)) * ALIGN
    before = jnp.arange(number)
    off = jnp.sum(jnp.where(before[None, :, None] < before[None, None, :], room[:, :, None], 0.0), 1)
    place = off[:, :, None] + rank
    slot = jnp.sum(jnp.where(match, place[None], 0.0), 2)
    slot = jnp.where(ids[:, :, 0] >= 0, slot, -1.0)
    table = jnp.stack([slot[0], slot[1], gates[0, :, 0], gates[1, :, 0]], 1)
    lanes = jnp.pad(count, ((0, 0), (0, depth - number)))
    return jnp.concatenate([table, lanes[:, None, :], jnp.zeros((BLOCKS, 3, depth), F32)], 1)


def whole(shape, dtype):
    return jax.ShapeDtypeStruct(shape, dtype)


IN_VMEM = pl.BlockSpec(memory_space=pltpu.VMEM)


def on_device(
    tokens, query_key_value, attention_out, first_gain, first_shift, second_gain, second_shift,
    expert_in, expert_out, expert_ids, gate_weights, cotangent,
):
    rows, width = tokens.shape
    padded = -(-rows // (ALIGN * BLOCKS)) * (ALIGN * BLOCKS)
    number = expert_in.shape[0]
    groups, span = lax.axis_size(DP), lax.axis_size("tensor")
    part = width // groups
    wide = width // span
    half = lax.axis_index("tensor")

    small = jnp.concatenate(
        [query_key_value.reshape(-1), attention_out.reshape(-1), first_gain, first_shift, second_gain, second_shift]
    )
    length = small.shape[0]
    chips = groups // 2
    slots_all = chips * span
    rounded = -(-length // 4096) * 4096
    gathered = pl.pallas_call(
        gather_small,
        out_shape=whole((2, slots_all, 2, rounded // 256, 128), BF16),
        in_specs=[IN_VMEM],
        out_specs=pl.BlockSpec(memory_space=pl.ANY),
        scratch_shapes=spread_sems(chips, span) + [pltpu.SemaphoreType.DMA((2,))],
        compiler_params=pltpu.CompilerParams(collective_id=0, has_side_effects=True, vmem_limit_bytes=VMEM_LIMIT),
        name="gather_small",
    )(jnp.pad(small, (0, rounded - length)).reshape(2, rounded // 256, 128))
    gathered = gathered.reshape(2, chips, span, rounded).transpose(1, 0, 2, 3).reshape(groups * span, rounded)
    sizes = (query_key_value.size, attention_out.size)
    wqkv = (
        gathered[:, : sizes[0]]
        .reshape(groups, span, part, 3, wide)
        .transpose(0, 2, 3, 1, 4)
        .reshape(width, 3 * width)
    )
    wout = (
        gathered[:, sizes[0] : sizes[0] + sizes[1]]
        .reshape(groups, span, wide, part)
        .transpose(1, 2, 0, 3)
        .reshape(width, width)
    )
    par = (
        gathered.reshape(groups, span, rounded)[:, 0, sizes[0] + sizes[1] : length]
        .reshape(groups, 4, part)
        .transpose(1, 0, 2)
        .reshape(4, width)
        .astype(F32)
    )
    shard = jnp.stack([expert_in.transpose(0, 2, 1), expert_out], 1)
    shards, units = slots_all, shard.shape[2]

    ids = lax.dynamic_slice_in_dim(expert_ids.T, half * rows, rows, 1)
    gates = lax.dynamic_slice_in_dim(gate_weights.T, half * rows, rows, 1)
    table = route(ids, gates, number, padded)
    table_sib = lax.ppermute(table, "core", SWAP)
    cot_own = jnp.pad(cotangent, ((0, padded - rows), (0, 0)))
    cot_sib = lax.ppermute(cot_own, "core", SWAP)

    normed, hidden, packed, mixed, lse, weights = pl.pallas_call(
        attention_forward,
        out_shape=(
            whole((padded, width), BF16),
            whole((padded, width), F32),
            whole((padded, 3 * width), BF16),
            whole((padded, width), BF16),
            whole((padded, 128), F32),
            whole((shards, 2, number // 2, 2, units, width), BF16),
        ),
        in_specs=[IN_VMEM] * 5,
        out_specs=(IN_VMEM,) * 5 + (pl.BlockSpec(memory_space=pl.ANY),),
        scratch_shapes=[pltpu.VMEM((padded, width), BF16)] + spread_sems(chips, span),
        compiler_params=pltpu.CompilerParams(vmem_limit_bytes=VMEM_LIMIT, collective_id=1, has_side_effects=True),
        cost_estimate=pl.CostEstimate(flops=6 * 10**9, bytes_accessed=14 * 10**6, transcendentals=3 * 10**6),
        name="attention_forward",
    )(tokens, wqkv, wout, par, shard.reshape(2, number // 2, 2, units, width))
    weights = weights.reshape(shards, number, 2, units, width)
    regroup = units % ALIGN != 0
    if regroup:
        weights = weights.transpose(1, 2, 0, 3, 4).reshape(1, number, 2, shards * units, width)
    normed_sib = lax.ppermute(normed, "core", SWAP)

    counts = jnp.concatenate([table[:, 4, :number], table_sib[:, 4, :number]], 0).astype(jnp.int32).reshape(-1)
    n_blocks = 2 * BLOCKS
    room = -(-(4 * rows + n_blocks * number * (ALIGN - 1) + number * (CHUNK - ALIGN)) // CHUNK) * CHUNK
    depth = padded // BLOCKS
    slots = -(-(2 * depth + number * (ALIGN - 1)) // (3 * ALIGN)) * (3 * ALIGN)
    held = weights.shape[0] * weights.shape[3]

    def full(*shape):
        return pl.BlockSpec(shape, lambda e, *_: (0,) * len(shape), pipeline_mode=pl.Buffered(1))

    by_expert = pl.BlockSpec(
        (weights.shape[0], 1, 2, weights.shape[3], width), lambda e, *_: (0, e, 0, 0, 0)
    )
    part_own, part_sib, grads = pl.pallas_call(
        experts,
        out_shape=(
            whole((padded, 2 * width), BF16),
            whole((padded, 2 * width), BF16),
            whole(weights.shape, BF16),
        ),
        grid_spec=pltpu.PrefetchScalarGridSpec(
            num_scalar_prefetch=1,
            grid=(number,),
            in_specs=[full(padded, width)] * 4 + [full(*table.shape)] * 2 + [by_expert],
            out_specs=(full(padded, 2 * width), full(padded, 2 * width), by_expert),
            scratch_shapes=[
                pltpu.VMEM((room, width), BF16),
                pltpu.VMEM((room, width), BF16),
                pltpu.VMEM((slots, width), BF16),
                pltpu.VMEM((slots, width), BF16),
                pltpu.VMEM((held, width), F32),
                pltpu.VMEM((held, width), F32),
                pltpu.SMEM((n_blocks * number,), jnp.int32),
                pltpu.SMEM((n_blocks * number,), jnp.int32),
                pltpu.SMEM((number,), jnp.int32),
                pltpu.SMEM((number,), jnp.int32),
            ],
        ),
        compiler_params=pltpu.CompilerParams(
            vmem_limit_bytes=VMEM_LIMIT, dimension_semantics=("arbitrary",)
        ),
        cost_estimate=pl.CostEstimate(flops=50 * 10**9, bytes_accessed=40 * 10**6, transcendentals=12 * 10**6),
        name="experts",
    )(counts, normed, normed_sib, cot_own, cot_sib, table, table_sib, weights)
    part_other = lax.ppermute(part_sib, "core", SWAP)
    if regroup:
        grads = grads.reshape(number, 2, shards, units, width).transpose(2, 0, 1, 3, 4)
    grad_shard = lax.psum_scatter(grads, RING, scatter_dimension=0, tiled=False).astype(F32)

    output, grad_tokens, gqkv, gout, gpar = pl.pallas_call(
        attention_backward,
        out_shape=(
            whole((rows, width), BF16),
            whole((rows, width), F32),
            whole((width, 3 * width), F32),
            whole((width, width), F32),
            whole((8, width), F32),
        ),
        in_specs=[IN_VMEM] * 11,
        out_specs=(IN_VMEM,) * 5,
        scratch_shapes=[
            pltpu.VMEM((padded, width), BF16),
            pltpu.VMEM((padded, width), BF16),
            pltpu.VMEM((padded, width), BF16),
            pltpu.VMEM((padded, width), F32),
        ],
        compiler_params=pltpu.CompilerParams(vmem_limit_bytes=VMEM_LIMIT),
        cost_estimate=pl.CostEstimate(flops=15 * 10**9, bytes_accessed=25 * 10**6, transcendentals=3 * 10**6),
        name="attention_backward",
    )(tokens, cotangent, hidden, packed, mixed, lse, part_own, part_other, wqkv, wout, par)

    owed = jnp.concatenate(
        [
            gqkv.reshape(groups, part, 3, span, wide).transpose(0, 3, 1, 2, 4).reshape(groups * span, -1),
            gout.reshape(span, wide, groups, part).transpose(2, 0, 1, 3).reshape(groups * span, -1),
            jnp.repeat(gpar[:4].reshape(4, groups, part).transpose(1, 0, 2).reshape(groups, -1), span, axis=0),
        ],
        1,
    )
    owed = jnp.pad(owed, ((0, 0), (0, rounded - length)))
    mine = lax.psum_scatter(owed, ALL, scatter_dimension=0, tiled=False)
    vectors = mine[sizes[0] + sizes[1] : length].reshape(4, part)
    return (
        output,
        grad_tokens,
        mine[: sizes[0]].reshape(part, 3, wide),
        mine[sizes[0] : sizes[0] + sizes[1]].reshape(wide, part),
        vectors[0],
        vectors[1],
        vectors[2],
        vectors[3],
        grad_shard[:, 0].transpose(0, 2, 1),
        grad_shard[:, 1],
    )


def solution(mesh):
    groups, span = mesh.devices.shape
    split = Mesh(mesh.devices.reshape(groups // 2, 2, span), ALL)
    return jax.shard_map(
        on_device,
        mesh=split,
        in_specs=(
            P(ALL, None),
            P(DP, None, "tensor"),
            P("tensor", DP),
            P(DP),
            P(DP),
            P(DP),
            P(DP),
            P(None, None, ALL),
            P(None, ALL, None),
            P(DP, None),
            P(DP, None),
            P(ALL, None),
        ),
        out_specs=(
            P(ALL, None),
            P(ALL, None),
            P(DP, None, "tensor"),
            P("tensor", DP),
            P(DP),
            P(DP),
            P(DP),
            P(DP),
            P(None, None, ALL),
            P(None, ALL, None),
        ),
        check_vma=False,
    )
```

```python
import functools

import jax
import jax.numpy as jnp
from jax import lax
from jax.experimental import pallas as pl
from jax.experimental.pallas import tpu as pltpu
from jax.sharding import Mesh
from jax.sharding import PartitionSpec as P

HEAD_DIM = 64
SEQ = 197
EPSILON = 1e-06
ALIGN = 16
WIN = 224
CHUNK = 256
BLOCKS = 4
NEG = -1e30
F32 = jnp.float32
BF16 = jnp.bfloat16
INV_ROOT_TAU = 0.3989422804014327
ALL = ("chip", "core", "tensor")
DP = ("chip", "core")
RING = ("chip", "tensor")
SWAP = [(0, 1), (1, 0)]
VMEM_LIMIT = 60 * 1024 * 1024


def nn(a, b):
    return lax.dot_general(a, b, (((1,), (0,)), ((), ())), preferred_element_type=F32)


def nt(a, b):
    return lax.dot_general(a, b, (((1,), (1,)), ((), ())), preferred_element_type=F32)


def tn(a, b):
    return lax.dot_general(a, b, (((0,), (0,)), ((), ())), preferred_element_type=F32)


def standardize(matrix):
    centre = matrix - jnp.mean(matrix, -1, keepdims=True)
    variance = jnp.mean(centre * centre, -1, keepdims=True)
    inverse = lax.rsqrt(variance + EPSILON)
    return centre * inverse, inverse


def norm_back(weighted, scaled, inverse):
    return inverse * (
        weighted
        - jnp.mean(weighted, -1, keepdims=True)
        - scaled * jnp.mean(weighted * scaled, -1, keepdims=True)
    )


def window(i):
    first = i * SEQ
    start = pl.multiple_of((first // ALIGN) * ALIGN, ALIGN)
    return start, first - start


def put(ref, start, keep, value):
    head = pl.ds(start, ALIGN)
    ref[head, :] = jnp.where(keep, value[:ALIGN], ref[head, :])
    ref[pl.ds(start + ALIGN, WIN - ALIGN), :] = value[ALIGN:]


def fill(dst, src, rows):
    padded = dst.shape[0]
    dst[padded - ALIGN :, :] = jnp.zeros((ALIGN, dst.shape[1]), dst.dtype)
    dst[0:rows, :] = src[...]


def masks(offset):
    row = lax.broadcasted_iota(jnp.int32, (WIN, 1), 0)
    col = lax.broadcasted_iota(jnp.int32, (1, WIN), 1)
    valid = (row >= offset) & (row < offset + SEQ)
    bias = jnp.where((col >= offset) & (col < offset + SEQ), 0.0, NEG).astype(F32)
    keep = lax.broadcasted_iota(jnp.int32, (ALIGN, 1), 0) >= offset
    return valid, bias, keep


class Place:
    def __init__(self):
        self.chips, self.span = lax.axis_size("chip"), lax.axis_size("tensor")
        self.length = self.chips // 2
        chip = lax.axis_index("chip")
        self.z, self.x, self.y = chip // 2, chip % 2, lax.axis_index("tensor")
        self.sends = []

    def slot(self, z, x, y):
        return (z * 2 + x) * self.span + y

    def links(self):
        return (
            (self.z > 0, {"chip": (self.z - 1) * 2 + self.x}),
            (self.z < self.length - 1, {"chip": (self.z + 1) * 2 + self.x}),
            (None, {"chip": self.z * 2 + 1 - self.x}),
            (None, {"tensor": 1 - self.y}),
        )

    def greet(self, extra=()):
        barrier = pltpu.get_barrier_semaphore()
        for guard, device in self.links() + tuple(extra):
            run(guard, lambda device=device: pl.semaphore_signal(
                barrier, inc=1, device_id=device, device_id_type=pl.DeviceIdType.MESH))
        edge = jnp.where(self.z > 0, 1, 0) + jnp.where(self.z < self.length - 1, 1, 0)
        pl.semaphore_wait(barrier, 2 + len(extra) + edge)

    def post(self, guard, src, dst, recv_sem, link):
        index = len(self.sends)
        edge, device = self.links()[link]
        guard = both(guard, edge)

        def make():
            return remote(src, dst, self.send.at[index], recv_sem, device)

        self.sends.append((guard, make))
        run(guard, lambda: make().start())

    def receive(self, guard, dst, recv_sem):
        run(guard, lambda: remote(dst, dst, self.send.at[0], recv_sem, self.links()[2][1]).wait_recv())

    def drain(self):
        for guard, make in self.sends:
            run(guard, lambda make=make: make().wait_send())


def remote(src, dst, send_sem, recv_sem, device):
    return pltpu.make_async_remote_copy(
        src_ref=src, dst_ref=dst, send_sem=send_sem, recv_sem=recv_sem,
        device_id=device, device_id_type=pl.DeviceIdType.MESH,
    )


class Spread(Place):
    def __init__(self, src, dst, send, recv, own_sem):
        super().__init__()
        self.src, self.dst, self.send, self.recv, self.own_sem = src, dst, send, recv, own_sem

    def start(self, guard, half, place, link, own=False):
        to = self.dst.at[self.slot(*place), half]
        self.post(guard, self.src.at[half] if own else to, to, self.recv.at[self.slot(*place), half], link)

    def arrive(self, guard, half, place):
        self.receive(guard, self.dst.at[self.slot(*place), half], self.recv.at[self.slot(*place), half])

    def enter(self, guard, z, own=False):
        for half, link in ((0, 2), (1, 3), (0, 3), (1, 2)):
            self.start(guard, half, (z, self.x, self.y), link, own)

    def cross(self, guard, z):
        for half, place, link in (
            (0, (z, 1 - self.x, self.y), 3),
            (1, (z, self.x, 1 - self.y), 2),
        ):
            self.arrive(guard, half, place)
            self.start(guard, half, place, link)

    def keep(self):
        return pltpu.make_async_copy(self.src, self.dst.at[self.slot(self.z, self.x, self.y)], self.own_sem)

    def steps(self):
        def first():
            self.keep().start()
            for link in (0, 1):
                for half in range(2):
                    self.start(None, half, (self.z, self.x, self.y), link, True)
            self.enter(None, self.z, True)

        def hop(d):
            for side, onward in ((-1, 1), (1, 0)):
                z = self.z + side * d
                guard = z >= 0 if side < 0 else z < self.length
                for half in range(2):
                    self.arrive(guard, half, (z, self.x, self.y))
                    self.start(guard, half, (z, self.x, self.y), onward)
                self.enter(guard, z)
            self.crossing(d - 1)

        def last():
            self.crossing(self.length - 1)
            for z in range(self.length):
                for half, place in (
                    (0, (z, self.x, 1 - self.y)),
                    (0, (z, 1 - self.x, 1 - self.y)),
                    (1, (z, 1 - self.x, self.y)),
                    (1, (z, 1 - self.x, 1 - self.y)),
                ):
                    self.arrive(None, half, place)
            self.drain()
            self.keep().wait()

        return [first] + [functools.partial(hop, d) for d in range(1, self.length)] + [last]

    def crossing(self, d):
        if d == 0:
            self.cross(None, self.z)
        else:
            self.cross(self.z - d >= 0, self.z - d)
            self.cross(self.z + d < self.length, self.z + d)


def accumulate(dst, src):
    def add(d, s):
        d[...] = (d[...].astype(F32) + s[...].astype(F32)).astype(d.dtype)

    if len(dst.shape) == 2:
        add(dst, src)
        return

    def body(i, carry):
        add(dst.at[i], src.at[i])
        return carry

    lax.fori_loop(0, dst.shape[0], body, 0)


class Reduce(Place):
    def __init__(self, src, first, second, third, out, send, recv1, recv2, recv3, own=None, own_sem=None):
        super().__init__()
        self.src, self.first, self.second, self.third, self.out = src, first, second, third, out
        self.send, self.recv1, self.recv2, self.recv3 = send, recv1, recv2, recv3
        self.own, self.own_sem = own, own_sem

    def target(self, k):
        picked = 0
        for z in range(self.length):
            order = sorted(range(self.length), key=lambda to: (-abs(to - z), to))
            picked = picked + jnp.where(self.z == z, order[k], 0)
        return picked

    def sides(self):
        return ((0, 3, 2, 1 - self.x, self.x), (1, 2, 3, 1 - self.y, self.y))

    def kept(self, half, z, q):
        return self.slot(z, q, self.y) if half == 0 else self.slot(z, self.x, q)

    def sent(self, half, z, q):
        return self.slot(z, q, 1 - self.y) if half == 0 else self.slot(z, 1 - self.x, q)

    def load(self, half, z, q):
        at = 2 * z + q
        return pltpu.make_async_copy(
            self.src.at[self.kept(half, z, q), half], self.own.at[half, at], self.own_sem.at[half, at]
        )

    def stage(self, k):
        z = self.target(k)
        for half, _, _, far, near in self.sides():
            for q in (far, near):
                self.load(half, z, q).start()

    def one(self, k):
        z = self.target(k)
        for half, link, _, far, near in self.sides():
            for q in (far, near):
                self.post(
                    None, self.src.at[self.sent(half, z, q), half], self.first.at[half, 2 * z + q],
                    self.recv1.at[half, 2 * z + q], link,
                )

    def join(self, half, z, q):
        at = 2 * z + q
        self.receive(None, self.first.at[half, at], self.recv1.at[half, at])
        if self.own is None:
            mine = self.src.at[self.kept(half, z, q), half]
        else:
            self.load(half, z, q).wait()
            mine = self.own.at[half, at]
        accumulate(self.first.at[half, at], mine)

    def two(self, k):
        z = self.target(k)
        for half, _, link, far, near in self.sides():
            self.join(half, z, far)
            self.post(
                None, self.first.at[half, 2 * z + far], self.second.at[half, z], self.recv2.at[half, z], link
            )
        for half, _, link, far, near in self.sides():
            self.join(half, z, near)

    def three(self, k):
        z = self.target(k)
        left, right = self.z > 0, self.z < self.length - 1
        for half, _, _, _, near in self.sides():
            run_sum = self.second.at[half, z]
            self.receive(None, run_sum, self.recv2.at[half, z])
            accumulate(run_sum, self.first.at[half, 2 * z + near])
            for guard, more, link, at in (
                (z < self.z, right, 0, jnp.where(z == self.z - 1, self.length, z)),
                (z > self.z, left, 1, z),
            ):
                def take(half=half, run_sum=run_sum):
                    self.receive(None, self.third.at[half, z], self.recv3.at[half, z])
                    accumulate(run_sum, self.third.at[half, z])

                run(guard & more, take)
                self.post(guard, run_sum, self.third.at[half, at], self.recv3.at[half, at], link)

            def settle(half=half, run_sum=run_sum):
                out = self.out.at[half]
                out[...] = run_sum[...].astype(out.dtype)
                for guard, at in ((left, z), (right, self.length)):
                    def take(at=at):
                        self.receive(None, self.third.at[half, at], self.recv3.at[half, at])
                        accumulate(out, self.third.at[half, at])

                    run(guard, take)

            run(z == self.z, settle)


def reduce_sems(length):
    return [
        pltpu.SemaphoreType.DMA((10 * length,)),
        pltpu.SemaphoreType.DMA((2, 2 * length)),
        pltpu.SemaphoreType.DMA((2, length)),
        pltpu.SemaphoreType.DMA((2, length + 1)),
    ]


def reduce_room(length, block, dtype):
    return [pltpu.VMEM((2, n) + block, dtype) for n in (2 * length, length, length + 1)]


def both(a, b):
    if a is None or b is None:
        return b if a is None else a
    return a & b


def run(guard, body):
    if guard is None:
        body()
    else:
        pl.when(guard)(body)


def spread_sems(chips, span):
    length = chips // 2
    return [
        pltpu.SemaphoreType.DMA((8 + (2 * length - 2) * 6 + (2 * length - 1) * 2 + 8,)),
        pltpu.SemaphoreType.DMA((chips * span, 2)),
        pltpu.SemaphoreType.DMA,
    ]


def gather_small(src, wqkv_o, wout_o, par_o, dst, big, send, recv, own_sem, core_sem):
    core = lax.axis_index("core")
    sibling = {"core": 1 - core}
    spread = Spread(src, dst.at[core], send, recv, own_sem)
    spread.greet(((None, sibling),))
    for step in spread.steps():
        step()
    remote(dst.at[core], dst.at[core], core_sem.at[0], core_sem.at[1], sibling).start()
    remote(dst.at[core], dst.at[core], core_sem.at[0], core_sem.at[1], sibling).wait_send()
    remote(dst.at[1 - core], dst.at[1 - core], core_sem.at[0], core_sem.at[1], sibling).wait_recv()
    width, span = wqkv_o.shape[0], spread.span
    part, wide = width // (2 * spread.chips), width // span
    for group in range(2 * spread.chips):
        at = slice(part * group, part * (group + 1))
        for t in range(span):
            slot = (group // 2) * span + t
            piece = jnp.concatenate([dst[group % 2, slot, 0], dst[group % 2, slot, 1]], -1).astype(F32)[:part]
            for k in range(4):
                big[at, width * k + wide * t : width * k + wide * (t + 1)] = piece[:, wide * k : wide * (k + 1)]
            if t == 0:
                big[at, 4 * width : 4 * width + 128] = piece[:, 4 * wide : 4 * wide + 128]
    wqkv_o[...] = big[:, : 3 * width].astype(BF16)
    wout_o[...] = big[:, 3 * width : 4 * width].astype(BF16)
    par_o[...] = big[:, 4 * width : 4 * width + 128].T[0:8]


def attention_forward(
    tok, wqkv, wout, par, shard, normed_o, hidden_o, packed_o, mixed_o, lse_o, all_o, xs, send, recv, own_sem
):
    rows, width = tok.shape
    spread = Spread(shard, all_o, send, recv, own_sem)
    spread.greet()
    first, *rest = spread.steps()
    first()
    fill(xs, tok, rows)
    lane = lax.broadcasted_iota(jnp.int32, (1, 128), 1)
    low = lane < HEAD_DIM
    gain1, shift1, gain2, shift2 = (par[k : k + 1, :] for k in range(4))

    def image(i, carry):
        start, offset = window(i)
        valid, bias, keep = masks(offset)
        x = xs[pl.ds(start, WIN), :].astype(F32)
        scaled1, _ = standardize(x)
        normed1 = (scaled1 * gain1 + shift1).astype(BF16)
        packed = nn(normed1, wqkv[...]).astype(BF16)
        pieces = []
        lse = jnp.zeros((WIN, 128), F32)
        for pair in range(width // 128):
            at = 128 * pair
            q2 = packed[:, at : at + 128]
            k2 = packed[:, width + at : width + at + 128]
            v2 = packed[:, 2 * width + at : 2 * width + at + 128]
            halves = []
            for half in range(2):
                mine = low if half == 0 else ~low
                qm = jnp.where(mine, q2, jnp.zeros_like(q2)) * jnp.asarray(0.125, BF16)
                s = nt(qm, k2) + bias
                top = jnp.max(s, -1, keepdims=True)
                e = jnp.exp(s - top)
                total = jnp.sum(e, -1, keepdims=True)
                halves.append(nn(e.astype(BF16), v2) * (1.0 / total))
                lse = jnp.where(lane == 2 * pair + half, top + jnp.log(total), lse)
            pieces.append(jnp.where(low, halves[0], halves[1]).astype(BF16))
        mixed = jnp.concatenate(pieces, -1)
        hidden = x + nt(mixed, wout[...])
        scaled2, _ = standardize(hidden)
        put(normed_o, start, keep, (scaled2 * gain2 + shift2).astype(BF16))
        put(hidden_o, start, keep, hidden)
        put(packed_o, start, keep, packed)
        put(mixed_o, start, keep, mixed)
        put(lse_o, start, keep, lse)
        return carry

    images = rows // SEQ
    lax.fori_loop(0, images // 2, image, 0)
    rest[0]()
    lax.fori_loop(images // 2, images, image, 0)
    for step in rest[1:]:
        step()


def attention_backward(
    custom, tok, cot, hidden_r, packed_r, mixed_r, lse_r, own, other, wqkv, wout, par, grads,
    out_o, gtok_o, *refs,
):
    if custom:
        (
            gshard_o, small_o, xs, cs, outs, gtoks, gqkv_o, gout_o, gpar_o, pile, theirs,
            w_own, w1, w2, w3, s1, s2, s3, w_send, w_r1, w_r2, w_r3, w_own_sem,
            s_send, s_r1, s_r2, s_r3, core_sem,
        ) = refs
        core = lax.axis_index("core")
        sibling = {"core": 1 - core}
        big = Reduce(grads, w1, w2, w3, gshard_o, w_send, w_r1, w_r2, w_r3, w_own, w_own_sem)
        little = Reduce(pile.at[core], s1, s2, s3, small_o, s_send, s_r1, s_r2, s_r3)
        big.greet(((None, sibling),))
        ranks = range(big.length)
        big.one(0)
        big.one(1)
        for k in ranks:
            big.stage(k)
    else:
        gqkv_o, gout_o, gpar_o, xs, cs, outs, gtoks = refs
    rows, width = tok.shape
    fill(xs, tok, rows)
    fill(cs, cot, rows)
    gqkv_o[...] = jnp.zeros_like(gqkv_o)
    gout_o[...] = jnp.zeros_like(gout_o)
    gpar_o[...] = jnp.zeros_like(gpar_o)
    lane = lax.broadcasted_iota(jnp.int32, (1, 128), 1)
    low = lane < HEAD_DIM
    gain1, shift1, gain2 = (par[k : k + 1, :] for k in range(3))
    eighth = jnp.asarray(0.125, BF16)

    def image(i, carry):
        start, offset = window(i)
        valid, bias, keep = masks(offset)
        here = pl.ds(start, WIN)
        hidden = hidden_r[here, :]
        put(
            outs, start, keep,
            (hidden + own[here, 0:width].astype(F32) + other[here, 0:width].astype(F32)).astype(BF16),
        )
        scaled2, inverse2 = standardize(hidden)
        g2 = own[here, width:].astype(F32) + other[here, width:].astype(F32)
        g2 = jnp.where(valid, g2, 0.0)
        gpar_o[2:3, :] += jnp.sum(g2 * scaled2, 0, keepdims=True)
        gpar_o[3:4, :] += jnp.sum(g2, 0, keepdims=True)
        ghid = cs[here, :].astype(F32) + norm_back(g2 * gain2, scaled2, inverse2)
        branch = jnp.where(valid, ghid, 0.0).astype(BF16)
        gout_o[...] += tn(branch, mixed_r[here, :])
        gmix = nn(branch, wout[...]).astype(BF16)
        gq, gk, gv = [], [], []
        for pair in range(width // 128):
            at = 128 * pair
            q2 = packed_r[here, at : at + 128]
            k2 = packed_r[here, width + at : width + at + 128]
            v2 = packed_r[here, 2 * width + at : 2 * width + at + 128]
            gm2 = gmix[:, at : at + 128]
            sums = [0.0, 0.0, 0.0]
            for half in range(2):
                mine = low if half == 0 else ~low
                qm = jnp.where(mine, q2, jnp.zeros_like(q2)) * eighth
                km = jnp.where(mine, k2, jnp.zeros_like(k2)) * eighth
                gm = jnp.where(mine, gm2, jnp.zeros_like(gm2))
                head = 2 * pair + half
                lse = jnp.where(valid, lse_r[here, head : head + 1], -NEG)
                p = jnp.exp(nt(qm, k2) + bias - lse)
                gp = nt(gm, v2)
                inner = jnp.sum(gp * p, -1, keepdims=True)
                gs = (p * (gp - inner)).astype(BF16)
                sums[0] += nn(gs, km)
                sums[1] += tn(gs, qm)
                sums[2] += tn(p.astype(BF16), gm)
            for store, total in zip((gq, gk, gv), sums):
                store.append(total.astype(BF16))
        gpacked = jnp.concatenate(gq + gk + gv, -1)
        scaled1, inverse1 = standardize(xs[here, :].astype(F32))
        normed1 = (scaled1 * gain1 + shift1).astype(BF16)
        gqkv_o[...] += tn(normed1, gpacked)
        g1 = nt(gpacked, wqkv[...])
        gpar_o[0:1, :] += jnp.sum(g1 * scaled1, 0, keepdims=True)
        gpar_o[1:2, :] += jnp.sum(g1, 0, keepdims=True)
        put(gtoks, start, keep, ghid + norm_back(g1 * gain1, scaled1, inverse1))
        return carry

    images = rows // SEQ

    def finish():
        out_o[...] = outs[0:rows, :]
        gtok_o[...] = gtoks[0:rows, :]

    if not custom:
        lax.fori_loop(0, images, image, 0)
        finish()
        return

    lax.fori_loop(0, 3, image, 0)
    big.two(0)
    big.one(2)
    lax.fori_loop(3, 6, image, 0)
    big.two(1)
    big.one(3)
    lax.fori_loop(6, 8, image, 0)
    big.three(0)
    lax.fori_loop(8, images, image, 0)
    span = big.span
    part, wide = width // (2 * big.chips), width // span
    vectors = gpar_o[...].T
    for t in range(span):
        table = jnp.concatenate(
            [gqkv_o[:, width * k + wide * t : width * k + wide * (t + 1)] for k in range(3)]
            + [gout_o[:, wide * t : wide * (t + 1)], vectors, jnp.zeros_like(vectors)],
            -1,
        )
        for group in range(2 * big.chips):
            for half in range(2):
                pile[group % 2, (group // 2) * span + t, half] = table[
                    part * group : part * (group + 1), 512 * half : 512 * (half + 1)
                ]
    def across():
        return remote(pile.at[1 - core], theirs, core_sem.at[0], core_sem.at[1], sibling)

    across().start()
    big.two(2)
    big.three(1)
    finish()
    across().wait()

    def merge(i, carry):
        accumulate(pile.at[core, i, 0], theirs.at[i, 0])
        accumulate(pile.at[core, i, 1], theirs.at[i, 1])
        return carry

    lax.fori_loop(0, theirs.shape[0], merge, 0)
    for k in ranks:
        little.one(k)
    big.two(3)
    big.three(2)
    for k in ranks:
        little.two(k)
    big.three(3)
    for k in ranks:
        little.three(k)
    big.drain()
    little.drain()


def gelu_parts(v):
    e = jnp.exp(v * v * -0.5)
    t = 1.0 / (1.0 + jnp.abs(v) * (0.3275911 * 0.7071067811865476))
    q = 0.5 * 1.061405429
    for c in (-1.453152027, 1.421413741, -0.284496736, 0.254829592):
        q = q * t + 0.5 * c
    q = q * t * e
    return jnp.where(v < 0, q, 1.0 - q), e * INV_ROOT_TAU


def experts(
    cnt, rown, rsib, cown, csib, town, tsib, w_ref,
    pown, psib, g_ref, xb, gb, tmpx, tmpg, acc1, acc2, off, dst, base, tot,
):
    number = pl.num_programs(0)
    e_now = pl.program_id(0)
    depth = town.shape[2]
    width = rown.shape[1]
    slots = tmpx.shape[0]
    step = slots // 3

    def blocks(fn):
        for side, (table, r, c, out) in enumerate(((town, rown, cown, pown), (tsib, rsib, csib, psib))):
            def body(j, carry, side=side, table=table, r=r, c=c, out=out):
                fn(side * BLOCKS + j, table[j], r, c, out, pl.ds(pl.multiple_of(j * depth, ALIGN), depth))
                return carry

            lax.fori_loop(0, BLOCKS, body, 0)

    def onehot(table, at):
        slot = (lax.broadcasted_iota(jnp.int32, (step, 1), 0) + at).astype(F32)
        first = table[0:1, :] == slot
        second = table[1:2, :] == slot
        gate = jnp.where(first, table[2:3, :], jnp.where(second, table[3:4, :], 0.0))
        pick = jnp.where(first | second, 1.0, 0.0).astype(BF16)
        return pick, jnp.sum(gate, -1, keepdims=True)

    def segments(b, move):
        def per(e, carry):
            k = b * number + e
            o, d = off[k], dst[k]

            def tile(t, carry):
                move(
                    pl.ds(pl.multiple_of(o + t * ALIGN, ALIGN), ALIGN),
                    pl.ds(pl.multiple_of(d + t * ALIGN, ALIGN), ALIGN),
                )
                return carry

            return lax.fori_loop(0, (cnt[k] + (ALIGN - 1)) // ALIGN, tile, carry)

        lax.fori_loop(0, number, per, 0)

    @pl.when(e_now == 0)
    def _():
        def plan_expert(e, at):
            base[e] = at

            def plan_block(b, run):
                dst[b * number + e] = at + run
                return run + (cnt[b * number + e] + (ALIGN - 1)) // ALIGN * ALIGN

            total = lax.fori_loop(0, 2 * BLOCKS, plan_block, 0)
            tot[e] = total
            return at + (total + (CHUNK - 1)) // CHUNK * CHUNK

        lax.fori_loop(0, number, plan_expert, 0)

        def plan_off(b, carry):
            def one(e, run):
                off[b * number + e] = run
                return run + (cnt[b * number + e] + (ALIGN - 1)) // ALIGN * ALIGN

            lax.fori_loop(0, number, one, 0)
            return carry

        lax.fori_loop(0, 2 * BLOCKS, plan_off, 0)

        def dispatch(b, table, r, c, out, here):
            rows, cots = r[here, :], c[here, :]
            for k in range(3):
                pick, gate = onehot(table, k * step)
                tmpx[k * step : (k + 1) * step, :] = nn(pick, rows).astype(BF16)
                tmpg[k * step : (k + 1) * step, :] = (nn(pick, cots) * gate).astype(BF16)

            def move(local, far):
                xb[far, :] = tmpx[local, :]
                gb[far, :] = tmpg[local, :]

            segments(b, move)

        blocks(dispatch)

        def clear(e, carry):
            total = tot[e]
            end = base[e] + total

            def tile(t, carry):
                far = pl.ds(pl.multiple_of(end + t * ALIGN, ALIGN), ALIGN)
                xb[far, :] = jnp.zeros((ALIGN, width), BF16)
                gb[far, :] = jnp.zeros((ALIGN, width), BF16)
                return carry

            rest = (total + (CHUNK - 1)) // CHUNK * CHUNK - total
            return lax.fori_loop(0, rest // ALIGN, tile, carry)

        lax.fori_loop(0, number, clear, 0)

    shards, units = w_ref.shape[0], w_ref.shape[2] // 2
    hidden = shards * units
    acc1[...] = jnp.zeros_like(acc1)
    acc2[...] = jnp.zeros_like(acc2)

    def chunk(t, carry):
        here = pl.ds(pl.multiple_of(base[e_now] + t * CHUNK, ALIGN), CHUNK)
        first = w_ref[:, 0, 0:units].reshape(hidden, width)
        second = w_ref[:, 0, units:].reshape(hidden, width)
        x, g = xb[here, :], gb[here, :]
        v = nt(x, first)
        big, small = gelu_parts(v)
        act = (v * big).astype(BF16)
        gpre = (nt(g, second) * (big + v * small)).astype(BF16)
        acc1[...] += tn(gpre, x)
        acc2[...] += tn(act, g)
        xb[here, :] = nn(act, second).astype(BF16)
        gb[here, :] = nn(gpre, first).astype(BF16)
        return carry

    lax.fori_loop(0, (tot[e_now] + (CHUNK - 1)) // CHUNK, chunk, 0)
    g_ref[:, 0, 0:units] = acc1[...].reshape(shards, units, width).astype(BF16)
    g_ref[:, 0, units:] = acc2[...].reshape(shards, units, width).astype(BF16)

    @pl.when(e_now == number - 1)
    def _():
        def combine(b, table, r, c, out, here):
            def move(local, far):
                tmpx[local, :] = xb[far, :]
                tmpg[local, :] = gb[far, :]

            segments(b, move)
            forward, back = 0.0, 0.0
            for k in range(3):
                pick, gate = onehot(table, k * step)
                part = slice(k * step, (k + 1) * step)
                forward += tn(pick, (tmpx[part, :].astype(F32) * gate).astype(BF16))
                back += tn(pick, tmpg[part, :])
            out[here, 0:width] = forward.astype(BF16)
            out[here, width:] = back.astype(BF16)

        blocks(combine)


def route(ids, gates, number, padded):
    rows = ids.shape[1]
    depth = padded // BLOCKS
    ids = jnp.pad(ids, ((0, 0), (0, padded - rows)), constant_values=-1)
    gates = jnp.pad(gates, ((0, 0), (0, padded - rows)))
    ids = ids.reshape(2, BLOCKS, 1, depth)
    gates = gates.reshape(2, BLOCKS, 1, depth)
    match = ids == jnp.arange(number, dtype=jnp.int32)[None, None, :, None]
    named = (match[0] | match[1]).astype(BF16)
    order = jnp.arange(depth)
    earlier = (order[:, None] < order[None, :]).astype(BF16)
    rank = jnp.einsum("ber,rs->bes", named, earlier, preferred_element_type=F32)
    count = jnp.sum(named.astype(F32), -1)
    room = jnp.ceil(count * (1.0 / ALIGN)) * ALIGN
    before = jnp.arange(number)
    off = jnp.sum(jnp.where(before[None, :, None] < before[None, None, :], room[:, :, None], 0.0), 1)
    place = off[:, :, None] + rank
    slot = jnp.sum(jnp.where(match, place[None], 0.0), 2)
    slot = jnp.where(ids[:, :, 0] >= 0, slot, -1.0)
    table = jnp.stack([slot[0], slot[1], gates[0, :, 0], gates[1, :, 0]], 1)
    lanes = jnp.pad(count, ((0, 0), (0, depth - number)))
    return jnp.concatenate([table, lanes[:, None, :], jnp.zeros((BLOCKS, 3, depth), F32)], 1)


def whole(shape, dtype):
    return jax.ShapeDtypeStruct(shape, dtype)


IN_VMEM = pl.BlockSpec(memory_space=pltpu.VMEM)


def on_device(
    tokens, query_key_value, attention_out, first_gain, first_shift, second_gain, second_shift,
    expert_in, expert_out, expert_ids, gate_weights, cotangent,
):
    rows, width = tokens.shape
    padded = -(-rows // (ALIGN * BLOCKS)) * (ALIGN * BLOCKS)
    number = expert_in.shape[0]
    groups, span = lax.axis_size(DP), lax.axis_size("tensor")
    part = width // groups
    wide = width // span
    half = lax.axis_index("tensor")

    chips = groups // 2
    slots_all = chips * span
    custom = chips == 8 and span == 2 and part % 8 == 0
    vectors = jnp.stack([first_gain, first_shift, second_gain, second_shift], 1)
    small = jnp.concatenate(
        [
            query_key_value.reshape(part, 3 * wide),
            attention_out.T,
            jnp.pad(vectors, ((0, 0), (0, 1024 - 4 * wide - 4))),
        ],
        1,
    )
    shard = jnp.concatenate([expert_in.transpose(0, 2, 1), expert_out], 1)
    shards, units = slots_all, shard.shape[1] // 2
    if custom:
        lines = -(-part // ALIGN) * ALIGN
        wqkv, wout, par = pl.pallas_call(
            gather_small,
            out_shape=(
                whole((width, 3 * width), BF16),
                whole((width, width), BF16),
                whole((8, width), F32),
            ),
            in_specs=[IN_VMEM],
            out_specs=(IN_VMEM,) * 3,
            scratch_shapes=[
                pltpu.VMEM((2, slots_all, 2, lines, 512), BF16),
                pltpu.VMEM((width, 4 * width + 128), F32),
            ]
            + spread_sems(chips, span)
            + [pltpu.SemaphoreType.DMA((2,))],
            compiler_params=pltpu.CompilerParams(collective_id=0, has_side_effects=True, vmem_limit_bytes=VMEM_LIMIT),
            name="gather_small",
        )(jnp.pad(small, ((0, lines - part), (0, 0))).reshape(lines, 2, 512).transpose(1, 0, 2))
    else:
        gathered = lax.all_gather(small, ALL, axis=0, tiled=False).reshape(groups, span, part, 1024)
        taken = gathered[..., : 4 * wide].reshape(groups, span, part, 4, wide)
        taken = taken.transpose(0, 2, 3, 1, 4).reshape(width, 4, width)
        wqkv, wout = taken[:, :3].reshape(width, 3 * width), taken[:, 3]
        par = gathered[:, 0, :, 4 * wide : 4 * wide + 8].reshape(width, 8).T.astype(F32)

    ids = lax.dynamic_slice_in_dim(expert_ids.T, half * rows, rows, 1)
    gates = lax.dynamic_slice_in_dim(gate_weights.T, half * rows, rows, 1)
    table = route(ids, gates, number, padded)
    table_sib = lax.ppermute(table, "core", SWAP)
    cot_own = jnp.pad(cotangent, ((0, padded - rows), (0, 0)))
    cot_sib = lax.ppermute(cot_own, "core", SWAP)

    normed, hidden, packed, mixed, lse, weights = pl.pallas_call(
        attention_forward,
        out_shape=(
            whole((padded, width), BF16),
            whole((padded, width), F32),
            whole((padded, 3 * width), BF16),
            whole((padded, width), BF16),
            whole((padded, 128), F32),
            whole((shards, 2, number // 2, 2 * units, width), BF16),
        ),
        in_specs=[IN_VMEM] * 5,
        out_specs=(IN_VMEM,) * 5 + (pl.BlockSpec(memory_space=pl.ANY),),
        scratch_shapes=[pltpu.VMEM((padded, width), BF16)] + spread_sems(chips, span),
        compiler_params=pltpu.CompilerParams(vmem_limit_bytes=VMEM_LIMIT, collective_id=1, has_side_effects=True),
        cost_estimate=pl.CostEstimate(flops=6 * 10**9, bytes_accessed=14 * 10**6, transcendentals=3 * 10**6),
        name="attention_forward",
    )(tokens, wqkv, wout, par, shard.reshape(2, number // 2, 2 * units, width))
    weights = weights.reshape(shards, number, 2 * units, width)
    regroup = units % ALIGN != 0
    if regroup:
        weights = weights.reshape(shards, number, 2, units, width)
        weights = weights.transpose(1, 2, 0, 3, 4).reshape(1, number, 2 * shards * units, width)
    normed_sib = lax.ppermute(normed, "core", SWAP)

    counts = jnp.concatenate([table[:, 4, :number], table_sib[:, 4, :number]], 0).astype(jnp.int32).reshape(-1)
    n_blocks = 2 * BLOCKS
    room = -(-(4 * rows + n_blocks * number * (ALIGN - 1) + number * (CHUNK - ALIGN)) // CHUNK) * CHUNK
    depth = padded // BLOCKS
    slots = -(-(2 * depth + number * (ALIGN - 1)) // (3 * ALIGN)) * (3 * ALIGN)
    held = weights.shape[0] * weights.shape[2] // 2

    def full(*shape):
        return pl.BlockSpec(shape, lambda e, *_: (0,) * len(shape), pipeline_mode=pl.Buffered(1))

    by_expert = pl.BlockSpec(
        (weights.shape[0], 1, weights.shape[2], width), lambda e, *_: (0, e, 0, 0)
    )
    part_own, part_sib, grads = pl.pallas_call(
        experts,
        out_shape=(
            whole((padded, 2 * width), BF16),
            whole((padded, 2 * width), BF16),
            whole(weights.shape, BF16),
        ),
        grid_spec=pltpu.PrefetchScalarGridSpec(
            num_scalar_prefetch=1,
            grid=(number,),
            in_specs=[full(padded, width)] * 4 + [full(*table.shape)] * 2 + [by_expert],
            out_specs=(full(padded, 2 * width), full(padded, 2 * width), by_expert),
            scratch_shapes=[
                pltpu.VMEM((room, width), BF16),
                pltpu.VMEM((room, width), BF16),
                pltpu.VMEM((slots, width), BF16),
                pltpu.VMEM((slots, width), BF16),
                pltpu.VMEM((held, width), F32),
                pltpu.VMEM((held, width), F32),
                pltpu.SMEM((n_blocks * number,), jnp.int32),
                pltpu.SMEM((n_blocks * number,), jnp.int32),
                pltpu.SMEM((number,), jnp.int32),
                pltpu.SMEM((number,), jnp.int32),
            ],
        ),
        compiler_params=pltpu.CompilerParams(
            vmem_limit_bytes=VMEM_LIMIT, dimension_semantics=("arbitrary",)
        ),
        cost_estimate=pl.CostEstimate(flops=50 * 10**9, bytes_accessed=40 * 10**6, transcendentals=12 * 10**6),
        name="experts",
    )(counts, normed, normed_sib, cot_own, cot_sib, table, table_sib, weights)
    part_other = lax.ppermute(part_sib, "core", SWAP)
    if regroup:
        grads = grads.reshape(number, 2, shards, units, width).transpose(2, 0, 1, 3, 4)
        grads = grads.reshape(shards, number, 2 * units, width)

    sums = [
        pltpu.VMEM((width, 3 * width), F32),
        pltpu.VMEM((width, width), F32),
        pltpu.VMEM((128, width), F32),
    ]
    rows_scratch = [
        pltpu.VMEM((padded, width), BF16),
        pltpu.VMEM((padded, width), BF16),
        pltpu.VMEM((padded, width), BF16),
        pltpu.VMEM((padded, width), F32),
    ]
    operands = (tokens, cotangent, hidden, packed, mixed, lse, part_own, part_other, wqkv, wout, par)
    shapes = (whole((rows, width), BF16), whole((rows, width), F32))
    estimate = pl.CostEstimate(flops=15 * 10**9, bytes_accessed=25 * 10**6, transcendentals=3 * 10**6)
    if custom:
        length = chips // 2
        block, tile = (number // 2, 2 * units, width), (part, 512)
        output, grad_tokens, grad_shard, mine = pl.pallas_call(
            functools.partial(attention_backward, True),
            out_shape=shapes + (whole((2,) + block, F32), whole((2,) + tile, F32)),
            in_specs=[IN_VMEM] * 11 + [pl.BlockSpec(memory_space=pl.ANY)],
            out_specs=(IN_VMEM,) * 4,
            scratch_shapes=rows_scratch
            + sums
            + [pltpu.VMEM((2, shards, 2) + tile, F32), pltpu.VMEM((shards, 2) + tile, F32)]
            + [pltpu.VMEM((2, 2 * length) + block, BF16)]
            + reduce_room(length, block, BF16)
            + reduce_room(length, tile, F32)
            + reduce_sems(length)
            + [pltpu.SemaphoreType.DMA((2, 2 * length))]
            + reduce_sems(length)
            + [pltpu.SemaphoreType.DMA((2,))],
            compiler_params=pltpu.CompilerParams(
                vmem_limit_bytes=VMEM_LIMIT, collective_id=2, has_side_effects=True
            ),
            cost_estimate=estimate,
            name="attention_backward",
        )(*operands, grads.reshape((shards, 2) + block))
        mine = mine.transpose(1, 0, 2).reshape(part, 1024)
        grad_shard = grad_shard.reshape(number, 2 * units, width)
    else:
        output, grad_tokens, gqkv, gout, gpar = pl.pallas_call(
            functools.partial(attention_backward, False),
            out_shape=shapes + tuple(whole(ref.shape, F32) for ref in sums),
            in_specs=[IN_VMEM] * 11 + [pl.BlockSpec(memory_space=pl.ANY)],
            out_specs=(IN_VMEM,) * 5,
            scratch_shapes=rows_scratch,
            compiler_params=pltpu.CompilerParams(vmem_limit_bytes=VMEM_LIMIT),
            cost_estimate=estimate,
            name="attention_backward",
        )(*operands, grads)
        grad_shard = lax.psum_scatter(grads, RING, scatter_dimension=0, tiled=False).astype(F32)
        owed = jnp.concatenate([gqkv.reshape(width, 3, width), gout[:, None]], 1)
        owed = owed.reshape(groups, part, 4, span, wide).transpose(0, 3, 1, 2, 4)
        owed = owed.reshape(groups, span, part, 4 * wide)
        own_vectors = jnp.broadcast_to(gpar[:8].T.reshape(groups, 1, part, 8), (groups, span, part, 8))
        owed = jnp.concatenate([owed, own_vectors], -1).reshape(groups * span, part, 4 * wide + 8)
        mine = lax.psum_scatter(owed, ALL, scatter_dimension=0, tiled=False)
    vectors = mine[:, 4 * wide : 4 * wide + 4]
    return (
        output,
        grad_tokens,
        mine[:, : 3 * wide].reshape(part, 3, wide),
        mine[:, 3 * wide : 4 * wide].T,
        vectors[:, 0],
        vectors[:, 1],
        vectors[:, 2],
        vectors[:, 3],
        grad_shard[:, :units].transpose(0, 2, 1),
        grad_shard[:, units:],
    )


def solution(mesh):
    groups, span = mesh.devices.shape
    split = Mesh(mesh.devices.reshape(groups // 2, 2, span), ALL)
    return jax.shard_map(
        on_device,
        mesh=split,
        in_specs=(
            P(ALL, None),
            P(DP, None, "tensor"),
            P("tensor", DP),
            P(DP),
            P(DP),
            P(DP),
            P(DP),
            P(None, None, ALL),
            P(None, ALL, None),
            P(DP, None),
            P(DP, None),
            P(ALL, None),
        ),
        out_specs=(
            P(ALL, None),
            P(ALL, None),
            P(DP, None, "tensor"),
            P("tensor", DP),
            P(DP),
            P(DP),
            P(DP),
            P(DP),
            P(None, None, ALL),
            P(None, ALL, None),
        ),
        check_vma=False,
    )
```

```python
import functools

import jax
import jax.numpy as jnp
from jax import lax
from jax.experimental import pallas as pl
from jax.experimental.pallas import tpu as pltpu
from jax.sharding import Mesh
from jax.sharding import PartitionSpec as P

HEAD_DIM = 64
SEQ = 197
EPSILON = 1e-06
ALIGN = 16
WIN = 224
CHUNK = 256
BLOCKS = 4
STEP = 192
NEG = -1e30
F32 = jnp.float32
BF16 = jnp.bfloat16
INV_ROOT_TAU = 0.3989422804014327
ALL = ("chip", "core", "tensor")
DP = ("chip", "core")
RING = ("chip", "tensor")
SWAP = [(0, 1), (1, 0)]
VMEM_LIMIT = 60 * 1024 * 1024


def nn(a, b):
    return lax.dot_general(a, b, (((1,), (0,)), ((), ())), preferred_element_type=F32)


def nt(a, b):
    return lax.dot_general(a, b, (((1,), (1,)), ((), ())), preferred_element_type=F32)


def tn(a, b):
    return lax.dot_general(a, b, (((0,), (0,)), ((), ())), preferred_element_type=F32)


def standardize(matrix):
    centre = matrix - jnp.mean(matrix, -1, keepdims=True)
    variance = jnp.mean(centre * centre, -1, keepdims=True)
    inverse = lax.rsqrt(variance + EPSILON)
    return centre * inverse, inverse


def norm_back(weighted, scaled, inverse):
    return inverse * (
        weighted
        - jnp.mean(weighted, -1, keepdims=True)
        - scaled * jnp.mean(weighted * scaled, -1, keepdims=True)
    )


def window(i):
    first = i * SEQ
    start = pl.multiple_of((first // ALIGN) * ALIGN, ALIGN)
    return start, first - start


def put(ref, start, keep, value):
    head = pl.ds(start, ALIGN)
    ref[head, :] = jnp.where(keep, value[:ALIGN], ref[head, :])
    ref[pl.ds(start + ALIGN, WIN - ALIGN), :] = value[ALIGN:]


def fill(dst, src, rows):
    padded = dst.shape[0]
    dst[padded - ALIGN :, :] = jnp.zeros((ALIGN, dst.shape[1]), dst.dtype)
    dst[0:rows, :] = src[...]


def masks(offset):
    row = lax.broadcasted_iota(jnp.int32, (WIN, 1), 0)
    col = lax.broadcasted_iota(jnp.int32, (1, WIN), 1)
    valid = (row >= offset) & (row < offset + SEQ)
    bias = jnp.where((col >= offset) & (col < offset + SEQ), 0.0, NEG).astype(F32)
    keep = lax.broadcasted_iota(jnp.int32, (ALIGN, 1), 0) >= offset
    return valid, bias, keep


class Place:
    def __init__(self):
        self.chips, self.span = lax.axis_size("chip"), lax.axis_size("tensor")
        self.length = self.chips // 2
        chip = lax.axis_index("chip")
        self.z, self.x, self.y = chip // 2, chip % 2, lax.axis_index("tensor")
        self.sends = []

    def slot(self, z, x, y):
        return (z * 2 + x) * self.span + y

    def links(self):
        return (
            (self.z > 0, {"chip": (self.z - 1) * 2 + self.x}),
            (self.z < self.length - 1, {"chip": (self.z + 1) * 2 + self.x}),
            (None, {"chip": self.z * 2 + 1 - self.x}),
            (None, {"tensor": 1 - self.y}),
        )

    def greet(self, extra=()):
        barrier = pltpu.get_barrier_semaphore()
        for guard, device in self.links() + tuple(extra):
            run(guard, lambda device=device: pl.semaphore_signal(
                barrier, inc=1, device_id=device, device_id_type=pl.DeviceIdType.MESH))
        edge = jnp.where(self.z > 0, 1, 0) + jnp.where(self.z < self.length - 1, 1, 0)
        pl.semaphore_wait(barrier, 2 + len(extra) + edge)

    def post(self, guard, src, dst, recv_sem, link):
        index = len(self.sends)
        edge, device = self.links()[link]
        guard = both(guard, edge)

        def make():
            return remote(src, dst, self.send.at[index], recv_sem, device)

        self.sends.append((guard, make))
        run(guard, lambda: make().start())

    def receive(self, guard, dst, recv_sem):
        run(guard, lambda: remote(dst, dst, self.send.at[0], recv_sem, self.links()[2][1]).wait_recv())

    def drain(self):
        for guard, make in self.sends:
            run(guard, lambda make=make: make().wait_send())


def remote(src, dst, send_sem, recv_sem, device):
    return pltpu.make_async_remote_copy(
        src_ref=src, dst_ref=dst, send_sem=send_sem, recv_sem=recv_sem,
        device_id=device, device_id_type=pl.DeviceIdType.MESH,
    )


class Spread(Place):
    def __init__(self, src, own, other, send, recv, keep_sem):
        super().__init__()
        self.src, self.own, self.other = src, own, other
        self.send, self.recv, self.keep_sem = send, recv, keep_sem

    def sides(self):
        return ((0, 2, 3, self.x), (1, 3, 2, self.y))

    def start(self, guard, half, at, rel, link, fresh=False):
        src = self.src[half] if fresh else self.own[half].at[at]
        dst = (self.own, self.other)[rel][half].at[at]
        self.post(guard, src, dst, self.recv.at[half, rel, at], link)

    def arrive(self, guard, half, at, rel):
        self.receive(guard, (self.own, self.other)[rel][half].at[at], self.recv.at[half, rel, at])

    def enter(self, guard, z, fresh=False):
        for half, near_link, far_link, near in self.sides():
            self.start(guard, half, 2 * z + near, 0, near_link, fresh)
        if self.other is not None:
            for half, near_link, far_link, near in self.sides():
                self.start(guard, half, 2 * z + near, 1, far_link, fresh)

    def cross(self, guard, z):
        for half, near_link, far_link, near in self.sides():
            at = 2 * z + 1 - near
            self.arrive(guard, half, at, 0)
            if self.other is not None:
                self.start(guard, half, at, 1, far_link)

    def keep(self, half):
        near = self.sides()[half][3]
        return pltpu.make_async_copy(self.src[half], self.own[half].at[2 * self.z + near], self.keep_sem.at[half])

    def first(self):
        for half in range(2):
            self.keep(half).start()
        for link in (0, 1):
            for half, _, _, near in self.sides():
                self.start(None, half, 2 * self.z + near, 0, link, True)
        self.enter(None, self.z, True)

    def hop(self, d):
        for side, onward in ((-1, 1), (1, 0)):
            z = self.z + side * d
            guard = z >= 0 if side < 0 else z < self.length
            for half, _, _, near in self.sides():
                self.arrive(guard, half, 2 * z + near, 0)
                self.start(guard, half, 2 * z + near, 0, onward)
            self.enter(guard, z)
        self.crossing(d - 1)

    def last(self):
        self.crossing(self.length - 1)
        if self.other is not None:
            for half in range(2):
                for at in range(2 * self.length):
                    self.arrive(None, half, at, 1)
        self.drain()
        for half in range(2):
            self.keep(half).wait()

    def crossing(self, d):
        if d == 0:
            self.cross(None, self.z)
        else:
            self.cross(self.z - d >= 0, self.z - d)
            self.cross(self.z + d < self.length, self.z + d)


def accumulate(dst, src):
    def add(d, s):
        d[...] = (d[...].astype(F32) + s[...].astype(F32)).astype(d.dtype)

    if len(dst.shape) == 2:
        add(dst, src)
        return

    def body(i, carry):
        add(dst.at[i], src.at[i])
        return carry

    lax.fori_loop(0, dst.shape[0], body, 0)


class Reduce(Place):
    def __init__(self, kept, sent, got, first, second, third, out, send, recv1, recv2, recv3, own=None, own_sem=None):
        super().__init__()
        self.kept, self.sent, self.got = kept, sent, got
        self.first, self.second, self.third, self.out = first, second, third, out
        self.send, self.recv1, self.recv2, self.recv3 = send, recv1, recv2, recv3
        self.own, self.own_sem = own, own_sem

    def target(self, k):
        picked = 0
        for z in range(self.length):
            order = sorted(range(self.length), key=lambda to: (-abs(to - z), to))
            picked = picked + jnp.where(self.z == z, order[k], 0)
        return picked

    def sides(self):
        return ((0, 3, 2, 1 - self.x, self.x), (1, 2, 3, 1 - self.y, self.y))

    def loads(self, half, z, q):
        at = 2 * z + q
        copies = []
        if self.own is not None:
            copies.append(
                pltpu.make_async_copy(self.kept(half, z, q), self.own.at[half, at], self.own_sem.at[half, at])
            )
        if self.got is not None:
            copies.append(
                pltpu.make_async_copy(self.got(half, z, q), self.first.at[half, at], self.recv1.at[half, at])
            )
        return copies

    def stage(self, k):
        z = self.target(k)
        for half, _, _, far, near in self.sides():
            for q in (far, near):
                for load in self.loads(half, z, q):
                    load.start()

    def one(self, k):
        z = self.target(k)
        for half, link, _, far, near in self.sides():
            for q in (far, near):
                self.post(
                    None, self.sent(half, z, q), self.first.at[half, 2 * z + q],
                    self.recv1.at[half, 2 * z + q], link,
                )

    def join(self, half, z, q):
        at = 2 * z + q
        if self.got is None:
            self.receive(None, self.first.at[half, at], self.recv1.at[half, at])
        for load in self.loads(half, z, q):
            load.wait()
        accumulate(self.first.at[half, at], self.kept(half, z, q) if self.own is None else self.own.at[half, at])

    def two(self, k):
        z = self.target(k)
        for half, _, link, far, near in self.sides():
            self.join(half, z, far)
            self.post(
                None, self.first.at[half, 2 * z + far], self.second.at[half, z], self.recv2.at[half, z], link
            )
        for half, _, link, far, near in self.sides():
            self.join(half, z, near)

    def three(self, k):
        z = self.target(k)
        left, right = self.z > 0, self.z < self.length - 1
        for half, _, _, _, near in self.sides():
            run_sum = self.second.at[half, z]
            self.receive(None, run_sum, self.recv2.at[half, z])
            accumulate(run_sum, self.first.at[half, 2 * z + near])
            for guard, more, link, at in (
                (z < self.z, right, 0, jnp.where(z == self.z - 1, self.length, z)),
                (z > self.z, left, 1, z),
            ):
                def take(half=half, run_sum=run_sum):
                    self.receive(None, self.third.at[half, z], self.recv3.at[half, z])
                    accumulate(run_sum, self.third.at[half, z])

                run(guard & more, take)
                self.post(guard, run_sum, self.third.at[half, at], self.recv3.at[half, at], link)

            def settle(half=half, run_sum=run_sum):
                out = self.out.at[half]
                out[...] = run_sum[...].astype(out.dtype)
                for guard, at in ((left, z), (right, self.length)):
                    def take(at=at):
                        self.receive(None, self.third.at[half, at], self.recv3.at[half, at])
                        accumulate(out, self.third.at[half, at])

                    run(guard, take)

            run(z == self.z, settle)


def reduce_sems(length):
    return [
        pltpu.SemaphoreType.DMA((10 * length,)),
        pltpu.SemaphoreType.DMA((2, 2 * length)),
        pltpu.SemaphoreType.DMA((2, length)),
        pltpu.SemaphoreType.DMA((2, length + 1)),
    ]


def reduce_room(length, block, dtype):
    return [pltpu.VMEM((2, n) + block, dtype) for n in (2 * length, length, length + 1)]


def both(a, b):
    if a is None or b is None:
        return b if a is None else a
    return a & b


def run(guard, body):
    if guard is None:
        body()
    else:
        pl.when(guard)(body)


def spread_sems(length, rels):
    return [
        pltpu.SemaphoreType.DMA((4 + 2 * rels + (length - 1) * (8 + 4 * rels) + (2 * length - 1) * 2 + 8,)),
        pltpu.SemaphoreType.DMA((2, rels, 2 * length)),
        pltpu.SemaphoreType.DMA((2,)),
    ]


def gather_small(src, wqkv_o, wout_o, par_o, own, other, own_s, other_s, big, send, recv, keep_sem, core_sem):
    core = lax.axis_index("core")
    sibling = {"core": 1 - core}
    halves = range(2)
    spread = Spread(
        [src.at[h] for h in halves], [own.at[h] for h in halves], [other.at[h] for h in halves], send, recv, keep_sem
    )
    spread.greet(((None, sibling),))
    spread.first()
    for d in range(1, spread.length):
        spread.hop(d)
    spread.last()
    across = [remote(a, b, core_sem.at[0, i], core_sem.at[1, i], sibling)
              for i, (a, b) in enumerate(((own, own_s), (other, other_s)))]
    for copy in across:
        copy.start()
    width = wqkv_o.shape[0]
    part, wide = width // (2 * spread.chips), width // spread.span

    def place(core_of, parts, rel):
        for z in range(spread.length):
            for q in range(2):
                for half in halves:
                    piece = parts[half, 2 * z + q].astype(F32)[:part]
                    x = q if half == 0 else (spread.x if rel == 0 else 1 - spread.x)
                    t = q if half == 1 else (spread.y if rel == 0 else 1 - spread.y)
                    group = (2 * z + x) * 2 + core_of
                    at = pl.ds(pl.multiple_of(part * group, 8), part)
                    big[half, t, at, :] = piece

    place(core, own, 0)
    place(core, other, 1)
    for copy in across:
        copy.wait()
    place(1 - core, own_s, 0)
    place(1 - core, other_s, 1)
    pieces = [jnp.concatenate([big[0, t], big[1, t]], -1) for t in range(spread.span)]
    for k in range(4):
        line = jnp.concatenate([p[:, wide * k : wide * (k + 1)] for p in pieces], -1).astype(BF16)
        if k < 3:
            wqkv_o[:, width * k : width * (k + 1)] = line
        else:
            wout_o[...] = line
    par_o[...] = pieces[0][:, 4 * wide : 4 * wide + 128].T[0:8]


def attention_forward(custom, tok, wqkv, wout, par, *refs):
    rows, width = tok.shape
    if custom:
        (
            shard, normed_o, hidden_o, packed_o, mixed_o, lse_o, normed_s, e0, e1, f0, f1, l0, l1,
            xs, e_send, e_recv, e_keep, l_send, l_recv, l_keep, core_sem,
        ) = refs
        early = Spread([shard.at[0], shard.at[1]], [e0, e1], [f0, f1], e_send, e_recv, e_keep)
        late = Spread([shard.at[2], shard.at[3]], [l0, l1], None, l_send, l_recv, l_keep)
        sibling = {"core": 1 - lax.axis_index("core")}
        early.greet(((None, sibling),))
        early.first()
        late.first()
    else:
        normed_o, hidden_o, packed_o, mixed_o, lse_o, xs = refs
    fill(xs, tok, rows)
    lane = lax.broadcasted_iota(jnp.int32, (1, 128), 1)
    low = lane < HEAD_DIM
    gain1, shift1, gain2, shift2 = (par[k : k + 1, :] for k in range(4))

    def image(i, carry):
        start, offset = window(i)
        valid, bias, keep = masks(offset)
        x = xs[pl.ds(start, WIN), :].astype(F32)
        scaled1, _ = standardize(x)
        normed1 = (scaled1 * gain1 + shift1).astype(BF16)
        packed = nn(normed1, wqkv[...]).astype(BF16)
        pieces = []
        lse = jnp.zeros((WIN, 128), F32)
        for pair in range(width // 128):
            at = 128 * pair
            q2 = packed[:, at : at + 128]
            k2 = packed[:, width + at : width + at + 128]
            v2 = packed[:, 2 * width + at : 2 * width + at + 128]
            halves = []
            for half in range(2):
                mine = low if half == 0 else ~low
                qm = jnp.where(mine, q2, jnp.zeros_like(q2)) * jnp.asarray(0.125, BF16)
                s = nt(qm, k2) + bias
                top = jnp.max(s, -1, keepdims=True)
                e = jnp.exp(s - top)
                total = jnp.sum(e, -1, keepdims=True)
                halves.append(nn(e.astype(BF16), v2) * (1.0 / total))
                lse = jnp.where(lane == 2 * pair + half, top + jnp.log(total), lse)
            pieces.append(jnp.where(low, halves[0], halves[1]).astype(BF16))
        mixed = jnp.concatenate(pieces, -1)
        hidden = x + nt(mixed, wout[...])
        scaled2, _ = standardize(hidden)
        put(normed_o, start, keep, (scaled2 * gain2 + shift2).astype(BF16))
        put(hidden_o, start, keep, hidden)
        put(packed_o, start, keep, packed)
        put(mixed_o, start, keep, mixed)
        put(lse_o, start, keep, lse)
        return carry

    images = rows // SEQ
    if not custom:
        lax.fori_loop(0, images, image, 0)
        return
    lax.fori_loop(0, 6, image, 0)
    early.hop(1)
    late.hop(1)
    lax.fori_loop(6, images, image, 0)
    across = remote(normed_o, normed_s, core_sem.at[0], core_sem.at[1], sibling)
    across.start()
    for d in range(2, early.length):
        early.hop(d)
        late.hop(d)
    early.last()
    late.last()
    across.wait()


def attention_backward(custom, tok, cot, hidden_r, packed_r, mixed_r, lse_r, own, given, wqkv, wout, par, *refs):
    rows, width = tok.shape
    other = given
    if custom:
        (
            ek0, ek1, er0, er1, lk0, lk1, ls0, ls1,
            out_o, gtok_o, early_o, late_o, small_o, xs, cs, outs, gtoks, gqkv_o, gout_o, gpar_o, pile, theirs, others,
            *room,
        ) = refs
        core = lax.axis_index("core")
        sibling = {"core": 1 - core}
        (e_own, e1, e2, e3, l_own, l1, l2, l3, s1, s2, s3,
         e_send, e_r1, e_r2, e_r3, e_sem, l_send, l_r1, l_r2, l_r3, l_sem, s_send, s_r1, s_r2, s_r3, core_sem) = room
        ek, er, lk, ls = (ek0, ek1), (er0, er1), (lk0, lk1), (ls0, ls1)
        early = Reduce(
            lambda half, z, q: ek[half].at[2 * z + q], None, lambda half, z, q: er[half].at[2 * z + q],
            e1, e2, e3, early_o, e_send, e_r1, e_r2, e_r3, e_own, e_sem,
        )
        late = Reduce(
            lambda half, z, q: lk[half].at[2 * z + q], lambda half, z, q: ls[half].at[2 * z + q], None,
            l1, l2, l3, late_o, l_send, l_r1, l_r2, l_r3, l_own, l_sem,
        )
        def pile_at(half, z, x, y):
            return pile.at[core, late.slot(z, x, y), half]

        little = Reduce(
            lambda half, z, q: pile_at(half, z, q, late.y) if half == 0 else pile_at(half, z, late.x, q),
            lambda half, z, q: pile_at(half, z, q, 1 - late.y) if half == 0 else pile_at(half, z, 1 - late.x, q),
            None, s1, s2, s3, small_o, s_send, s_r1, s_r2, s_r3,
        )
        late.greet(((None, sibling),))
        ranks = range(late.length)
        middle = others.shape[0] // 2

        def rows_across(i):
            part = pl.ds(i * middle, middle)
            return remote(given.at[part], others.at[part], core_sem.at[0, i], core_sem.at[1, i], sibling)

        for i in range(2):
            rows_across(i).start()
        late.one(0)
        for k in ranks:
            early.stage(k)
            late.stage(k)
        early.two(0)
        late.one(1)
        early.two(1)
        other = others
        rows_across(0).wait()
    else:
        out_o, gtok_o, gqkv_o, gout_o, gpar_o, xs, cs, outs, gtoks = refs
    fill(xs, tok, rows)
    fill(cs, cot, rows)
    gqkv_o[...] = jnp.zeros_like(gqkv_o)
    gout_o[...] = jnp.zeros_like(gout_o)
    gpar_o[...] = jnp.zeros_like(gpar_o)
    lane = lax.broadcasted_iota(jnp.int32, (1, 128), 1)
    low = lane < HEAD_DIM
    gain1, shift1, gain2 = (par[k : k + 1, :] for k in range(3))
    eighth = jnp.asarray(0.125, BF16)

    def image(i, carry):
        start, offset = window(i)
        valid, bias, keep = masks(offset)
        here = pl.ds(start, WIN)
        hidden = hidden_r[here, :]
        put(
            outs, start, keep,
            (hidden + own[here, 0:width].astype(F32) + other[here, 0:width].astype(F32)).astype(BF16),
        )
        scaled2, inverse2 = standardize(hidden)
        g2 = own[here, width:].astype(F32) + other[here, width:].astype(F32)
        g2 = jnp.where(valid, g2, 0.0)
        gpar_o[2:3, :] += jnp.sum(g2 * scaled2, 0, keepdims=True)
        gpar_o[3:4, :] += jnp.sum(g2, 0, keepdims=True)
        ghid = cs[here, :].astype(F32) + norm_back(g2 * gain2, scaled2, inverse2)
        branch = jnp.where(valid, ghid, 0.0).astype(BF16)
        gout_o[...] += tn(branch, mixed_r[here, :])
        gmix = nn(branch, wout[...]).astype(BF16)
        gq, gk, gv = [], [], []
        for pair in range(width // 128):
            at = 128 * pair
            q2 = packed_r[here, at : at + 128]
            k2 = packed_r[here, width + at : width + at + 128]
            v2 = packed_r[here, 2 * width + at : 2 * width + at + 128]
            gm2 = gmix[:, at : at + 128]
            sums = [0.0, 0.0, 0.0]
            for half in range(2):
                mine = low if half == 0 else ~low
                qm = jnp.where(mine, q2, jnp.zeros_like(q2)) * eighth
                km = jnp.where(mine, k2, jnp.zeros_like(k2)) * eighth
                gm = jnp.where(mine, gm2, jnp.zeros_like(gm2))
                head = 2 * pair + half
                lse = jnp.where(valid, lse_r[here, head : head + 1], -NEG)
                p = jnp.exp(nt(qm, k2) + bias - lse)
                gp = nt(gm, v2)
                inner = jnp.sum(gp * p, -1, keepdims=True)
                gs = (p * (gp - inner)).astype(BF16)
                sums[0] += nn(gs, km)
                sums[1] += tn(gs, qm)
                sums[2] += tn(p.astype(BF16), gm)
            for store, total in zip((gq, gk, gv), sums):
                store.append(total.astype(BF16))
        gpacked = jnp.concatenate(gq + gk + gv, -1)
        scaled1, inverse1 = standardize(xs[here, :].astype(F32))
        normed1 = (scaled1 * gain1 + shift1).astype(BF16)
        gqkv_o[...] += tn(normed1, gpacked)
        g1 = nt(gpacked, wqkv[...])
        gpar_o[0:1, :] += jnp.sum(g1 * scaled1, 0, keepdims=True)
        gpar_o[1:2, :] += jnp.sum(g1, 0, keepdims=True)
        put(gtoks, start, keep, ghid + norm_back(g1 * gain1, scaled1, inverse1))
        return carry

    images = rows // SEQ

    def finish():
        out_o[...] = outs[0:rows, :]
        gtok_o[...] = gtoks[0:rows, :]

    if not custom:
        lax.fori_loop(0, images, image, 0)
        finish()
        return

    lax.fori_loop(0, 3, image, 0)
    rows_across(1).wait()
    late.two(0)
    late.one(2)
    early.two(2)
    early.three(0)
    lax.fori_loop(3, 6, image, 0)
    late.two(1)
    late.one(3)
    early.two(3)
    early.three(1)
    late.three(0)
    lax.fori_loop(6, 8, image, 0)
    late.two(2)
    early.three(2)
    lax.fori_loop(8, images, image, 0)
    span = late.span
    part, wide = width // (2 * late.chips), width // span
    vectors = gpar_o[...].T
    for t in range(span):
        table = jnp.concatenate(
            [gqkv_o[:, width * k + wide * t : width * k + wide * (t + 1)] for k in range(3)]
            + [gout_o[:, wide * t : wide * (t + 1)], vectors, jnp.zeros_like(vectors)],
            -1,
        )
        for group in range(2 * late.chips):
            for half in range(2):
                pile[group % 2, (group // 2) * span + t, half] = table[
                    part * group : part * (group + 1), 512 * half : 512 * (half + 1)
                ]

    def across():
        return remote(pile.at[1 - core], theirs, core_sem.at[0, 2], core_sem.at[1, 2], sibling)

    across().start()
    late.two(3)
    late.three(1)
    early.three(3)
    finish()
    across().wait()

    def merge(i, carry):
        accumulate(pile.at[core, i, 0], theirs.at[i, 0])
        accumulate(pile.at[core, i, 1], theirs.at[i, 1])
        return carry

    lax.fori_loop(0, theirs.shape[0], merge, 0)
    for k in ranks:
        little.one(k)
    late.three(2)
    for k in ranks:
        little.two(k)
    late.three(3)
    for k in ranks:
        little.three(k)
    early.drain()
    late.drain()
    little.drain()


def gelu_parts(v):
    e = jnp.exp(v * v * -0.5)
    t = 1.0 / (1.0 + jnp.abs(v) * (0.3275911 * 0.7071067811865476))
    q = 0.5 * 1.061405429
    for c in (-1.453152027, 1.421413741, -0.284496736, 0.254829592):
        q = q * t + 0.5 * c
    q = q * t * e
    return jnp.where(v < 0, q, 1.0 - q), e * INV_ROOT_TAU


def experts(row, prior, cnt, rown, rsib, cown, csib, town, tsib, *refs):
    if prior:
        pown_i, psib_i, *refs = refs
    else:
        pown_i = psib_i = None
    (
        own0, oth0, own1, oth1, pown, psib, k0, n0, k1, n1,
        xb, gb, tmpx, tmpg, acc1, acc2, wa, wb, fw, bk, off, dst, base, tot,
    ) = refs
    number = pl.num_programs(0)
    e_now = pl.program_id(0)
    depth = town.shape[2]
    width = rown.shape[1]

    def blocks(fn):
        for side, args in enumerate(((town, rown, cown, pown, pown_i), (tsib, rsib, csib, psib, psib_i))):
            def body(j, carry, side=side, args=args):
                fn(side * BLOCKS + j, args[0][j], *args[1:], pl.ds(pl.multiple_of(j * depth, ALIGN), depth))
                return carry

            lax.fori_loop(0, BLOCKS, body, 0)

    def onehot(table, at):
        slot = (lax.broadcasted_iota(jnp.int32, (STEP, 1), 0) + at).astype(F32)
        first = table[row : row + 1, :] == slot
        second = table[row + 1 : row + 2, :] == slot
        gate = jnp.where(first, table[2:3, :], jnp.where(second, table[3:4, :], 0.0))
        pick = jnp.where(first | second, 1.0, 0.0).astype(BF16)
        return pick, jnp.sum(gate, -1, keepdims=True)

    def padded(k):
        return (cnt[k] + (ALIGN - 1)) // ALIGN * ALIGN

    def steps(b):
        last = b * number + number - 1
        return (off[last] + padded(last) + (STEP - 1)) // STEP

    def segments(b, move):
        def per(e, carry):
            k = b * number + e
            o, d = off[k], dst[k]

            def tile(t, carry):
                move(
                    pl.ds(pl.multiple_of(o + t * ALIGN, ALIGN), ALIGN),
                    pl.ds(pl.multiple_of(d + t * ALIGN, ALIGN), ALIGN),
                )
                return carry

            return lax.fori_loop(0, padded(k) // ALIGN, tile, carry)

        lax.fori_loop(0, number, per, 0)

    @pl.when(e_now == 0)
    def _():
        def plan_expert(e, at):
            base[e] = at

            def plan_block(b, run):
                dst[b * number + e] = at + run
                return run + padded(b * number + e)

            total = lax.fori_loop(0, 2 * BLOCKS, plan_block, 0)
            tot[e] = total
            return at + (total + (CHUNK - 1)) // CHUNK * CHUNK

        lax.fori_loop(0, number, plan_expert, 0)

        def plan_off(b, carry):
            def one(e, run):
                off[b * number + e] = run
                return run + padded(b * number + e)

            lax.fori_loop(0, number, one, 0)
            return carry

        lax.fori_loop(0, 2 * BLOCKS, plan_off, 0)

        def dispatch(b, table, r, c, out, before, here):
            def some(k, carry):
                at = pl.multiple_of(k * STEP, ALIGN)
                pick, gate = onehot(table, at)
                tmpx[pl.ds(at, STEP), :] = nn(pick, r[here, :]).astype(BF16)
                tmpg[pl.ds(at, STEP), :] = (nn(pick, c[here, :]) * gate).astype(BF16)
                return carry

            lax.fori_loop(0, steps(b), some, 0)

            def move(local, far):
                xb[far, :] = tmpx[local, :]
                gb[far, :] = tmpg[local, :]

            segments(b, move)

        blocks(dispatch)

        def clear(e, carry):
            total = tot[e]
            end = base[e] + total

            def tile(t, carry):
                far = pl.ds(pl.multiple_of(end + t * ALIGN, ALIGN), ALIGN)
                xb[far, :] = jnp.zeros((ALIGN, width), BF16)
                gb[far, :] = jnp.zeros((ALIGN, width), BF16)
                return carry

            rest = (total + (CHUNK - 1)) // CHUNK * CHUNK - total
            return lax.fori_loop(0, rest // ALIGN, tile, carry)

        lax.fori_loop(0, number, clear, 0)

    shards, units = own0.shape[0], own0.shape[2] // 2
    middle = shards * units
    lower = e_now < number // 2

    def load(own, other):
        for i, ref in enumerate((own, other)):
            to = slice(i * middle, (i + 1) * middle)
            wa[to, :] = ref[:, 0, 0:units].reshape(middle, width)
            wb[to, :] = ref[:, 0, units:].reshape(middle, width)

    pl.when(lower)(lambda: load(own0, oth0))
    pl.when(~lower)(lambda: load(own1, oth1))
    acc1[...] = jnp.zeros_like(acc1)
    acc2[...] = jnp.zeros_like(acc2)

    def chunk(t, carry):
        here = pl.ds(pl.multiple_of(base[e_now] + t * CHUNK, ALIGN), CHUNK)
        first, second = wa[...], wb[...]
        x, g = xb[here, :], gb[here, :]
        v = nt(x, first)
        big, small = gelu_parts(v)
        act = (v * big).astype(BF16)
        gpre = (nt(g, second) * (big + v * small)).astype(BF16)
        acc1[...] += tn(gpre, x)
        acc2[...] += tn(act, g)
        xb[here, :] = nn(act, second).astype(BF16)
        gb[here, :] = nn(gpre, first).astype(BF16)
        return carry

    lax.fori_loop(0, (tot[e_now] + (CHUNK - 1)) // CHUNK, chunk, 0)

    def save(kept, sent):
        for i, ref in enumerate((kept, sent)):
            part = slice(i * middle, (i + 1) * middle)
            ref[:, 0, 0:units] = acc1[part, :].reshape(shards, units, width).astype(BF16)
            ref[:, 0, units:] = acc2[part, :].reshape(shards, units, width).astype(BF16)

    pl.when(lower)(lambda: save(k0, n0))
    pl.when(~lower)(lambda: save(k1, n1))

    @pl.when(e_now == number - 1)
    def _():
        def combine(b, table, r, c, out, before, here):
            def move(local, far):
                tmpx[local, :] = xb[far, :]
                tmpg[local, :] = gb[far, :]

            segments(b, move)
            if before is None:
                fw[...] = jnp.zeros_like(fw)
                bk[...] = jnp.zeros_like(bk)
            else:
                fw[...] = before[here, 0:width].astype(F32)
                bk[...] = before[here, width:].astype(F32)

            def some(k, carry):
                at = pl.multiple_of(k * STEP, ALIGN)
                pick, gate = onehot(table, at)
                fw[...] += tn(pick, (tmpx[pl.ds(at, STEP), :].astype(F32) * gate).astype(BF16))
                bk[...] += tn(pick, tmpg[pl.ds(at, STEP), :])
                return carry

            lax.fori_loop(0, steps(b), some, 0)
            out[here, 0:width] = fw[...].astype(BF16)
            out[here, width:] = bk[...].astype(BF16)

        blocks(combine)


def run_experts(late, tables, counts, row_refs, weights, prior):
    padded, width = row_refs[0].shape
    number, n_blocks = 2 * weights[0].shape[1], 2 * BLOCKS
    depth = padded // BLOCKS
    pairs = 4 * padded
    room = -(-(pairs + n_blocks * number * (ALIGN - 1) + number * (CHUNK - ALIGN)) // CHUNK) * CHUNK
    slots = -(-(2 * depth + number * (ALIGN - 1)) // STEP) * STEP
    shards, _, lines, _ = weights[0].shape
    held = shards * lines

    def full(*shape):
        return pl.BlockSpec(shape, lambda e, *_: (0,) * len(shape), pipeline_mode=pl.Buffered(1))

    block = (shards, 1, lines, width)
    lower = pl.BlockSpec(block, lambda e, *_: (0, jnp.minimum(e, number // 2 - 1), 0, 0))
    upper = pl.BlockSpec(block, lambda e, *_: (0, jnp.maximum(e - number // 2, 0), 0, 0))
    sums = full(padded, 2 * width)
    grad = whole(weights[0].shape, BF16)
    return pl.pallas_call(
        functools.partial(experts, 5 if late else 0, prior is not None),
        out_shape=(whole((padded, 2 * width), BF16),) * 2 + (grad,) * 4,
        grid_spec=pltpu.PrefetchScalarGridSpec(
            num_scalar_prefetch=1,
            grid=(number,),
            in_specs=[full(padded, width)] * 4
            + [full(*tables[0].shape)] * 2
            + [sums] * (0 if prior is None else 2)
            + [lower, lower, upper, upper],
            out_specs=(sums, sums, lower, lower, upper, upper),
            scratch_shapes=[
                pltpu.VMEM((room, width), BF16),
                pltpu.VMEM((room, width), BF16),
                pltpu.VMEM((slots, width), BF16),
                pltpu.VMEM((slots, width), BF16),
                pltpu.VMEM((held, width), F32),
                pltpu.VMEM((held, width), F32),
                pltpu.VMEM((held, width), BF16),
                pltpu.VMEM((held, width), BF16),
                pltpu.VMEM((depth, width), F32),
                pltpu.VMEM((depth, width), F32),
                pltpu.SMEM((n_blocks * number,), jnp.int32),
                pltpu.SMEM((n_blocks * number,), jnp.int32),
                pltpu.SMEM((number,), jnp.int32),
                pltpu.SMEM((number,), jnp.int32),
            ],
        ),
        compiler_params=pltpu.CompilerParams(
            vmem_limit_bytes=VMEM_LIMIT, dimension_semantics=("arbitrary",)
        ),
        cost_estimate=pl.CostEstimate(flops=25 * 10**9, bytes_accessed=20 * 10**6, transcendentals=6 * 10**6),
        name="experts_late" if late else "experts_early",
    )(counts, *row_refs, *tables, *(() if prior is None else prior), *weights)


def route(ids, gates, number, padded):
    rows = ids.shape[1]
    depth = padded // BLOCKS
    ids = jnp.pad(ids, ((0, 0), (0, padded - rows)), constant_values=-1)
    gates = jnp.pad(gates, ((0, 0), (0, padded - rows)))
    ids = ids.reshape(2, BLOCKS, 1, depth)
    gates = gates.reshape(2, BLOCKS, 1, depth)
    listed = jnp.arange(number, dtype=jnp.int32)
    match = ids == listed[None, None, :, None]
    named = (match[0] | match[1]).astype(BF16)
    order = jnp.arange(depth)
    earlier = (order[:, None] < order[None, :]).astype(BF16)
    rank = jnp.einsum("ber,rs->bes", named, earlier, preferred_element_type=F32)
    count = jnp.sum(named.astype(F32), -1)
    room = jnp.ceil(count * (1.0 / ALIGN)) * ALIGN
    middle = number // 2
    ahead = (listed[:, None] < listed[None, :]) & (listed[:, None] // middle == listed[None, :] // middle)
    off = jnp.sum(jnp.where(ahead[None], room[:, :, None], 0.0), 1)
    place = off[:, :, None] + rank
    slot = jnp.sum(jnp.where(match, place[None], 0.0), 2)
    flat = ids[:, :, 0]
    first = jnp.where((flat >= 0) & (flat < middle), slot, -1.0)
    second = jnp.where(flat >= middle, slot, -1.0)
    lanes = jnp.pad(count, ((0, 0), (0, depth - number)))
    return jnp.stack(
        [first[0], first[1], gates[0, :, 0], gates[1, :, 0], lanes, second[0], second[1], jnp.zeros_like(lanes)], 1
    )


def whole(shape, dtype):
    return jax.ShapeDtypeStruct(shape, dtype)


IN_VMEM = pl.BlockSpec(memory_space=pltpu.VMEM)
ANYWHERE = pl.BlockSpec(memory_space=pl.ANY)


def on_device(
    tokens, query_key_value, attention_out, first_gain, first_shift, second_gain, second_shift,
    expert_in, expert_out, expert_ids, gate_weights, cotangent,
):
    rows, width = tokens.shape
    padded = -(-rows // (ALIGN * BLOCKS)) * (ALIGN * BLOCKS)
    number = expert_in.shape[0]
    groups, span = lax.axis_size(DP), lax.axis_size("tensor")
    part = width // groups
    wide = width // span
    side = lax.axis_index("tensor")
    chips = groups // 2
    length = chips // 2
    custom = chips == 8 and span == 2 and part % 8 == 0
    vectors = jnp.stack([first_gain, first_shift, second_gain, second_shift], 1)
    small = jnp.concatenate(
        [
            query_key_value.reshape(part, 3 * wide),
            attention_out.T,
            jnp.pad(vectors, ((0, 0), (0, 1024 - 4 * wide - 4))),
        ],
        1,
    )
    shard = jnp.concatenate([expert_in.transpose(0, 2, 1), expert_out], 1)
    units = shard.shape[1] // 2
    if custom:
        lines = -(-part // ALIGN) * ALIGN
        wqkv, wout, par = pl.pallas_call(
            gather_small,
            out_shape=(
                whole((width, 3 * width), BF16),
                whole((width, width), BF16),
                whole((8, width), F32),
            ),
            in_specs=[IN_VMEM],
            out_specs=(IN_VMEM,) * 3,
            scratch_shapes=[pltpu.VMEM((2, 2 * length, lines, 512), BF16)] * 4
            + [pltpu.VMEM((2, span, width, 512), F32)]
            + spread_sems(length, 2)
            + [pltpu.SemaphoreType.DMA((2, 2))],
            compiler_params=pltpu.CompilerParams(collective_id=0, has_side_effects=True, vmem_limit_bytes=VMEM_LIMIT),
            name="gather_small",
        )(jnp.pad(small, ((0, lines - part), (0, 0))).reshape(lines, 2, 512).transpose(1, 0, 2))
    else:
        gathered = lax.all_gather(small, ALL, axis=0, tiled=False).reshape(groups, span, part, 1024)
        taken = gathered[..., : 4 * wide].reshape(groups, span, part, 4, wide)
        taken = taken.transpose(0, 2, 3, 1, 4).reshape(width, 4, width)
        wqkv, wout = taken[:, :3].reshape(width, 3 * width), taken[:, 3]
        par = gathered[:, 0, :, 4 * wide : 4 * wide + 8].reshape(width, 8).T.astype(F32)

    ids = lax.dynamic_slice_in_dim(expert_ids.T, side * rows, rows, 1)
    gates = lax.dynamic_slice_in_dim(gate_weights.T, side * rows, rows, 1)
    table = route(ids, gates, number, padded)
    table_sib = lax.ppermute(table, "core", SWAP)
    cot_own = jnp.pad(cotangent, ((0, padded - rows), (0, 0)))
    cot_sib = lax.ppermute(cot_own, "core", SWAP)

    row_shapes = (
        whole((padded, width), BF16),
        whole((padded, width), F32),
        whole((padded, 3 * width), BF16),
        whole((padded, width), BF16),
        whole((padded, 128), F32),
    )
    estimate = pl.CostEstimate(flops=6 * 10**9, bytes_accessed=14 * 10**6, transcendentals=3 * 10**6)
    xs_scratch = [pltpu.VMEM((padded, width), BF16)]
    quarter = number // 4
    if custom:
        held = whole((2 * length, quarter, 2 * units, width), BF16)
        normed, hidden, packed, mixed, lse, normed_sib, e0, e1, f0, f1, l0, l1 = pl.pallas_call(
            functools.partial(attention_forward, True),
            out_shape=row_shapes + (row_shapes[0],) + (held,) * 6,
            in_specs=[IN_VMEM] * 5,
            out_specs=(IN_VMEM,) * 6 + (ANYWHERE,) * 6,
            scratch_shapes=xs_scratch
            + spread_sems(length, 2)
            + spread_sems(length, 1)
            + [pltpu.SemaphoreType.DMA((2,))],
            compiler_params=pltpu.CompilerParams(vmem_limit_bytes=VMEM_LIMIT, collective_id=1, has_side_effects=True),
            cost_estimate=estimate,
            name="attention_forward",
        )(tokens, wqkv, wout, par, shard.reshape(4, quarter, 2 * units, width))
        across_y = functools.partial(lax.ppermute, axis_name="tensor", perm=SWAP)
        across_x = functools.partial(lax.ppermute, axis_name="chip", perm=[(c, c ^ 1) for c in range(chips)])
        early_weights = (e0, f0, e1, f1)
        late_weights = (l0, across_y(l0), l1, across_x(l1))
    else:
        normed, hidden, packed, mixed, lse = pl.pallas_call(
            functools.partial(attention_forward, False),
            out_shape=row_shapes,
            in_specs=[IN_VMEM] * 4,
            out_specs=(IN_VMEM,) * 5,
            scratch_shapes=xs_scratch,
            compiler_params=pltpu.CompilerParams(vmem_limit_bytes=VMEM_LIMIT),
            cost_estimate=estimate,
            name="attention_forward",
        )(tokens, wqkv, wout, par)
        normed_sib = lax.ppermute(normed, "core", SWAP)
        weights = lax.all_gather(shard, RING, axis=0, tiled=False)
        shards = weights.shape[0]
        weights = weights.reshape(2, shards // 2, 4, quarter, 2, units, width).transpose(2, 0, 3, 4, 1, 5, 6)
        weights = weights.reshape(4, 2, 1, quarter, shards * units, width)
        early_weights = tuple(weights[i, j] for i in (0, 1) for j in (0, 1))
        late_weights = tuple(weights[i, j] for i in (2, 3) for j in (0, 1))

    middle = number // 2
    both_counts = jnp.concatenate([table[:, 4, :number], table_sib[:, 4, :number]], 0).astype(jnp.int32)
    row_refs = (normed, normed_sib, cot_own, cot_sib)
    tables = (table, table_sib)
    own1, sib1, *early = run_experts(
        False, tables, both_counts[:, :middle].reshape(-1), row_refs, early_weights, None
    )
    if custom:
        got = (across_y(early[1]), across_x(early[3]))
    part_own, part_sib, *late = run_experts(
        True, tables, both_counts[:, middle:].reshape(-1), row_refs, late_weights, (own1, sib1)
    )

    sums = [
        pltpu.VMEM((width, 3 * width), F32),
        pltpu.VMEM((width, width), F32),
        pltpu.VMEM((128, width), F32),
    ]
    rows_scratch = [
        pltpu.VMEM((padded, width), BF16),
        pltpu.VMEM((padded, width), BF16),
        pltpu.VMEM((padded, width), BF16),
        pltpu.VMEM((padded, width), F32),
    ]
    saved = (tokens, cotangent, hidden, packed, mixed, lse, part_own)
    shapes = (whole((rows, width), BF16), whole((rows, width), F32))
    estimate = pl.CostEstimate(flops=15 * 10**9, bytes_accessed=25 * 10**6, transcendentals=3 * 10**6)
    if custom:
        block, tile = (quarter, 2 * units, width), (part, 512)
        output, grad_tokens, early_grad, late_grad, mine = pl.pallas_call(
            functools.partial(attention_backward, True),
            out_shape=shapes + (whole((2,) + block, F32),) * 2 + (whole((2,) + tile, F32),),
            in_specs=[IN_VMEM] * 7 + [ANYWHERE] + [IN_VMEM] * 3 + [ANYWHERE] * 8,
            out_specs=(IN_VMEM,) * 5,
            scratch_shapes=rows_scratch
            + sums
            + [pltpu.VMEM((2, 2 * chips, 2) + tile, F32), pltpu.VMEM((2 * chips, 2) + tile, F32)]
            + [pltpu.VMEM((padded, 2 * width), BF16)]
            + ([pltpu.VMEM((2, 2 * length) + block, BF16)] + reduce_room(length, block, BF16)) * 2
            + reduce_room(length, tile, F32)
            + (reduce_sems(length) + [pltpu.SemaphoreType.DMA((2, 2 * length))]) * 2
            + reduce_sems(length)
            + [pltpu.SemaphoreType.DMA((2, 3))],
            compiler_params=pltpu.CompilerParams(
                vmem_limit_bytes=VMEM_LIMIT, collective_id=2, has_side_effects=True
            ),
            cost_estimate=estimate,
            name="attention_backward",
        )(*saved, part_sib, wqkv, wout, par, early[0], early[2], *got, late[0], late[2], late[1], late[3])
        mine = mine.transpose(1, 0, 2).reshape(part, 1024)
        grad_shard = jnp.concatenate([early_grad, late_grad], 0).reshape(number, 2 * units, width)
    else:
        part_other = lax.ppermute(part_sib, "core", SWAP)
        output, grad_tokens, gqkv, gout, gpar = pl.pallas_call(
            functools.partial(attention_backward, False),
            out_shape=shapes + tuple(whole(ref.shape, F32) for ref in sums),
            in_specs=[IN_VMEM] * 11,
            out_specs=(IN_VMEM,) * 5,
            scratch_shapes=rows_scratch,
            compiler_params=pltpu.CompilerParams(vmem_limit_bytes=VMEM_LIMIT),
            cost_estimate=estimate,
            name="attention_backward",
        )(*saved, part_other, wqkv, wout, par)
        grads = jnp.stack(early + late).reshape(4, 2, quarter, 2, shards // 2, units, width)
        grads = grads.transpose(1, 4, 0, 2, 3, 5, 6).reshape(shards, number, 2 * units, width)
        grad_shard = lax.psum_scatter(grads, RING, scatter_dimension=0, tiled=False).astype(F32)
        owed = jnp.concatenate([gqkv.reshape(width, 3, width), gout[:, None]], 1)
        owed = owed.reshape(groups, part, 4, span, wide).transpose(0, 3, 1, 2, 4)
        owed = owed.reshape(groups, span, part, 4 * wide)
        own_vectors = jnp.broadcast_to(gpar[:8].T.reshape(groups, 1, part, 8), (groups, span, part, 8))
        owed = jnp.concatenate([owed, own_vectors], -1).reshape(groups * span, part, 4 * wide + 8)
        mine = lax.psum_scatter(owed, ALL, scatter_dimension=0, tiled=False)
    vectors = mine[:, 4 * wide : 4 * wide + 4]
    return (
        output,
        grad_tokens,
        mine[:, : 3 * wide].reshape(part, 3, wide),
        mine[:, 3 * wide : 4 * wide].T,
        vectors[:, 0],
        vectors[:, 1],
        vectors[:, 2],
        vectors[:, 3],
        grad_shard[:, :units].transpose(0, 2, 1),
        grad_shard[:, units:],
    )


def solution(mesh):
    groups, span = mesh.devices.shape
    split = Mesh(mesh.devices.reshape(groups // 2, 2, span), ALL)
    return jax.shard_map(
        on_device,
        mesh=split,
        in_specs=(
            P(ALL, None),
            P(DP, None, "tensor"),
            P("tensor", DP),
            P(DP),
            P(DP),
            P(DP),
            P(DP),
            P(None, None, ALL),
            P(None, ALL, None),
            P(DP, None),
            P(DP, None),
            P(ALL, None),
        ),
        out_specs=(
            P(ALL, None),
            P(ALL, None),
            P(DP, None, "tensor"),
            P("tensor", DP),
            P(DP),
            P(DP),
            P(DP),
            P(DP),
            P(None, None, ALL),
            P(None, ALL, None),
        ),
        check_vma=False,
    )
```

```python
import functools

import jax
import jax.numpy as jnp
from jax import lax
from jax.experimental import pallas as pl
from jax.experimental.pallas import tpu as pltpu
from jax.sharding import Mesh
from jax.sharding import PartitionSpec as P

HEAD_DIM = 64
SEQ = 197
EPSILON = 1e-06
ALIGN = 16
WIN = 224
CHUNK = 384
BLOCKS = 4
STEP = 576
NEG = -1e30
F32 = jnp.float32
BF16 = jnp.bfloat16
INV_ROOT_TAU = 0.3989422804014327
ALL = ("chip", "core", "tensor")
DP = ("chip", "core")
RING = ("chip", "tensor")
SWAP = [(0, 1), (1, 0)]
VMEM_LIMIT = 60 * 1024 * 1024


def nn(a, b):
    return lax.dot_general(a, b, (((1,), (0,)), ((), ())), preferred_element_type=F32)


def nt(a, b):
    return lax.dot_general(a, b, (((1,), (1,)), ((), ())), preferred_element_type=F32)


def tn(a, b):
    return lax.dot_general(a, b, (((0,), (0,)), ((), ())), preferred_element_type=F32)


def standardize(matrix):
    centre = matrix - jnp.mean(matrix, -1, keepdims=True)
    variance = jnp.mean(centre * centre, -1, keepdims=True)
    inverse = lax.rsqrt(variance + EPSILON)
    return centre * inverse, inverse


def norm_back(weighted, scaled, inverse):
    return inverse * (
        weighted
        - jnp.mean(weighted, -1, keepdims=True)
        - scaled * jnp.mean(weighted * scaled, -1, keepdims=True)
    )


def window(i):
    first = i * SEQ
    start = pl.multiple_of((first // ALIGN) * ALIGN, ALIGN)
    return start, first - start


def put(ref, start, keep, value):
    head = pl.ds(start, ALIGN)
    ref[head, :] = jnp.where(keep, value[:ALIGN], ref[head, :])
    ref[pl.ds(start + ALIGN, WIN - ALIGN), :] = value[ALIGN:]


def fill(dst, src, rows):
    whole_rows = rows // ALIGN * ALIGN
    dst[whole_rows:, :] = jnp.zeros((dst.shape[0] - whole_rows, dst.shape[1]), dst.dtype)
    dst[0:rows, :] = src[...]


def masks(offset):
    row = lax.broadcasted_iota(jnp.int32, (WIN, 1), 0)
    col = lax.broadcasted_iota(jnp.int32, (1, WIN), 1)
    valid = (row >= offset) & (row < offset + SEQ)
    bias = jnp.where((col >= offset) & (col < offset + SEQ), 0.0, NEG).astype(F32)
    keep = lax.broadcasted_iota(jnp.int32, (ALIGN, 1), 0) >= offset
    return valid, bias, keep


class Place:
    def __init__(self):
        self.chips, self.span = lax.axis_size("chip"), lax.axis_size("tensor")
        self.length = self.chips // 2
        chip = lax.axis_index("chip")
        self.z, self.x, self.y = chip // 2, chip % 2, lax.axis_index("tensor")
        self.sends = []

    def slot(self, z, x, y):
        return (z * 2 + x) * self.span + y

    def links(self):
        return (
            (self.z > 0, {"chip": (self.z - 1) * 2 + self.x}),
            (self.z < self.length - 1, {"chip": (self.z + 1) * 2 + self.x}),
            (None, {"chip": self.z * 2 + 1 - self.x}),
            (None, {"tensor": 1 - self.y}),
        )

    def greet(self, extra=()):
        barrier = pltpu.get_barrier_semaphore()
        for guard, device in self.links() + tuple(extra):
            run(guard, lambda device=device: pl.semaphore_signal(
                barrier, inc=1, device_id=device, device_id_type=pl.DeviceIdType.MESH))
        edge = jnp.where(self.z > 0, 1, 0) + jnp.where(self.z < self.length - 1, 1, 0)
        pl.semaphore_wait(barrier, 2 + len(extra) + edge)

    def post(self, guard, src, dst, recv_sem, link):
        index = len(self.sends)
        edge, device = self.links()[link]
        guard = both(guard, edge)

        def make():
            return remote(src, dst, self.send.at[index], recv_sem, device)

        self.sends.append((guard, make))
        run(guard, lambda: make().start())

    def receive(self, guard, dst, recv_sem):
        run(guard, lambda: remote(dst, dst, self.send.at[0], recv_sem, self.links()[2][1]).wait_recv())

    def drain(self):
        for guard, make in self.sends:
            run(guard, lambda make=make: make().wait_send())


def remote(src, dst, send_sem, recv_sem, device):
    return pltpu.make_async_remote_copy(
        src_ref=src, dst_ref=dst, send_sem=send_sem, recv_sem=recv_sem,
        device_id=device, device_id_type=pl.DeviceIdType.MESH,
    )


class Spread(Place):
    def __init__(self, src, own, other, send, recv, keep_sem):
        super().__init__()
        self.src, self.own, self.other = src, own, other
        self.send, self.recv, self.keep_sem = send, recv, keep_sem

    def sides(self):
        return ((0, 2, 3, self.x), (1, 3, 2, self.y))

    def start(self, guard, half, at, rel, link, fresh=False):
        src = self.src[half] if fresh else self.own[half].at[at]
        dst = (self.own, self.other)[rel][half].at[at]
        self.post(guard, src, dst, self.recv.at[half, rel, at], link)

    def arrive(self, guard, half, at, rel):
        self.receive(guard, (self.own, self.other)[rel][half].at[at], self.recv.at[half, rel, at])

    def enter(self, guard, z, fresh=False):
        for half, near_link, far_link, near in self.sides():
            self.start(guard, half, 2 * z + near, 0, near_link, fresh)
        if self.other is not None:
            for half, near_link, far_link, near in self.sides():
                self.start(guard, half, 2 * z + near, 1, far_link, fresh)

    def cross(self, guard, z):
        for half, near_link, far_link, near in self.sides():
            at = 2 * z + 1 - near
            self.arrive(guard, half, at, 0)
            if self.other is not None:
                self.start(guard, half, at, 1, far_link)

    def keep(self, half):
        near = self.sides()[half][3]
        return pltpu.make_async_copy(self.src[half], self.own[half].at[2 * self.z + near], self.keep_sem.at[half])

    def first(self):
        for half in range(2):
            self.keep(half).start()
        for link in (0, 1):
            for half, _, _, near in self.sides():
                self.start(None, half, 2 * self.z + near, 0, link, True)
        self.enter(None, self.z, True)

    def hop(self, d):
        for side, onward in ((-1, 1), (1, 0)):
            z = self.z + side * d
            guard = z >= 0 if side < 0 else z < self.length
            for half, _, _, near in self.sides():
                self.arrive(guard, half, 2 * z + near, 0)
                self.start(guard, half, 2 * z + near, 0, onward)
            self.enter(guard, z)
        self.crossing(d - 1)

    def last(self):
        self.crossing(self.length - 1)
        if self.other is not None:
            for half in range(2):
                for at in range(2 * self.length):
                    self.arrive(None, half, at, 1)
        self.drain()
        for half in range(2):
            self.keep(half).wait()

    def crossing(self, d):
        if d == 0:
            self.cross(None, self.z)
        else:
            self.cross(self.z - d >= 0, self.z - d)
            self.cross(self.z + d < self.length, self.z + d)


def accumulate(dst, src):
    def add(d, s):
        d[...] = (d[...].astype(F32) + s[...].astype(F32)).astype(d.dtype)

    if len(dst.shape) == 2:
        add(dst, src)
        return

    def body(i, carry):
        add(dst.at[i], src.at[i])
        return carry

    lax.fori_loop(0, dst.shape[0], body, 0)


class Reduce(Place):
    def __init__(self, kept, sent, got, first, second, third, out, send, recv1, recv2, recv3, own=None, own_sem=None):
        super().__init__()
        self.kept, self.sent, self.got = kept, sent, got
        self.first, self.second, self.third, self.out = first, second, third, out
        self.send, self.recv1, self.recv2, self.recv3 = send, recv1, recv2, recv3
        self.own, self.own_sem = own, own_sem

    def target(self, k):
        picked = 0
        for z in range(self.length):
            order = sorted(range(self.length), key=lambda to: (-abs(to - z), to))
            picked = picked + jnp.where(self.z == z, order[k], 0)
        return picked

    def sides(self):
        return ((0, 3, 2, 1 - self.x, self.x), (1, 2, 3, 1 - self.y, self.y))

    def loads(self, half, z, q):
        at = 2 * z + q
        copies = []
        if self.own is not None:
            copies.append(
                pltpu.make_async_copy(self.kept(half, z, q), self.own.at[half, at], self.own_sem.at[half, at])
            )
        if self.got is not None:
            copies.append(
                pltpu.make_async_copy(self.got(half, z, q), self.first.at[half, at], self.recv1.at[half, at])
            )
        return copies

    def stage(self, k):
        z = self.target(k)
        for half, _, _, far, near in self.sides():
            for q in (far, near):
                for load in self.loads(half, z, q):
                    load.start()

    def one(self, k):
        z = self.target(k)
        for half, link, _, far, near in self.sides():
            for q in (far, near):
                self.post(
                    None, self.sent(half, z, q), self.first.at[half, 2 * z + q],
                    self.recv1.at[half, 2 * z + q], link,
                )

    def join(self, half, z, q):
        at = 2 * z + q
        if self.got is None:
            self.receive(None, self.first.at[half, at], self.recv1.at[half, at])
        for load in self.loads(half, z, q):
            load.wait()
        accumulate(self.first.at[half, at], self.kept(half, z, q) if self.own is None else self.own.at[half, at])

    def two(self, k):
        z = self.target(k)
        for half, _, link, far, near in self.sides():
            self.join(half, z, far)
            self.post(
                None, self.first.at[half, 2 * z + far], self.second.at[half, z], self.recv2.at[half, z], link
            )
        for half, _, link, far, near in self.sides():
            self.join(half, z, near)

    def three(self, k):
        z = self.target(k)
        left, right = self.z > 0, self.z < self.length - 1
        for half, _, _, _, near in self.sides():
            run_sum = self.second.at[half, z]
            self.receive(None, run_sum, self.recv2.at[half, z])
            accumulate(run_sum, self.first.at[half, 2 * z + near])
            for guard, more, link, at in (
                (z < self.z, right, 0, jnp.where(z == self.z - 1, self.length, z)),
                (z > self.z, left, 1, z),
            ):
                def take(half=half, run_sum=run_sum):
                    self.receive(None, self.third.at[half, z], self.recv3.at[half, z])
                    accumulate(run_sum, self.third.at[half, z])

                run(guard & more, take)
                self.post(guard, run_sum, self.third.at[half, at], self.recv3.at[half, at], link)

            def settle(half=half, run_sum=run_sum):
                out = self.out.at[half]
                out[...] = run_sum[...].astype(out.dtype)
                for guard, at in ((left, z), (right, self.length)):
                    def take(at=at):
                        self.receive(None, self.third.at[half, at], self.recv3.at[half, at])
                        accumulate(out, self.third.at[half, at])

                    run(guard, take)

            run(z == self.z, settle)


def reduce_sems(length):
    return [
        pltpu.SemaphoreType.DMA((10 * length,)),
        pltpu.SemaphoreType.DMA((2, 2 * length)),
        pltpu.SemaphoreType.DMA((2, length)),
        pltpu.SemaphoreType.DMA((2, length + 1)),
    ]


def reduce_room(length, block, dtype):
    return [pltpu.VMEM((2, n) + block, dtype) for n in (2 * length, length, length + 1)]


def both(a, b):
    if a is None or b is None:
        return b if a is None else a
    return a & b


def run(guard, body):
    if guard is None:
        body()
    else:
        pl.when(guard)(body)


def spread_sems(length, rels):
    return [
        pltpu.SemaphoreType.DMA((4 + 2 * rels + (length - 1) * (8 + 4 * rels) + (2 * length - 1) * 2 + 8,)),
        pltpu.SemaphoreType.DMA((2, rels, 2 * length)),
        pltpu.SemaphoreType.DMA((2,)),
    ]


class Parameters(Spread):
    def __init__(self, src, outs, own, other, own_s, other_s, table, send, recv, keep_sem, core_sem):
        halves = range(2)
        super().__init__(
            [src.at[h] for h in halves], [own.at[h] for h in halves], [other.at[h] for h in halves],
            send, recv, keep_sem,
        )
        self.outs, self.table = outs, table
        self.core = lax.axis_index("core")
        self.pairs = ((own, own_s), (other, other_s))
        self.core_sem = core_sem

    def across(self):
        return [
            remote(a, b, self.core_sem.at[0, i], self.core_sem.at[1, i], {"core": 1 - self.core})
            for i, (a, b) in enumerate(self.pairs)
        ]

    def place(self, core, parts, rel):
        part = self.table.shape[2] // (2 * self.chips)
        for z in range(self.length):
            for q in range(2):
                for half in range(2):
                    piece = parts[half, 2 * z + q].astype(F32)[:part]
                    x = q if half == 0 else (self.x if rel == 0 else 1 - self.x)
                    t = q if half == 1 else (self.y if rel == 0 else 1 - self.y)
                    at = pl.multiple_of(part * ((2 * z + x) * 2 + core), 8)
                    self.table[half, t, pl.ds(at, part), :] = piece

    def settle(self):
        wqkv_o, wout_o, par_o = self.outs
        for copy in self.across():
            copy.start()
        for rel in range(2):
            self.place(self.core, self.pairs[rel][0], rel)
        for copy in self.across():
            copy.wait()
        for rel in range(2):
            self.place(1 - self.core, self.pairs[rel][1], rel)
        width = wqkv_o.shape[0]
        wide = width // self.span
        pieces = [jnp.concatenate([self.table[0, t], self.table[1, t]], -1) for t in range(self.span)]
        for k in range(4):
            line = jnp.concatenate([p[:, wide * k : wide * (k + 1)] for p in pieces], -1).astype(BF16)
            if k < 3:
                wqkv_o[:, width * k : width * (k + 1)] = line
            else:
                wout_o[...] = line
        par_o[...] = pieces[0][:, 4 * wide : 4 * wide + 128].T[0:8]


def attention_forward(custom, tok, *refs):
    rows, width = tok.shape
    if custom:
        (
            small, shard, wqkv, wout, par, normed_o, hidden_o, packed_o, mixed_o, lse_o, normed_s, e0, e1, f0, f1, l0, l1,
            p_own, p_other, p_own_s, p_other_s, table, p_send, p_recv, p_keep, p_core,
            xs, e_send, e_recv, e_keep, l_send, l_recv, l_keep, core_sem,
        ) = refs
        params = Parameters(
            small, (wqkv, wout, par), p_own, p_other, p_own_s, p_other_s, table, p_send, p_recv, p_keep, p_core
        )
        early = Spread([shard.at[0], shard.at[1]], [e0, e1], [f0, f1], e_send, e_recv, e_keep)
        late = Spread([shard.at[2], shard.at[3]], [l0, l1], None, l_send, l_recv, l_keep)
        sibling = {"core": 1 - lax.axis_index("core")}
        early.greet(((None, sibling),))
        params.first()
        early.first()
        params.hop(1)
        late.first()
        params.hop(2)
        early.hop(1)
        params.hop(3)
        params.last()
        late.hop(1)
        params.settle()
    else:
        wqkv, wout, par, normed_o, hidden_o, packed_o, mixed_o, lse_o, xs = refs
    fill(xs, tok, rows)
    normed_o[rows // ALIGN * ALIGN :, :] = jnp.zeros((normed_o.shape[0] - rows // ALIGN * ALIGN, width), BF16)
    lane = lax.broadcasted_iota(jnp.int32, (1, 128), 1)
    low = lane < HEAD_DIM
    gain1, shift1, gain2, shift2 = (par[k : k + 1, :] for k in range(4))

    def image(i, carry):
        start, offset = window(i)
        valid, bias, keep = masks(offset)
        x = xs[pl.ds(start, WIN), :].astype(F32)
        scaled1, _ = standardize(x)
        normed1 = (scaled1 * gain1 + shift1).astype(BF16)
        packed = nn(normed1, wqkv[...]).astype(BF16)
        pieces = []
        lse = jnp.zeros((WIN, 128), F32)
        for pair in range(width // 128):
            at = 128 * pair
            q2 = packed[:, at : at + 128]
            k2 = packed[:, width + at : width + at + 128]
            v2 = packed[:, 2 * width + at : 2 * width + at + 128]
            halves = []
            for half in range(2):
                mine = low if half == 0 else ~low
                qm = jnp.where(mine, q2, jnp.zeros_like(q2)) * jnp.asarray(0.125, BF16)
                s = nt(qm, k2) + bias
                top = jnp.max(s, -1, keepdims=True)
                e = jnp.exp(s - top)
                total = jnp.sum(e, -1, keepdims=True)
                halves.append(nn(e.astype(BF16), v2) * (1.0 / total))
                lse = jnp.where(lane == 2 * pair + half, top + jnp.log(total), lse)
            pieces.append(jnp.where(low, halves[0], halves[1]).astype(BF16))
        mixed = jnp.concatenate(pieces, -1)
        hidden = x + nt(mixed, wout[...])
        scaled2, _ = standardize(hidden)
        put(normed_o, start, keep, (scaled2 * gain2 + shift2).astype(BF16))
        put(hidden_o, start, keep, hidden)
        put(packed_o, start, keep, packed)
        put(mixed_o, start, keep, mixed)
        put(lse_o, start, keep, lse)
        return carry

    images = rows // SEQ
    if not custom:
        lax.fori_loop(0, images, image, 0)
        return
    early.hop(2)
    late.hop(2)
    lax.fori_loop(0, 5, image, 0)
    early.hop(3)
    late.hop(3)
    lax.fori_loop(5, images, image, 0)
    across = remote(normed_o, normed_s, core_sem.at[0], core_sem.at[1], sibling)
    across.start()
    early.last()
    late.last()
    across.wait()


def attention_backward(custom, tok, cot, hidden_r, packed_r, mixed_r, lse_r, own, given, wqkv, wout, par, *refs):
    rows, width = tok.shape
    other = given
    if custom:
        (
            ek0, ek1, er0, er1, lk0, lk1, ls0, ls1,
            out_o, gtok_o, early_o, late_o, small_o, xs, cs, outs, gtoks, gqkv_o, gout_o, gpar_o, pile, theirs, others,
            *room,
        ) = refs
        core = lax.axis_index("core")
        sibling = {"core": 1 - core}
        (e_own, e1, e2, e3, l_own, l1, l2, l3, s1, s2, s3,
         e_send, e_r1, e_r2, e_r3, e_sem, l_send, l_r1, l_r2, l_r3, l_sem, s_send, s_r1, s_r2, s_r3, core_sem) = room
        ek, er, lk, ls = (ek0, ek1), (er0, er1), (lk0, lk1), (ls0, ls1)
        early = Reduce(
            lambda half, z, q: ek[half].at[2 * z + q], None, lambda half, z, q: er[half].at[2 * z + q],
            e1, e2, e3, early_o, e_send, e_r1, e_r2, e_r3, e_own, e_sem,
        )
        late = Reduce(
            lambda half, z, q: lk[half].at[2 * z + q], lambda half, z, q: ls[half].at[2 * z + q], None,
            l1, l2, l3, late_o, l_send, l_r1, l_r2, l_r3, l_own, l_sem,
        )
        def pile_at(half, z, x, y):
            return pile.at[core, late.slot(z, x, y), half]

        little = Reduce(
            lambda half, z, q: pile_at(half, z, q, late.y) if half == 0 else pile_at(half, z, late.x, q),
            lambda half, z, q: pile_at(half, z, q, 1 - late.y) if half == 0 else pile_at(half, z, 1 - late.x, q),
            None, s1, s2, s3, small_o, s_send, s_r1, s_r2, s_r3,
        )
        late.greet(((None, sibling),))
        ranks = range(late.length)
        middle = others.shape[0] // 2

        def rows_across(i):
            part = pl.ds(i * middle, middle)
            return remote(given.at[part], others.at[part], core_sem.at[0, i], core_sem.at[1, i], sibling)

        for i in range(2):
            rows_across(i).start()
        late.one(0)
        for k in ranks:
            early.stage(k)
            late.stage(k)
        early.two(0)
        late.one(1)
        early.two(1)
        other = others
        rows_across(0).wait()
    else:
        out_o, gtok_o, gqkv_o, gout_o, gpar_o, xs, cs, outs, gtoks = refs
    fill(xs, tok, rows)
    fill(cs, cot, rows)
    gqkv_o[...] = jnp.zeros_like(gqkv_o)
    gout_o[...] = jnp.zeros_like(gout_o)
    gpar_o[...] = jnp.zeros_like(gpar_o)
    lane = lax.broadcasted_iota(jnp.int32, (1, 128), 1)
    low = lane < HEAD_DIM
    gain1, shift1, gain2 = (par[k : k + 1, :] for k in range(3))
    eighth = jnp.asarray(0.125, BF16)

    def image(i, carry):
        start, offset = window(i)
        valid, bias, keep = masks(offset)
        here = pl.ds(start, WIN)
        hidden = hidden_r[here, :]
        put(
            outs, start, keep,
            (hidden + own[here, 0:width].astype(F32) + other[here, 0:width].astype(F32)).astype(BF16),
        )
        scaled2, inverse2 = standardize(hidden)
        g2 = own[here, width:].astype(F32) + other[here, width:].astype(F32)
        g2 = jnp.where(valid, g2, 0.0)
        gpar_o[2:3, :] += jnp.sum(g2 * scaled2, 0, keepdims=True)
        gpar_o[3:4, :] += jnp.sum(g2, 0, keepdims=True)
        ghid = cs[here, :].astype(F32) + norm_back(g2 * gain2, scaled2, inverse2)
        branch = jnp.where(valid, ghid, 0.0).astype(BF16)
        gout_o[...] += tn(branch, mixed_r[here, :])
        gmix = nn(branch, wout[...]).astype(BF16)
        gq, gk, gv = [], [], []
        for pair in range(width // 128):
            at = 128 * pair
            q2 = packed_r[here, at : at + 128]
            k2 = packed_r[here, width + at : width + at + 128]
            v2 = packed_r[here, 2 * width + at : 2 * width + at + 128]
            gm2 = gmix[:, at : at + 128]
            sums = [0.0, 0.0, 0.0]
            for half in range(2):
                mine = low if half == 0 else ~low
                qm = jnp.where(mine, q2, jnp.zeros_like(q2)) * eighth
                km = jnp.where(mine, k2, jnp.zeros_like(k2)) * eighth
                gm = jnp.where(mine, gm2, jnp.zeros_like(gm2))
                head = 2 * pair + half
                lse = jnp.where(valid, lse_r[here, head : head + 1], -NEG)
                p = jnp.exp(nt(qm, k2) + bias - lse)
                gp = nt(gm, v2)
                inner = jnp.sum(gp * p, -1, keepdims=True)
                gs = (p * (gp - inner)).astype(BF16)
                sums[0] += nn(gs, km)
                sums[1] += tn(gs, qm)
                sums[2] += tn(p.astype(BF16), gm)
            for store, total in zip((gq, gk, gv), sums):
                store.append(total.astype(BF16))
        gpacked = jnp.concatenate(gq + gk + gv, -1)
        scaled1, inverse1 = standardize(xs[here, :].astype(F32))
        normed1 = (scaled1 * gain1 + shift1).astype(BF16)
        gqkv_o[...] += tn(normed1, gpacked)
        g1 = nt(gpacked, wqkv[...])
        gpar_o[0:1, :] += jnp.sum(g1 * scaled1, 0, keepdims=True)
        gpar_o[1:2, :] += jnp.sum(g1, 0, keepdims=True)
        put(gtoks, start, keep, ghid + norm_back(g1 * gain1, scaled1, inverse1))
        return carry

    images = rows // SEQ

    def finish():
        out_o[...] = outs[0:rows, :]
        gtok_o[...] = gtoks[0:rows, :]

    if not custom:
        lax.fori_loop(0, images, image, 0)
        finish()
        return

    lax.fori_loop(0, 3, image, 0)
    rows_across(1).wait()
    late.two(0)
    late.one(2)
    early.two(2)
    early.three(0)
    lax.fori_loop(3, 6, image, 0)
    late.two(1)
    late.one(3)
    early.two(3)
    early.three(1)
    late.three(0)
    lax.fori_loop(6, 8, image, 0)
    late.two(2)
    early.three(2)
    lax.fori_loop(8, images, image, 0)
    span = late.span
    part, wide = width // (2 * late.chips), width // span
    vectors = gpar_o[...].T
    for t in range(span):
        table = jnp.concatenate(
            [gqkv_o[:, width * k + wide * t : width * k + wide * (t + 1)] for k in range(3)]
            + [gout_o[:, wide * t : wide * (t + 1)], vectors, jnp.zeros_like(vectors)],
            -1,
        )
        for group in range(2 * late.chips):
            for half in range(2):
                pile[group % 2, (group // 2) * span + t, half] = table[
                    part * group : part * (group + 1), 512 * half : 512 * (half + 1)
                ]

    def across():
        return remote(pile.at[1 - core], theirs, core_sem.at[0, 2], core_sem.at[1, 2], sibling)

    across().start()
    late.two(3)
    late.three(1)
    early.three(3)
    finish()
    across().wait()

    def merge(i, carry):
        accumulate(pile.at[core, i, 0], theirs.at[i, 0])
        accumulate(pile.at[core, i, 1], theirs.at[i, 1])
        return carry

    lax.fori_loop(0, theirs.shape[0], merge, 0)
    for k in ranks:
        little.one(k)
    late.three(2)
    for k in ranks:
        little.two(k)
    late.three(3)
    for k in ranks:
        little.three(k)
    early.drain()
    late.drain()
    little.drain()


def gelu_parts(v):
    e = jnp.exp(v * v * -0.5)
    t = 1.0 / (1.0 + jnp.abs(v) * (0.3275911 * 0.7071067811865476))
    q = 0.5 * 1.061405429
    for c in (-1.453152027, 1.421413741, -0.284496736, 0.254829592):
        q = q * t + 0.5 * c
    q = q * t * e
    return jnp.where(v < 0, q, 1.0 - q), e * INV_ROOT_TAU


def experts(row, prior, cnt, rown, rsib, cown, csib, town, tsib, *refs):
    if prior:
        pown_i, psib_i, *refs = refs
    else:
        pown_i = psib_i = None
    (
        own0, oth0, own1, oth1, pown, psib, k0, n0, k1, n1,
        xb, gb, tmpx, tmpg, acc1, acc2, wa, wb, fw, bk, off, dst, base, tot,
    ) = refs
    number = pl.num_programs(0)
    e_now = pl.program_id(0)
    depth = town.shape[2]
    width = rown.shape[1]

    def blocks(fn):
        for side, args in enumerate(((town, rown, cown, pown, pown_i), (tsib, rsib, csib, psib, psib_i))):
            def body(j, carry, side=side, args=args):
                fn(side * BLOCKS + j, args[0][j], *args[1:], pl.ds(pl.multiple_of(j * depth, ALIGN), depth))
                return carry

            lax.fori_loop(0, BLOCKS, body, 0)

    def onehot(table, at):
        slot = (lax.broadcasted_iota(jnp.int32, (STEP, 1), 0) + at).astype(F32)
        first = table[row : row + 1, :] == slot
        second = table[row + 1 : row + 2, :] == slot
        gate = jnp.where(first, table[2:3, :], jnp.where(second, table[3:4, :], 0.0))
        pick = jnp.where(first | second, 1.0, 0.0).astype(BF16)
        return pick, jnp.sum(gate, -1, keepdims=True)

    def padded(k):
        return (cnt[k] + (ALIGN - 1)) // ALIGN * ALIGN

    def steps(b):
        last = b * number + number - 1
        return (off[last] + padded(last) + (STEP - 1)) // STEP

    def segments(b, move):
        def per(e, carry):
            k = b * number + e
            o, d = off[k], dst[k]

            def tile(t, carry):
                move(
                    pl.ds(pl.multiple_of(o + t * ALIGN, ALIGN), ALIGN),
                    pl.ds(pl.multiple_of(d + t * ALIGN, ALIGN), ALIGN),
                )
                return carry

            return lax.fori_loop(0, padded(k) // ALIGN, tile, carry)

        lax.fori_loop(0, number, per, 0)

    @pl.when(e_now == 0)
    def _():
        def plan_expert(e, at):
            base[e] = at

            def plan_block(b, run):
                dst[b * number + e] = at + run
                return run + padded(b * number + e)

            total = lax.fori_loop(0, 2 * BLOCKS, plan_block, 0)
            tot[e] = total
            return at + (total + (CHUNK - 1)) // CHUNK * CHUNK

        lax.fori_loop(0, number, plan_expert, 0)

        def plan_off(b, carry):
            def one(e, run):
                off[b * number + e] = run
                return run + padded(b * number + e)

            lax.fori_loop(0, number, one, 0)
            return carry

        lax.fori_loop(0, 2 * BLOCKS, plan_off, 0)

        def dispatch(b, table, r, c, out, before, here):
            def some(k, carry):
                at = pl.multiple_of(k * STEP, ALIGN)
                pick, gate = onehot(table, at)
                tmpx[pl.ds(at, STEP), :] = nn(pick, r[here, :]).astype(BF16)
                tmpg[pl.ds(at, STEP), :] = (nn(pick, c[here, :]) * gate).astype(BF16)
                return carry

            lax.fori_loop(0, steps(b), some, 0)

            def move(local, far):
                xb[far, :] = tmpx[local, :]
                gb[far, :] = tmpg[local, :]

            segments(b, move)

        blocks(dispatch)

        def clear(e, carry):
            total = tot[e]
            end = base[e] + total

            def tile(t, carry):
                far = pl.ds(pl.multiple_of(end + t * ALIGN, ALIGN), ALIGN)
                xb[far, :] = jnp.zeros((ALIGN, width), BF16)
                gb[far, :] = jnp.zeros((ALIGN, width), BF16)
                return carry

            rest = (total + (CHUNK - 1)) // CHUNK * CHUNK - total
            return lax.fori_loop(0, rest // ALIGN, tile, carry)

        lax.fori_loop(0, number, clear, 0)

    shards, units = own0.shape[0], own0.shape[2] // 2
    middle = shards * units
    lower = e_now < number // 2

    def load(own, other):
        for i, ref in enumerate((own, other)):
            to = slice(i * middle, (i + 1) * middle)
            wa[to, :] = ref[:, 0, 0:units].reshape(middle, width)
            wb[to, :] = ref[:, 0, units:].reshape(middle, width)

    pl.when(lower)(lambda: load(own0, oth0))
    pl.when(~lower)(lambda: load(own1, oth1))
    acc1[...] = jnp.zeros_like(acc1)
    acc2[...] = jnp.zeros_like(acc2)

    def chunk(t, carry):
        here = pl.ds(pl.multiple_of(base[e_now] + t * CHUNK, ALIGN), CHUNK)
        first, second = wa[...], wb[...]
        x, g = xb[here, :], gb[here, :]
        v = nt(x, first)
        big, small = gelu_parts(v)
        act = (v * big).astype(BF16)
        gpre = (nt(g, second) * (big + v * small)).astype(BF16)
        acc1[...] += tn(gpre, x)
        acc2[...] += tn(act, g)
        xb[here, :] = nn(act, second).astype(BF16)
        gb[here, :] = nn(gpre, first).astype(BF16)
        return carry

    lax.fori_loop(0, (tot[e_now] + (CHUNK - 1)) // CHUNK, chunk, 0)

    def save(kept, sent):
        for i, ref in enumerate((kept, sent)):
            part = slice(i * middle, (i + 1) * middle)
            ref[:, 0, 0:units] = acc1[part, :].reshape(shards, units, width).astype(BF16)
            ref[:, 0, units:] = acc2[part, :].reshape(shards, units, width).astype(BF16)

    pl.when(lower)(lambda: save(k0, n0))
    pl.when(~lower)(lambda: save(k1, n1))

    @pl.when(e_now == number - 1)
    def _():
        def combine(b, table, r, c, out, before, here):
            def move(local, far):
                tmpx[local, :] = xb[far, :]
                tmpg[local, :] = gb[far, :]

            segments(b, move)
            if before is None:
                fw[...] = jnp.zeros_like(fw)
                bk[...] = jnp.zeros_like(bk)
            else:
                fw[...] = before[here, 0:width].astype(F32)
                bk[...] = before[here, width:].astype(F32)

            def some(k, carry):
                at = pl.multiple_of(k * STEP, ALIGN)
                pick, gate = onehot(table, at)
                fw[...] += tn(pick, (tmpx[pl.ds(at, STEP), :].astype(F32) * gate).astype(BF16))
                bk[...] += tn(pick, tmpg[pl.ds(at, STEP), :])
                return carry

            lax.fori_loop(0, steps(b), some, 0)
            out[here, 0:width] = fw[...].astype(BF16)
            out[here, width:] = bk[...].astype(BF16)

        blocks(combine)


def run_experts(late, tables, counts, row_refs, weights, prior):
    padded, width = row_refs[0].shape
    number, n_blocks = 2 * weights[0].shape[1], 2 * BLOCKS
    depth = padded // BLOCKS
    pairs = 4 * padded
    room = -(-(pairs + n_blocks * number * (ALIGN - 1) + number * (CHUNK - ALIGN)) // CHUNK) * CHUNK
    slots = -(-(2 * depth + number * (ALIGN - 1)) // STEP) * STEP
    shards, _, lines, _ = weights[0].shape
    held = shards * lines

    def full(*shape):
        return pl.BlockSpec(shape, lambda e, *_: (0,) * len(shape), pipeline_mode=pl.Buffered(1))

    block = (shards, 1, lines, width)
    lower = pl.BlockSpec(block, lambda e, *_: (0, jnp.minimum(e, number // 2 - 1), 0, 0))
    upper = pl.BlockSpec(block, lambda e, *_: (0, jnp.maximum(e - number // 2, 0), 0, 0))
    sums = full(padded, 2 * width)
    grad = whole(weights[0].shape, BF16)
    return pl.pallas_call(
        functools.partial(experts, 5 if late else 0, prior is not None),
        out_shape=(whole((padded, 2 * width), BF16),) * 2 + (grad,) * 4,
        grid_spec=pltpu.PrefetchScalarGridSpec(
            num_scalar_prefetch=1,
            grid=(number,),
            in_specs=[full(padded, width)] * 4
            + [full(*tables[0].shape)] * 2
            + [sums] * (0 if prior is None else 2)
            + [lower, lower, upper, upper],
            out_specs=(sums, sums, lower, lower, upper, upper),
            scratch_shapes=[
                pltpu.VMEM((room, width), BF16),
                pltpu.VMEM((room, width), BF16),
                pltpu.VMEM((slots, width), BF16),
                pltpu.VMEM((slots, width), BF16),
                pltpu.VMEM((held, width), F32),
                pltpu.VMEM((held, width), F32),
                pltpu.VMEM((held, width), BF16),
                pltpu.VMEM((held, width), BF16),
                pltpu.VMEM((depth, width), F32),
                pltpu.VMEM((depth, width), F32),
                pltpu.SMEM((n_blocks * number,), jnp.int32),
                pltpu.SMEM((n_blocks * number,), jnp.int32),
                pltpu.SMEM((number,), jnp.int32),
                pltpu.SMEM((number,), jnp.int32),
            ],
        ),
        compiler_params=pltpu.CompilerParams(
            vmem_limit_bytes=VMEM_LIMIT, dimension_semantics=("arbitrary",)
        ),
        cost_estimate=pl.CostEstimate(flops=25 * 10**9, bytes_accessed=20 * 10**6, transcendentals=6 * 10**6),
        name="experts_late" if late else "experts_early",
    )(counts, *row_refs, *tables, *(() if prior is None else prior), *weights)


def route(ids, gates, number, padded):
    rows = ids.shape[1]
    depth = padded // BLOCKS
    ids = jnp.pad(ids, ((0, 0), (0, padded - rows)), constant_values=-1)
    gates = jnp.pad(gates, ((0, 0), (0, padded - rows)))
    ids = ids.reshape(2, BLOCKS, 1, depth)
    gates = gates.reshape(2, BLOCKS, 1, depth)
    listed = jnp.arange(number, dtype=jnp.int32)
    match = ids == listed[None, None, :, None]
    named = (match[0] | match[1]).astype(BF16)
    order = jnp.arange(depth)
    earlier = (order[:, None] < order[None, :]).astype(BF16)
    rank = jnp.einsum("ber,rs->bes", named, earlier, preferred_element_type=F32)
    count = jnp.sum(named.astype(F32), -1)
    room = jnp.ceil(count * (1.0 / ALIGN)) * ALIGN
    middle = number // 2
    ahead = (listed[:, None] < listed[None, :]) & (listed[:, None] // middle == listed[None, :] // middle)
    off = jnp.sum(jnp.where(ahead[None], room[:, :, None], 0.0), 1)
    place = off[:, :, None] + rank
    slot = jnp.sum(jnp.where(match, place[None], 0.0), 2)
    flat = ids[:, :, 0]
    first = jnp.where((flat >= 0) & (flat < middle), slot, -1.0)
    second = jnp.where(flat >= middle, slot, -1.0)
    lanes = jnp.pad(count, ((0, 0), (0, depth - number)))
    return jnp.stack(
        [first[0], first[1], gates[0, :, 0], gates[1, :, 0], lanes, second[0], second[1], jnp.zeros_like(lanes)], 1
    )


def whole(shape, dtype):
    return jax.ShapeDtypeStruct(shape, dtype)


IN_VMEM = pl.BlockSpec(memory_space=pltpu.VMEM)
ANYWHERE = pl.BlockSpec(memory_space=pl.ANY)


def on_device(
    tokens, query_key_value, attention_out, first_gain, first_shift, second_gain, second_shift,
    expert_in, expert_out, expert_ids, gate_weights, cotangent,
):
    rows, width = tokens.shape
    padded = -(-rows // (ALIGN * BLOCKS)) * (ALIGN * BLOCKS)
    number = expert_in.shape[0]
    groups, span = lax.axis_size(DP), lax.axis_size("tensor")
    part = width // groups
    wide = width // span
    side = lax.axis_index("tensor")
    chips = groups // 2
    length = chips // 2
    custom = chips == 8 and span == 2 and part % 8 == 0
    vectors = jnp.stack([first_gain, first_shift, second_gain, second_shift], 1)
    small = jnp.concatenate(
        [
            query_key_value.reshape(part, 3 * wide),
            attention_out.T,
            jnp.pad(vectors, ((0, 0), (0, 1024 - 4 * wide - 4))),
        ],
        1,
    )
    shard = jnp.concatenate([expert_in.transpose(0, 2, 1), expert_out], 1)
    units = shard.shape[1] // 2
    if custom:
        lines = -(-part // ALIGN) * ALIGN
        small = jnp.pad(small, ((0, lines - part), (0, 0))).reshape(lines, 2, 512).transpose(1, 0, 2)
    else:
        gathered = lax.all_gather(small, ALL, axis=0, tiled=False).reshape(groups, span, part, 1024)
        taken = gathered[..., : 4 * wide].reshape(groups, span, part, 4, wide)
        taken = taken.transpose(0, 2, 3, 1, 4).reshape(width, 4, width)
        wqkv, wout = taken[:, :3].reshape(width, 3 * width), taken[:, 3]
        par = gathered[:, 0, :, 4 * wide : 4 * wide + 8].reshape(width, 8).T.astype(F32)

    ids = lax.dynamic_slice_in_dim(expert_ids.T, side * rows, rows, 1)
    gates = lax.dynamic_slice_in_dim(gate_weights.T, side * rows, rows, 1)
    table = route(ids, gates, number, padded)
    table_sib = lax.ppermute(table, "core", SWAP)
    cot_own = jnp.pad(cotangent, ((0, padded - rows), (0, 0)))
    cot_sib = lax.ppermute(cot_own, "core", SWAP)

    row_shapes = (
        whole((padded, width), BF16),
        whole((padded, width), F32),
        whole((padded, 3 * width), BF16),
        whole((padded, width), BF16),
        whole((padded, 128), F32),
    )
    estimate = pl.CostEstimate(flops=6 * 10**9, bytes_accessed=14 * 10**6, transcendentals=3 * 10**6)
    xs_scratch = [pltpu.VMEM((padded, width), BF16)]
    quarter = number // 4
    if custom:
        held = whole((2 * length, quarter, 2 * units, width), BF16)
        wqkv, wout, par, normed, hidden, packed, mixed, lse, normed_sib, e0, e1, f0, f1, l0, l1 = pl.pallas_call(
            functools.partial(attention_forward, True),
            out_shape=(whole((width, 3 * width), BF16), whole((width, width), BF16), whole((8, width), F32))
            + row_shapes
            + (row_shapes[0],)
            + (held,) * 6,
            in_specs=[IN_VMEM] * 3,
            out_specs=(IN_VMEM,) * 9 + (ANYWHERE,) * 6,
            scratch_shapes=[pltpu.VMEM((2, 2 * length, lines, 512), BF16)] * 4
            + [pltpu.VMEM((2, span, width, 512), F32)]
            + spread_sems(length, 2)
            + [pltpu.SemaphoreType.DMA((2, 2))]
            + xs_scratch
            + spread_sems(length, 2)
            + spread_sems(length, 1)
            + [pltpu.SemaphoreType.DMA((2,))],
            compiler_params=pltpu.CompilerParams(vmem_limit_bytes=VMEM_LIMIT, collective_id=1, has_side_effects=True),
            cost_estimate=estimate,
            name="attention_forward",
        )(tokens, small, shard.reshape(4, quarter, 2 * units, width))
        across_y = functools.partial(lax.ppermute, axis_name="tensor", perm=SWAP)
        across_x = functools.partial(lax.ppermute, axis_name="chip", perm=[(c, c ^ 1) for c in range(chips)])
        early_weights = (e0, f0, e1, f1)
        late_weights = (l0, across_y(l0), l1, across_x(l1))
    else:
        normed, hidden, packed, mixed, lse = pl.pallas_call(
            functools.partial(attention_forward, False),
            out_shape=row_shapes,
            in_specs=[IN_VMEM] * 4,
            out_specs=(IN_VMEM,) * 5,
            scratch_shapes=xs_scratch,
            compiler_params=pltpu.CompilerParams(vmem_limit_bytes=VMEM_LIMIT),
            cost_estimate=estimate,
            name="attention_forward",
        )(tokens, wqkv, wout, par)
        normed_sib = lax.ppermute(normed, "core", SWAP)
        weights = lax.all_gather(shard, RING, axis=0, tiled=False)
        shards = weights.shape[0]
        weights = weights.reshape(2, shards // 2, 4, quarter, 2, units, width).transpose(2, 0, 3, 4, 1, 5, 6)
        weights = weights.reshape(4, 2, 1, quarter, shards * units, width)
        early_weights = tuple(weights[i, j] for i in (0, 1) for j in (0, 1))
        late_weights = tuple(weights[i, j] for i in (2, 3) for j in (0, 1))

    middle = number // 2
    both_counts = jnp.concatenate([table[:, 4, :number], table_sib[:, 4, :number]], 0).astype(jnp.int32)
    row_refs = (normed, normed_sib, cot_own, cot_sib)
    tables = (table, table_sib)
    own1, sib1, *early = run_experts(
        False, tables, both_counts[:, :middle].reshape(-1), row_refs, early_weights, None
    )
    if custom:
        got = (across_y(early[1]), across_x(early[3]))
    part_own, part_sib, *late = run_experts(
        True, tables, both_counts[:, middle:].reshape(-1), row_refs, late_weights, (own1, sib1)
    )

    sums = [
        pltpu.VMEM((width, 3 * width), F32),
        pltpu.VMEM((width, width), F32),
        pltpu.VMEM((128, width), F32),
    ]
    rows_scratch = [
        pltpu.VMEM((padded, width), BF16),
        pltpu.VMEM((padded, width), BF16),
        pltpu.VMEM((padded, width), BF16),
        pltpu.VMEM((padded, width), F32),
    ]
    saved = (tokens, cotangent, hidden, packed, mixed, lse, part_own)
    shapes = (whole((rows, width), BF16), whole((rows, width), F32))
    estimate = pl.CostEstimate(flops=15 * 10**9, bytes_accessed=25 * 10**6, transcendentals=3 * 10**6)
    if custom:
        block, tile = (quarter, 2 * units, width), (part, 512)
        output, grad_tokens, early_grad, late_grad, mine = pl.pallas_call(
            functools.partial(attention_backward, True),
            out_shape=shapes + (whole((2,) + block, F32),) * 2 + (whole((2,) + tile, F32),),
            in_specs=[IN_VMEM] * 7 + [ANYWHERE] + [IN_VMEM] * 3 + [ANYWHERE] * 8,
            out_specs=(IN_VMEM,) * 5,
            scratch_shapes=rows_scratch
            + sums
            + [pltpu.VMEM((2, 2 * chips, 2) + tile, F32), pltpu.VMEM((2 * chips, 2) + tile, F32)]
            + [pltpu.VMEM((padded, 2 * width), BF16)]
            + ([pltpu.VMEM((2, 2 * length) + block, BF16)] + reduce_room(length, block, BF16)) * 2
            + reduce_room(length, tile, F32)
            + (reduce_sems(length) + [pltpu.SemaphoreType.DMA((2, 2 * length))]) * 2
            + reduce_sems(length)
            + [pltpu.SemaphoreType.DMA((2, 3))],
            compiler_params=pltpu.CompilerParams(
                vmem_limit_bytes=VMEM_LIMIT, collective_id=2, has_side_effects=True
            ),
            cost_estimate=estimate,
            name="attention_backward",
        )(*saved, part_sib, wqkv, wout, par, early[0], early[2], *got, late[0], late[2], late[1], late[3])
        mine = mine.transpose(1, 0, 2).reshape(part, 1024)
        grad_shard = jnp.concatenate([early_grad, late_grad], 0).reshape(number, 2 * units, width)
    else:
        part_other = lax.ppermute(part_sib, "core", SWAP)
        output, grad_tokens, gqkv, gout, gpar = pl.pallas_call(
            functools.partial(attention_backward, False),
            out_shape=shapes + tuple(whole(ref.shape, F32) for ref in sums),
            in_specs=[IN_VMEM] * 11,
            out_specs=(IN_VMEM,) * 5,
            scratch_shapes=rows_scratch,
            compiler_params=pltpu.CompilerParams(vmem_limit_bytes=VMEM_LIMIT),
            cost_estimate=estimate,
            name="attention_backward",
        )(*saved, part_other, wqkv, wout, par)
        grads = jnp.stack(early + late).reshape(4, 2, quarter, 2, shards // 2, units, width)
        grads = grads.transpose(1, 4, 0, 2, 3, 5, 6).reshape(shards, number, 2 * units, width)
        grad_shard = lax.psum_scatter(grads, RING, scatter_dimension=0, tiled=False).astype(F32)
        owed = jnp.concatenate([gqkv.reshape(width, 3, width), gout[:, None]], 1)
        owed = owed.reshape(groups, part, 4, span, wide).transpose(0, 3, 1, 2, 4)
        owed = owed.reshape(groups, span, part, 4 * wide)
        own_vectors = jnp.broadcast_to(gpar[:8].T.reshape(groups, 1, part, 8), (groups, span, part, 8))
        owed = jnp.concatenate([owed, own_vectors], -1).reshape(groups * span, part, 4 * wide + 8)
        mine = lax.psum_scatter(owed, ALL, scatter_dimension=0, tiled=False)
    vectors = mine[:, 4 * wide : 4 * wide + 4]
    return (
        output,
        grad_tokens,
        mine[:, : 3 * wide].reshape(part, 3, wide),
        mine[:, 3 * wide : 4 * wide].T,
        vectors[:, 0],
        vectors[:, 1],
        vectors[:, 2],
        vectors[:, 3],
        grad_shard[:, :units].transpose(0, 2, 1),
        grad_shard[:, units:],
    )


def solution(mesh):
    groups, span = mesh.devices.shape
    split = Mesh(mesh.devices.reshape(groups // 2, 2, span), ALL)
    return jax.shard_map(
        on_device,
        mesh=split,
        in_specs=(
            P(ALL, None),
            P(DP, None, "tensor"),
            P("tensor", DP),
            P(DP),
            P(DP),
            P(DP),
            P(DP),
            P(None, None, ALL),
            P(None, ALL, None),
            P(DP, None),
            P(DP, None),
            P(ALL, None),
        ),
        out_specs=(
            P(ALL, None),
            P(ALL, None),
            P(DP, None, "tensor"),
            P("tensor", DP),
            P(DP),
            P(DP),
            P(DP),
            P(DP),
            P(None, None, ALL),
            P(None, ALL, None),
        ),
        check_vma=False,
    )
```

```python
import functools

import jax
import jax.numpy as jnp
from jax import lax
from jax.experimental import pallas as pl
from jax.experimental.pallas import tpu as pltpu
from jax.sharding import Mesh
from jax.sharding import PartitionSpec as P

HEAD_DIM = 64
SEQ = 197
EPSILON = 1e-06
ALIGN = 16
WIN = 224
CHUNK = 384
BLOCKS = 4
STEP = 576
NEG = -1e30
F32 = jnp.float32
BF16 = jnp.bfloat16
INV_ROOT_TAU = 0.3989422804014327
ALL = ("chip", "core", "tensor")
DP = ("chip", "core")
RING = ("chip", "tensor")
SWAP = [(0, 1), (1, 0)]
VMEM_LIMIT = 60 * 1024 * 1024


def nn(a, b):
    return lax.dot_general(a, b, (((1,), (0,)), ((), ())), preferred_element_type=F32)


def nt(a, b):
    return lax.dot_general(a, b, (((1,), (1,)), ((), ())), preferred_element_type=F32)


def tn(a, b):
    return lax.dot_general(a, b, (((0,), (0,)), ((), ())), preferred_element_type=F32)


def standardize(matrix):
    centre = matrix - jnp.mean(matrix, -1, keepdims=True)
    variance = jnp.mean(centre * centre, -1, keepdims=True)
    inverse = lax.rsqrt(variance + EPSILON)
    return centre * inverse, inverse


def norm_back(weighted, scaled, inverse):
    return inverse * (
        weighted
        - jnp.mean(weighted, -1, keepdims=True)
        - scaled * jnp.mean(weighted * scaled, -1, keepdims=True)
    )


def window(i):
    first = i * SEQ
    start = pl.multiple_of((first // ALIGN) * ALIGN, ALIGN)
    return start, first - start


def put(ref, start, keep, value):
    head = pl.ds(start, ALIGN)
    ref[head, :] = jnp.where(keep, value[:ALIGN], ref[head, :])
    ref[pl.ds(start + ALIGN, WIN - ALIGN), :] = value[ALIGN:]


def fill(dst, src, rows):
    whole_rows = rows // ALIGN * ALIGN
    dst[whole_rows:, :] = jnp.zeros((dst.shape[0] - whole_rows, dst.shape[1]), dst.dtype)
    dst[0:rows, :] = src[...]


def masks(offset):
    row = lax.broadcasted_iota(jnp.int32, (WIN, 1), 0)
    col = lax.broadcasted_iota(jnp.int32, (1, WIN), 1)
    valid = (row >= offset) & (row < offset + SEQ)
    bias = jnp.where((col >= offset) & (col < offset + SEQ), 0.0, NEG).astype(F32)
    keep = lax.broadcasted_iota(jnp.int32, (ALIGN, 1), 0) >= offset
    return valid, bias, keep


class Place:
    def __init__(self):
        self.chips, self.span = lax.axis_size("chip"), lax.axis_size("tensor")
        self.length = self.chips // 2
        chip = lax.axis_index("chip")
        self.z, self.x, self.y = chip // 2, chip % 2, lax.axis_index("tensor")
        self.sends = []

    def slot(self, z, x, y):
        return (z * 2 + x) * self.span + y

    def links(self):
        return (
            (self.z > 0, {"chip": (self.z - 1) * 2 + self.x}),
            (self.z < self.length - 1, {"chip": (self.z + 1) * 2 + self.x}),
            (None, {"chip": self.z * 2 + 1 - self.x}),
            (None, {"tensor": 1 - self.y}),
        )

    def greet(self, extra=()):
        barrier = pltpu.get_barrier_semaphore()
        for guard, device in self.links() + tuple(extra):
            run(guard, lambda device=device: pl.semaphore_signal(
                barrier, inc=1, device_id=device, device_id_type=pl.DeviceIdType.MESH))
        edge = jnp.where(self.z > 0, 1, 0) + jnp.where(self.z < self.length - 1, 1, 0)
        pl.semaphore_wait(barrier, 2 + len(extra) + edge)

    def post(self, build, link):
        index = len(self.sends)

        def act(what):
            guard, src, dst, recv_sem = build()
            edge, device = self.links()[link]
            run(both(guard, edge), lambda: what(remote(src, dst, self.send.at[index], recv_sem, device)))

        self.sends.append(act)
        act(lambda copy: copy.start())

    def receive(self, guard, dst, recv_sem):
        run(guard, lambda: remote(dst, dst, self.send.at[0], recv_sem, self.links()[2][1]).wait_recv())

    def drain(self):
        for act in self.sends:
            act(lambda copy: copy.wait_send())


def remote(src, dst, send_sem, recv_sem, device):
    return pltpu.make_async_remote_copy(
        src_ref=src, dst_ref=dst, send_sem=send_sem, recv_sem=recv_sem,
        device_id=device, device_id_type=pl.DeviceIdType.MESH,
    )


class Spread(Place):
    def __init__(self, src, own, other, send, recv, keep_sem):
        super().__init__()
        self.src, self.own, self.other = src, own, other
        self.send, self.recv, self.keep_sem = send, recv, keep_sem
        self.sides = ((0, 2, 3, self.x, 1 - self.x), (1, 3, 2, self.y, 1 - self.y))
        self.places = {
            (side, d): self.z + side * d for side in (-1, 1) for d in range(1, self.length)
        }

    def there(self, side, z):
        return (lambda: z >= 0) if side < 0 else (lambda: z < self.length)

    def start(self, guard, half, z, q, rel, link, fresh=False):
        def build():
            at = 2 * z + q
            src = self.src[half] if fresh else self.own[half].at[at]
            return guard and guard(), src, (self.own, self.other)[rel][half].at[at], self.recv.at[half, rel, at]

        self.post(build, link)

    def arrive(self, guard, half, at, rel):
        self.receive(guard, (self.own, self.other)[rel][half].at[at], self.recv.at[half, rel, at])

    def enter(self, guard, z, fresh=False):
        for half, near_link, far_link, near, _ in self.sides:
            self.start(guard, half, z, near, 0, near_link, fresh)
        if self.other is not None:
            for half, near_link, far_link, near, _ in self.sides:
                self.start(guard, half, z, near, 1, far_link, fresh)

    def cross(self, guard, z):
        for half, near_link, far_link, _, far in self.sides:
            self.arrive(guard and guard(), half, 2 * z + far, 0)
            if self.other is not None:
                self.start(guard, half, z, far, 1, far_link)

    def keep(self, half):
        near = self.sides[half][3]
        return pltpu.make_async_copy(self.src[half], self.own[half].at[2 * self.z + near], self.keep_sem.at[half])

    def first(self):
        for half in range(2):
            self.keep(half).start()
        for link in (0, 1):
            for half, _, _, near, _ in self.sides:
                self.start(None, half, self.z, near, 0, link, True)
        self.enter(None, self.z, True)

    def hop(self, d):
        for side, onward in ((-1, 1), (1, 0)):
            z = self.places[side, d]
            guard = self.there(side, z)
            for half, _, _, near, _ in self.sides:
                self.arrive(guard(), half, 2 * z + near, 0)
                self.start(guard, half, z, near, 0, onward)
            self.enter(guard, z)
        self.crossing(d - 1)

    def last(self):
        self.crossing(self.length - 1)
        if self.other is not None:
            for half in range(2):
                for at in range(2 * self.length):
                    self.arrive(None, half, at, 1)
        self.drain()
        for half in range(2):
            self.keep(half).wait()

    def crossing(self, d):
        if d == 0:
            self.cross(None, self.z)
        else:
            for side in (-1, 1):
                z = self.places[side, d]
                self.cross(self.there(side, z), z)


def accumulate(dst, src):
    def add(d, s):
        d[...] = (d[...].astype(F32) + s[...].astype(F32)).astype(d.dtype)

    if len(dst.shape) == 2:
        add(dst, src)
        return

    def body(i, carry):
        add(dst.at[i], src.at[i])
        return carry

    lax.fori_loop(0, dst.shape[0], body, 0)


class Reduce(Place):
    def __init__(self, kept, sent, got, first, second, third, out, send, recv1, recv2, recv3, own=None, own_sem=None):
        super().__init__()
        self.kept, self.sent, self.got = kept, sent, got
        self.first, self.second, self.third, self.out = first, second, third, out
        self.send, self.recv1, self.recv2, self.recv3 = send, recv1, recv2, recv3
        self.own, self.own_sem = own, own_sem
        self.sides = ((0, 3, 2, 1 - self.x, self.x), (1, 2, 3, 1 - self.y, self.y))
        self.targets = [self.farthest(k) for k in range(self.length)]

    def farthest(self, k):
        picked = 0
        for z in range(self.length):
            order = sorted(range(self.length), key=lambda to: (-abs(to - z), to))
            picked = picked + jnp.where(self.z == z, order[k], 0)
        return picked

    def loads(self, half, z, q):
        at = 2 * z + q
        copies = []
        if self.own is not None:
            copies.append(
                pltpu.make_async_copy(self.kept(half, z, q), self.own.at[half, at], self.own_sem.at[half, at])
            )
        if self.got is not None:
            copies.append(
                pltpu.make_async_copy(self.got(half, z, q), self.first.at[half, at], self.recv1.at[half, at])
            )
        return copies

    def stage(self, k):
        z = self.targets[k]
        for half, _, _, far, near in self.sides:
            for q in (far, near):
                for load in self.loads(half, z, q):
                    load.start()

    def one(self, k):
        z = self.targets[k]
        for half, link, _, far, near in self.sides:
            for q in (far, near):
                self.post(
                    lambda half=half, q=q: (
                        None, self.sent(half, z, q), self.first.at[half, 2 * z + q], self.recv1.at[half, 2 * z + q]
                    ),
                    link,
                )

    def join(self, half, z, q):
        at = 2 * z + q
        if self.got is None:
            self.receive(None, self.first.at[half, at], self.recv1.at[half, at])
        for load in self.loads(half, z, q):
            load.wait()
        accumulate(self.first.at[half, at], self.kept(half, z, q) if self.own is None else self.own.at[half, at])

    def two(self, k):
        z = self.targets[k]
        for half, _, link, far, near in self.sides:
            self.join(half, z, far)
            self.post(
                lambda half=half, far=far: (
                    None, self.first.at[half, 2 * z + far], self.second.at[half, z], self.recv2.at[half, z]
                ),
                link,
            )
        for half, _, link, far, near in self.sides:
            self.join(half, z, near)

    def three(self, k):
        z = self.targets[k]
        left, right = self.z > 0, self.z < self.length - 1
        for half, _, _, _, near in self.sides:
            run_sum = self.second.at[half, z]
            self.receive(None, run_sum, self.recv2.at[half, z])
            accumulate(run_sum, self.first.at[half, 2 * z + near])
            for guard, more, link in (
                (lambda: z < self.z, right, 0),
                (lambda: z > self.z, left, 1),
            ):
                def take(half=half, run_sum=run_sum):
                    self.receive(None, self.third.at[half, z], self.recv3.at[half, z])
                    accumulate(run_sum, self.third.at[half, z])

                run(guard() & more, take)

                def build(half=half, guard=guard, link=link):
                    at = jnp.where(z == self.z - 1, self.length, z) if link == 0 else z
                    return guard(), self.second.at[half, z], self.third.at[half, at], self.recv3.at[half, at]

                self.post(build, link)

            def settle(half=half, run_sum=run_sum):
                out = self.out.at[half]
                out[...] = run_sum[...].astype(out.dtype)
                for guard, at in ((left, z), (right, self.length)):
                    def take(at=at):
                        self.receive(None, self.third.at[half, at], self.recv3.at[half, at])
                        accumulate(out, self.third.at[half, at])

                    run(guard, take)

            run(z == self.z, settle)


def reduce_sems(length):
    return [
        pltpu.SemaphoreType.DMA((10 * length,)),
        pltpu.SemaphoreType.DMA((2, 2 * length)),
        pltpu.SemaphoreType.DMA((2, length)),
        pltpu.SemaphoreType.DMA((2, length + 1)),
    ]


def reduce_room(length, block, dtype):
    return [pltpu.VMEM((2, n) + block, dtype) for n in (2 * length, length, length + 1)]


def both(a, b):
    if a is None or b is None:
        return b if a is None else a
    return a & b


def run(guard, body):
    if guard is None:
        body()
    else:
        pl.when(guard)(body)


def spread_sems(length, rels):
    return [
        pltpu.SemaphoreType.DMA((4 + 2 * rels + (length - 1) * (8 + 4 * rels) + (2 * length - 1) * 2 + 8,)),
        pltpu.SemaphoreType.DMA((2, rels, 2 * length)),
        pltpu.SemaphoreType.DMA((2,)),
    ]


class Parameters(Spread):
    def __init__(self, src, outs, own, other, own_s, other_s, table, send, recv, keep_sem, core_sem):
        halves = range(2)
        super().__init__(
            [src.at[h] for h in halves], [own.at[h] for h in halves], [other.at[h] for h in halves],
            send, recv, keep_sem,
        )
        self.outs, self.table = outs, table
        self.core = lax.axis_index("core")
        self.pairs = ((own, own_s), (other, other_s))
        self.core_sem = core_sem

    def across(self):
        return [
            remote(a, b, self.core_sem.at[0, i], self.core_sem.at[1, i], {"core": 1 - self.core})
            for i, (a, b) in enumerate(self.pairs)
        ]

    def place(self, core, parts, rel):
        part = self.table.shape[2] // (2 * self.chips)
        for z in range(self.length):
            for q in range(2):
                for half in range(2):
                    piece = parts[half, 2 * z + q].astype(F32)[:part]
                    x = q if half == 0 else (self.x if rel == 0 else 1 - self.x)
                    t = q if half == 1 else (self.y if rel == 0 else 1 - self.y)
                    at = pl.multiple_of(part * ((2 * z + x) * 2 + core), 8)
                    self.table[half, t, pl.ds(at, part), :] = piece

    def settle(self):
        wqkv_o, wout_o, par_o = self.outs
        for copy in self.across():
            copy.start()
        for rel in range(2):
            self.place(self.core, self.pairs[rel][0], rel)
        for copy in self.across():
            copy.wait()
        for rel in range(2):
            self.place(1 - self.core, self.pairs[rel][1], rel)
        width = wqkv_o.shape[0]
        wide = width // self.span
        pieces = [jnp.concatenate([self.table[0, t], self.table[1, t]], -1) for t in range(self.span)]
        for k in range(4):
            line = jnp.concatenate([p[:, wide * k : wide * (k + 1)] for p in pieces], -1).astype(BF16)
            if k < 3:
                wqkv_o[:, width * k : width * (k + 1)] = line
            else:
                wout_o[...] = line
        par_o[...] = pieces[0][:, 4 * wide : 4 * wide + 128].T[0:8]


def attention_forward(custom, tok, *refs):
    rows, width = tok.shape
    if custom:
        (
            small, shard, wqkv, wout, par, normed_o, hidden_o, packed_o, mixed_o, lse_o, normed_s, e0, e1, f0, f1, l0, l1,
            p_own, p_other, p_own_s, p_other_s, table, p_send, p_recv, p_keep, p_core,
            xs, e_send, e_recv, e_keep, l_send, l_recv, l_keep, core_sem,
        ) = refs
        params = Parameters(
            small, (wqkv, wout, par), p_own, p_other, p_own_s, p_other_s, table, p_send, p_recv, p_keep, p_core
        )
        early = Spread([shard.at[0], shard.at[1]], [e0, e1], [f0, f1], e_send, e_recv, e_keep)
        late = Spread([shard.at[2], shard.at[3]], [l0, l1], None, l_send, l_recv, l_keep)
        sibling = {"core": 1 - lax.axis_index("core")}
        early.greet(((None, sibling),))
        params.first()
        early.first()
        params.hop(1)
        late.first()
        params.hop(2)
        early.hop(1)
        params.hop(3)
        params.last()
        late.hop(1)
        params.settle()
    else:
        wqkv, wout, par, normed_o, hidden_o, packed_o, mixed_o, lse_o, xs = refs
    fill(xs, tok, rows)
    normed_o[rows // ALIGN * ALIGN :, :] = jnp.zeros((normed_o.shape[0] - rows // ALIGN * ALIGN, width), BF16)
    lane = lax.broadcasted_iota(jnp.int32, (1, 128), 1)
    low = lane < HEAD_DIM
    gain1, shift1, gain2, shift2 = (par[k : k + 1, :] for k in range(4))

    def image(i, carry):
        start, offset = window(i)
        valid, bias, keep = masks(offset)
        x = xs[pl.ds(start, WIN), :].astype(F32)
        scaled1, _ = standardize(x)
        normed1 = (scaled1 * gain1 + shift1).astype(BF16)
        packed = nn(normed1, wqkv[...]).astype(BF16)
        pieces = []
        lse = jnp.zeros((WIN, 128), F32)
        for pair in range(width // 128):
            at = 128 * pair
            q2 = packed[:, at : at + 128]
            k2 = packed[:, width + at : width + at + 128]
            v2 = packed[:, 2 * width + at : 2 * width + at + 128]
            halves = []
            for half in range(2):
                mine = low if half == 0 else ~low
                qm = jnp.where(mine, q2, jnp.zeros_like(q2)) * jnp.asarray(0.125, BF16)
                s = nt(qm, k2) + bias
                top = jnp.max(s, -1, keepdims=True)
                e = jnp.exp(s - top)
                total = jnp.sum(e, -1, keepdims=True)
                halves.append(nn(e.astype(BF16), v2) * (1.0 / total))
                lse = jnp.where(lane == 2 * pair + half, top + jnp.log(total), lse)
            pieces.append(jnp.where(low, halves[0], halves[1]).astype(BF16))
        mixed = jnp.concatenate(pieces, -1)
        hidden = x + nt(mixed, wout[...])
        scaled2, _ = standardize(hidden)
        put(normed_o, start, keep, (scaled2 * gain2 + shift2).astype(BF16))
        put(hidden_o, start, keep, hidden)
        put(packed_o, start, keep, packed)
        put(mixed_o, start, keep, mixed)
        put(lse_o, start, keep, lse)
        return carry

    images = rows // SEQ
    if not custom:
        lax.fori_loop(0, images, image, 0)
        return
    early.hop(2)
    late.hop(2)

    def step(i, carry):
        image(i, carry)

        @pl.when(i == 4)
        def _():
            early.hop(3)
            late.hop(3)

        return carry

    lax.fori_loop(0, images, step, 0)
    across = remote(normed_o, normed_s, core_sem.at[0], core_sem.at[1], sibling)
    across.start()
    early.last()
    late.last()
    across.wait()


def attention_backward(custom, tok, cot, hidden_r, packed_r, mixed_r, lse_r, own, given, wqkv, wout, par, *refs):
    rows, width = tok.shape
    other = given
    if custom:
        (
            ek0, ek1, er0, er1, lk0, lk1, ls0, ls1,
            out_o, gtok_o, early_o, late_o, small_o, xs, cs, outs, gtoks, gqkv_o, gout_o, gpar_o, pile, theirs, others,
            *room,
        ) = refs
        core = lax.axis_index("core")
        sibling = {"core": 1 - core}
        (e_own, e1, e2, e3, l_own, l1, l2, l3, s1, s2, s3,
         e_send, e_r1, e_r2, e_r3, e_sem, l_send, l_r1, l_r2, l_r3, l_sem, s_send, s_r1, s_r2, s_r3, core_sem) = room
        ek, er, lk, ls = (ek0, ek1), (er0, er1), (lk0, lk1), (ls0, ls1)
        early = Reduce(
            lambda half, z, q: ek[half].at[2 * z + q], None, lambda half, z, q: er[half].at[2 * z + q],
            e1, e2, e3, early_o, e_send, e_r1, e_r2, e_r3, e_own, e_sem,
        )
        late = Reduce(
            lambda half, z, q: lk[half].at[2 * z + q], lambda half, z, q: ls[half].at[2 * z + q], None,
            l1, l2, l3, late_o, l_send, l_r1, l_r2, l_r3, l_own, l_sem,
        )
        def pile_at(half, z, x, y):
            return pile.at[core, late.slot(z, x, y), half]

        little = Reduce(
            lambda half, z, q: pile_at(half, z, q, late.y) if half == 0 else pile_at(half, z, late.x, q),
            lambda half, z, q: pile_at(half, z, q, 1 - late.y) if half == 0 else pile_at(half, z, 1 - late.x, q),
            None, s1, s2, s3, small_o, s_send, s_r1, s_r2, s_r3,
        )
        late.greet(((None, sibling),))
        ranks = range(late.length)
        middle = others.shape[0] // 2

        def rows_across(i):
            part = pl.ds(i * middle, middle)
            return remote(given.at[part], others.at[part], core_sem.at[0, i], core_sem.at[1, i], sibling)

        for i in range(2):
            rows_across(i).start()
        late.one(0)
        for k in ranks:
            early.stage(k)
            late.stage(k)
        early.two(0)
        late.one(1)
        early.two(1)
        other = others
        rows_across(0).wait()
    else:
        out_o, gtok_o, gqkv_o, gout_o, gpar_o, xs, cs, outs, gtoks = refs
    fill(xs, tok, rows)
    fill(cs, cot, rows)
    gqkv_o[...] = jnp.zeros_like(gqkv_o)
    gout_o[...] = jnp.zeros_like(gout_o)
    gpar_o[...] = jnp.zeros_like(gpar_o)
    lane = lax.broadcasted_iota(jnp.int32, (1, 128), 1)
    low = lane < HEAD_DIM
    gain1, shift1, gain2 = (par[k : k + 1, :] for k in range(3))
    eighth = jnp.asarray(0.125, BF16)

    def image(i, carry):
        start, offset = window(i)
        valid, bias, keep = masks(offset)
        here = pl.ds(start, WIN)
        hidden = hidden_r[here, :]
        put(
            outs, start, keep,
            (hidden + own[here, 0:width].astype(F32) + other[here, 0:width].astype(F32)).astype(BF16),
        )
        scaled2, inverse2 = standardize(hidden)
        g2 = own[here, width:].astype(F32) + other[here, width:].astype(F32)
        g2 = jnp.where(valid, g2, 0.0)
        gpar_o[2:3, :] += jnp.sum(g2 * scaled2, 0, keepdims=True)
        gpar_o[3:4, :] += jnp.sum(g2, 0, keepdims=True)
        ghid = cs[here, :].astype(F32) + norm_back(g2 * gain2, scaled2, inverse2)
        branch = jnp.where(valid, ghid, 0.0).astype(BF16)
        gout_o[...] += tn(branch, mixed_r[here, :])
        gmix = nn(branch, wout[...]).astype(BF16)
        gq, gk, gv = [], [], []
        for pair in range(width // 128):
            at = 128 * pair
            q2 = packed_r[here, at : at + 128]
            k2 = packed_r[here, width + at : width + at + 128]
            v2 = packed_r[here, 2 * width + at : 2 * width + at + 128]
            gm2 = gmix[:, at : at + 128]
            sums = [0.0, 0.0, 0.0]
            for half in range(2):
                mine = low if half == 0 else ~low
                qm = jnp.where(mine, q2, jnp.zeros_like(q2)) * eighth
                km = jnp.where(mine, k2, jnp.zeros_like(k2)) * eighth
                gm = jnp.where(mine, gm2, jnp.zeros_like(gm2))
                head = 2 * pair + half
                lse = jnp.where(valid, lse_r[here, head : head + 1], -NEG)
                p = jnp.exp(nt(qm, k2) + bias - lse)
                gp = nt(gm, v2)
                inner = jnp.sum(gp * p, -1, keepdims=True)
                gs = (p * (gp - inner)).astype(BF16)
                sums[0] += nn(gs, km)
                sums[1] += tn(gs, qm)
                sums[2] += tn(p.astype(BF16), gm)
            for store, total in zip((gq, gk, gv), sums):
                store.append(total.astype(BF16))
        gpacked = jnp.concatenate(gq + gk + gv, -1)
        scaled1, inverse1 = standardize(xs[here, :].astype(F32))
        normed1 = (scaled1 * gain1 + shift1).astype(BF16)
        gqkv_o[...] += tn(normed1, gpacked)
        g1 = nt(gpacked, wqkv[...])
        gpar_o[0:1, :] += jnp.sum(g1 * scaled1, 0, keepdims=True)
        gpar_o[1:2, :] += jnp.sum(g1, 0, keepdims=True)
        put(gtoks, start, keep, ghid + norm_back(g1 * gain1, scaled1, inverse1))
        return carry

    images = rows // SEQ

    def finish():
        out_o[...] = outs[0:rows, :]
        gtok_o[...] = gtoks[0:rows, :]

    if not custom:
        lax.fori_loop(0, images, image, 0)
        finish()
        return

    def step(i, carry):
        image(i, carry)

        @pl.when(i == 2)
        def _():
            rows_across(1).wait()
            late.two(0)
            late.one(2)
            early.two(2)
            early.three(0)

        @pl.when(i == 5)
        def _():
            late.two(1)
            late.one(3)
            early.two(3)
            early.three(1)
            late.three(0)

        @pl.when(i == 7)
        def _():
            late.two(2)
            early.three(2)

        return carry

    lax.fori_loop(0, images, step, 0)
    span = late.span
    part, wide = width // (2 * late.chips), width // span
    vectors = gpar_o[...].T
    for t in range(span):
        table = jnp.concatenate(
            [gqkv_o[:, width * k + wide * t : width * k + wide * (t + 1)] for k in range(3)]
            + [gout_o[:, wide * t : wide * (t + 1)], vectors, jnp.zeros_like(vectors)],
            -1,
        )
        for group in range(2 * late.chips):
            for half in range(2):
                pile[group % 2, (group // 2) * span + t, half] = table[
                    part * group : part * (group + 1), 512 * half : 512 * (half + 1)
                ]

    def across():
        return remote(pile.at[1 - core], theirs, core_sem.at[0, 2], core_sem.at[1, 2], sibling)

    across().start()
    late.two(3)
    late.three(1)
    early.three(3)
    finish()
    across().wait()

    def merge(i, carry):
        accumulate(pile.at[core, i, 0], theirs.at[i, 0])
        accumulate(pile.at[core, i, 1], theirs.at[i, 1])
        return carry

    lax.fori_loop(0, theirs.shape[0], merge, 0)
    for k in ranks:
        little.one(k)
    late.three(2)
    for k in ranks:
        little.two(k)
    late.three(3)
    for k in ranks:
        little.three(k)
    early.drain()
    late.drain()
    little.drain()


def gelu_parts(v):
    e = jnp.exp(v * v * -0.5)
    t = 1.0 / (1.0 + jnp.abs(v) * (0.3275911 * 0.7071067811865476))
    q = 0.5 * 1.061405429
    for c in (-1.453152027, 1.421413741, -0.284496736, 0.254829592):
        q = q * t + 0.5 * c
    q = q * t * e
    return jnp.where(v < 0, q, 1.0 - q), e * INV_ROOT_TAU


def experts(row, prior, cnt, rown, rsib, cown, csib, town, tsib, *refs):
    if prior:
        pown_i, psib_i, *refs = refs
    else:
        pown_i = psib_i = None
    (
        own0, oth0, own1, oth1, pown, psib, k0, n0, k1, n1,
        xb, gb, tmpx, tmpg, acc1, acc2, wa, wb, fw, bk, off, dst, base, tot,
    ) = refs
    number = pl.num_programs(0)
    e_now = pl.program_id(0)
    depth = town.shape[2]
    width = rown.shape[1]

    def blocks(fn):
        for side, args in enumerate(((town, rown, cown, pown, pown_i), (tsib, rsib, csib, psib, psib_i))):
            def body(j, carry, side=side, args=args):
                fn(side * BLOCKS + j, args[0][j], *args[1:], pl.ds(pl.multiple_of(j * depth, ALIGN), depth))
                return carry

            lax.fori_loop(0, BLOCKS, body, 0)

    def onehot(table, at):
        slot = (lax.broadcasted_iota(jnp.int32, (STEP, 1), 0) + at).astype(F32)
        first = table[row : row + 1, :] == slot
        second = table[row + 1 : row + 2, :] == slot
        gate = jnp.where(first, table[2:3, :], jnp.where(second, table[3:4, :], 0.0))
        pick = jnp.where(first | second, 1.0, 0.0).astype(BF16)
        return pick, jnp.sum(gate, -1, keepdims=True)

    def padded(k):
        return (cnt[k] + (ALIGN - 1)) // ALIGN * ALIGN

    def steps(b):
        last = b * number + number - 1
        return (off[last] + padded(last) + (STEP - 1)) // STEP

    def segments(b, move):
        def per(e, carry):
            k = b * number + e
            o, d = off[k], dst[k]

            def tile(t, carry):
                move(
                    pl.ds(pl.multiple_of(o + t * ALIGN, ALIGN), ALIGN),
                    pl.ds(pl.multiple_of(d + t * ALIGN, ALIGN), ALIGN),
                )
                return carry

            return lax.fori_loop(0, padded(k) // ALIGN, tile, carry)

        lax.fori_loop(0, number, per, 0)

    @pl.when(e_now == 0)
    def _():
        def plan_expert(e, at):
            base[e] = at

            def plan_block(b, run):
                dst[b * number + e] = at + run
                return run + padded(b * number + e)

            total = lax.fori_loop(0, 2 * BLOCKS, plan_block, 0)
            tot[e] = total
            return at + (total + (CHUNK - 1)) // CHUNK * CHUNK

        lax.fori_loop(0, number, plan_expert, 0)

        def plan_off(b, carry):
            def one(e, run):
                off[b * number + e] = run
                return run + padded(b * number + e)

            lax.fori_loop(0, number, one, 0)
            return carry

        lax.fori_loop(0, 2 * BLOCKS, plan_off, 0)

        def dispatch(b, table, r, c, out, before, here):
            def some(k, carry):
                at = pl.multiple_of(k * STEP, ALIGN)
                pick, gate = onehot(table, at)
                tmpx[pl.ds(at, STEP), :] = nn(pick, r[here, :]).astype(BF16)
                tmpg[pl.ds(at, STEP), :] = (nn(pick, c[here, :]) * gate).astype(BF16)
                return carry

            lax.fori_loop(0, steps(b), some, 0)

            def move(local, far):
                xb[far, :] = tmpx[local, :]
                gb[far, :] = tmpg[local, :]

            segments(b, move)

        blocks(dispatch)

        def clear(e, carry):
            total = tot[e]
            end = base[e] + total

            def tile(t, carry):
                far = pl.ds(pl.multiple_of(end + t * ALIGN, ALIGN), ALIGN)
                xb[far, :] = jnp.zeros((ALIGN, width), BF16)
                gb[far, :] = jnp.zeros((ALIGN, width), BF16)
                return carry

            rest = (total + (CHUNK - 1)) // CHUNK * CHUNK - total
            return lax.fori_loop(0, rest // ALIGN, tile, carry)

        lax.fori_loop(0, number, clear, 0)

    shards, units = own0.shape[0], own0.shape[2] // 2
    middle = shards * units
    lower = e_now < number // 2

    def load(own, other):
        for i, ref in enumerate((own, other)):
            to = slice(i * middle, (i + 1) * middle)
            wa[to, :] = ref[:, 0, 0:units].reshape(middle, width)
            wb[to, :] = ref[:, 0, units:].reshape(middle, width)

    pl.when(lower)(lambda: load(own0, oth0))
    pl.when(~lower)(lambda: load(own1, oth1))
    acc1[...] = jnp.zeros_like(acc1)
    acc2[...] = jnp.zeros_like(acc2)

    def chunk(t, carry):
        here = pl.ds(pl.multiple_of(base[e_now] + t * CHUNK, ALIGN), CHUNK)
        first, second = wa[...], wb[...]
        x, g = xb[here, :], gb[here, :]
        v = nt(x, first)
        big, small = gelu_parts(v)
        act = (v * big).astype(BF16)
        gpre = (nt(g, second) * (big + v * small)).astype(BF16)
        acc1[...] += tn(gpre, x)
        acc2[...] += tn(act, g)
        xb[here, :] = nn(act, second).astype(BF16)
        gb[here, :] = nn(gpre, first).astype(BF16)
        return carry

    lax.fori_loop(0, (tot[e_now] + (CHUNK - 1)) // CHUNK, chunk, 0)

    def save(kept, sent):
        for i, ref in enumerate((kept, sent)):
            part = slice(i * middle, (i + 1) * middle)
            ref[:, 0, 0:units] = acc1[part, :].reshape(shards, units, width).astype(BF16)
            ref[:, 0, units:] = acc2[part, :].reshape(shards, units, width).astype(BF16)

    pl.when(lower)(lambda: save(k0, n0))
    pl.when(~lower)(lambda: save(k1, n1))

    @pl.when(e_now == number - 1)
    def _():
        def combine(b, table, r, c, out, before, here):
            def move(local, far):
                tmpx[local, :] = xb[far, :]
                tmpg[local, :] = gb[far, :]

            segments(b, move)
            if before is None:
                fw[...] = jnp.zeros_like(fw)
                bk[...] = jnp.zeros_like(bk)
            else:
                fw[...] = before[here, 0:width].astype(F32)
                bk[...] = before[here, width:].astype(F32)

            def some(k, carry):
                at = pl.multiple_of(k * STEP, ALIGN)
                pick, gate = onehot(table, at)
                fw[...] += tn(pick, (tmpx[pl.ds(at, STEP), :].astype(F32) * gate).astype(BF16))
                bk[...] += tn(pick, tmpg[pl.ds(at, STEP), :])
                return carry

            lax.fori_loop(0, steps(b), some, 0)
            out[here, 0:width] = fw[...].astype(BF16)
            out[here, width:] = bk[...].astype(BF16)

        blocks(combine)


def run_experts(late, tables, counts, row_refs, weights, prior):
    padded, width = row_refs[0].shape
    number, n_blocks = 2 * weights[0].shape[1], 2 * BLOCKS
    depth = padded // BLOCKS
    pairs = 4 * padded
    room = -(-(pairs + n_blocks * number * (ALIGN - 1) + number * (CHUNK - ALIGN)) // CHUNK) * CHUNK
    slots = -(-(2 * depth + number * (ALIGN - 1)) // STEP) * STEP
    shards, _, lines, _ = weights[0].shape
    held = shards * lines

    def full(*shape):
        return pl.BlockSpec(shape, lambda e, *_: (0,) * len(shape), pipeline_mode=pl.Buffered(1))

    block = (shards, 1, lines, width)
    lower = pl.BlockSpec(block, lambda e, *_: (0, jnp.minimum(e, number // 2 - 1), 0, 0))
    upper = pl.BlockSpec(block, lambda e, *_: (0, jnp.maximum(e - number // 2, 0), 0, 0))
    sums = full(padded, 2 * width)
    grad = whole(weights[0].shape, BF16)
    return pl.pallas_call(
        functools.partial(experts, 5 if late else 0, prior is not None),
        out_shape=(whole((padded, 2 * width), BF16),) * 2 + (grad,) * 4,
        grid_spec=pltpu.PrefetchScalarGridSpec(
            num_scalar_prefetch=1,
            grid=(number,),
            in_specs=[full(padded, width)] * 4
            + [full(*tables[0].shape)] * 2
            + [sums] * (0 if prior is None else 2)
            + [lower, lower, upper, upper],
            out_specs=(sums, sums, lower, lower, upper, upper),
            scratch_shapes=[
                pltpu.VMEM((room, width), BF16),
                pltpu.VMEM((room, width), BF16),
                pltpu.VMEM((slots, width), BF16),
                pltpu.VMEM((slots, width), BF16),
                pltpu.VMEM((held, width), F32),
                pltpu.VMEM((held, width), F32),
                pltpu.VMEM((held, width), BF16),
                pltpu.VMEM((held, width), BF16),
                pltpu.VMEM((depth, width), F32),
                pltpu.VMEM((depth, width), F32),
                pltpu.SMEM((n_blocks * number,), jnp.int32),
                pltpu.SMEM((n_blocks * number,), jnp.int32),
                pltpu.SMEM((number,), jnp.int32),
                pltpu.SMEM((number,), jnp.int32),
            ],
        ),
        compiler_params=pltpu.CompilerParams(
            vmem_limit_bytes=VMEM_LIMIT, dimension_semantics=("arbitrary",)
        ),
        cost_estimate=pl.CostEstimate(flops=25 * 10**9, bytes_accessed=20 * 10**6, transcendentals=6 * 10**6),
        name="experts_late" if late else "experts_early",
    )(counts, *row_refs, *tables, *(() if prior is None else prior), *weights)


def route(ids, gates, number, padded):
    rows = ids.shape[1]
    depth = padded // BLOCKS
    ids = jnp.pad(ids, ((0, 0), (0, padded - rows)), constant_values=-1)
    gates = jnp.pad(gates, ((0, 0), (0, padded - rows)))
    ids = ids.reshape(2, BLOCKS, 1, depth)
    gates = gates.reshape(2, BLOCKS, 1, depth)
    listed = jnp.arange(number, dtype=jnp.int32)
    match = ids == listed[None, None, :, None]
    named = (match[0] | match[1]).astype(BF16)
    order = jnp.arange(depth)
    earlier = (order[:, None] < order[None, :]).astype(BF16)
    rank = jnp.einsum("ber,rs->bes", named, earlier, preferred_element_type=F32)
    count = jnp.sum(named.astype(F32), -1)
    room = jnp.ceil(count * (1.0 / ALIGN)) * ALIGN
    middle = number // 2
    ahead = (listed[:, None] < listed[None, :]) & (listed[:, None] // middle == listed[None, :] // middle)
    off = jnp.sum(jnp.where(ahead[None], room[:, :, None], 0.0), 1)
    place = off[:, :, None] + rank
    slot = jnp.sum(jnp.where(match, place[None], 0.0), 2)
    flat = ids[:, :, 0]
    first = jnp.where((flat >= 0) & (flat < middle), slot, -1.0)
    second = jnp.where(flat >= middle, slot, -1.0)
    lanes = jnp.pad(count, ((0, 0), (0, depth - number)))
    return jnp.stack(
        [first[0], first[1], gates[0, :, 0], gates[1, :, 0], lanes, second[0], second[1], jnp.zeros_like(lanes)], 1
    )


def whole(shape, dtype):
    return jax.ShapeDtypeStruct(shape, dtype)


IN_VMEM = pl.BlockSpec(memory_space=pltpu.VMEM)
ANYWHERE = pl.BlockSpec(memory_space=pl.ANY)


def on_device(
    tokens, query_key_value, attention_out, first_gain, first_shift, second_gain, second_shift,
    expert_in, expert_out, expert_ids, gate_weights, cotangent,
):
    rows, width = tokens.shape
    padded = -(-rows // (ALIGN * BLOCKS)) * (ALIGN * BLOCKS)
    number = expert_in.shape[0]
    groups, span = lax.axis_size(DP), lax.axis_size("tensor")
    part = width // groups
    wide = width // span
    side = lax.axis_index("tensor")
    chips = groups // 2
    length = chips // 2
    custom = chips == 8 and span == 2 and part % 8 == 0
    vectors = jnp.stack([first_gain, first_shift, second_gain, second_shift], 1)
    small = jnp.concatenate(
        [
            query_key_value.reshape(part, 3 * wide),
            attention_out.T,
            jnp.pad(vectors, ((0, 0), (0, 1024 - 4 * wide - 4))),
        ],
        1,
    )
    shard = jnp.concatenate([expert_in.transpose(0, 2, 1), expert_out], 1)
    units = shard.shape[1] // 2
    if custom:
        lines = -(-part // ALIGN) * ALIGN
        small = jnp.pad(small, ((0, lines - part), (0, 0))).reshape(lines, 2, 512).transpose(1, 0, 2)
    else:
        gathered = lax.all_gather(small, ALL, axis=0, tiled=False).reshape(groups, span, part, 1024)
        taken = gathered[..., : 4 * wide].reshape(groups, span, part, 4, wide)
        taken = taken.transpose(0, 2, 3, 1, 4).reshape(width, 4, width)
        wqkv, wout = taken[:, :3].reshape(width, 3 * width), taken[:, 3]
        par = gathered[:, 0, :, 4 * wide : 4 * wide + 8].reshape(width, 8).T.astype(F32)

    ids = lax.dynamic_slice_in_dim(expert_ids.T, side * rows, rows, 1)
    gates = lax.dynamic_slice_in_dim(gate_weights.T, side * rows, rows, 1)
    table = route(ids, gates, number, padded)
    table_sib = lax.ppermute(table, "core", SWAP)
    cot_own = jnp.pad(cotangent, ((0, padded - rows), (0, 0)))
    cot_sib = lax.ppermute(cot_own, "core", SWAP)

    row_shapes = (
        whole((padded, width), BF16),
        whole((padded, width), F32),
        whole((padded, 3 * width), BF16),
        whole((padded, width), BF16),
        whole((padded, 128), F32),
    )
    estimate = pl.CostEstimate(flops=6 * 10**9, bytes_accessed=14 * 10**6, transcendentals=3 * 10**6)
    xs_scratch = [pltpu.VMEM((padded, width), BF16)]
    quarter = number // 4
    if custom:
        held = whole((2 * length, quarter, 2 * units, width), BF16)
        wqkv, wout, par, normed, hidden, packed, mixed, lse, normed_sib, e0, e1, f0, f1, l0, l1 = pl.pallas_call(
            functools.partial(attention_forward, True),
            out_shape=(whole((width, 3 * width), BF16), whole((width, width), BF16), whole((8, width), F32))
            + row_shapes
            + (row_shapes[0],)
            + (held,) * 6,
            in_specs=[IN_VMEM] * 3,
            out_specs=(IN_VMEM,) * 9 + (ANYWHERE,) * 6,
            scratch_shapes=[pltpu.VMEM((2, 2 * length, lines, 512), BF16)] * 4
            + [pltpu.VMEM((2, span, width, 512), F32)]
            + spread_sems(length, 2)
            + [pltpu.SemaphoreType.DMA((2, 2))]
            + xs_scratch
            + spread_sems(length, 2)
            + spread_sems(length, 1)
            + [pltpu.SemaphoreType.DMA((2,))],
            compiler_params=pltpu.CompilerParams(vmem_limit_bytes=VMEM_LIMIT, collective_id=1, has_side_effects=True),
            cost_estimate=estimate,
            name="attention_forward",
        )(tokens, small, shard.reshape(4, quarter, 2 * units, width))
        across_y = functools.partial(lax.ppermute, axis_name="tensor", perm=SWAP)
        across_x = functools.partial(lax.ppermute, axis_name="chip", perm=[(c, c ^ 1) for c in range(chips)])
        early_weights = (e0, f0, e1, f1)
        late_weights = (l0, across_y(l0), l1, across_x(l1))
    else:
        normed, hidden, packed, mixed, lse = pl.pallas_call(
            functools.partial(attention_forward, False),
            out_shape=row_shapes,
            in_specs=[IN_VMEM] * 4,
            out_specs=(IN_VMEM,) * 5,
            scratch_shapes=xs_scratch,
            compiler_params=pltpu.CompilerParams(vmem_limit_bytes=VMEM_LIMIT),
            cost_estimate=estimate,
            name="attention_forward",
        )(tokens, wqkv, wout, par)
        normed_sib = lax.ppermute(normed, "core", SWAP)
        weights = lax.all_gather(shard, RING, axis=0, tiled=False)
        shards = weights.shape[0]
        weights = weights.reshape(2, shards // 2, 4, quarter, 2, units, width).transpose(2, 0, 3, 4, 1, 5, 6)
        weights = weights.reshape(4, 2, 1, quarter, shards * units, width)
        early_weights = tuple(weights[i, j] for i in (0, 1) for j in (0, 1))
        late_weights = tuple(weights[i, j] for i in (2, 3) for j in (0, 1))

    middle = number // 2
    both_counts = jnp.concatenate([table[:, 4, :number], table_sib[:, 4, :number]], 0).astype(jnp.int32)
    row_refs = (normed, normed_sib, cot_own, cot_sib)
    tables = (table, table_sib)
    own1, sib1, *early = run_experts(
        False, tables, both_counts[:, :middle].reshape(-1), row_refs, early_weights, None
    )
    if custom:
        got = (across_y(early[1]), across_x(early[3]))
    part_own, part_sib, *late = run_experts(
        True, tables, both_counts[:, middle:].reshape(-1), row_refs, late_weights, (own1, sib1)
    )

    sums = [
        pltpu.VMEM((width, 3 * width), F32),
        pltpu.VMEM((width, width), F32),
        pltpu.VMEM((128, width), F32),
    ]
    rows_scratch = [
        pltpu.VMEM((padded, width), BF16),
        pltpu.VMEM((padded, width), BF16),
        pltpu.VMEM((padded, width), BF16),
        pltpu.VMEM((padded, width), F32),
    ]
    saved = (tokens, cotangent, hidden, packed, mixed, lse, part_own)
    shapes = (whole((rows, width), BF16), whole((rows, width), F32))
    estimate = pl.CostEstimate(flops=15 * 10**9, bytes_accessed=25 * 10**6, transcendentals=3 * 10**6)
    if custom:
        block, tile = (quarter, 2 * units, width), (part, 512)
        output, grad_tokens, early_grad, late_grad, mine = pl.pallas_call(
            functools.partial(attention_backward, True),
            out_shape=shapes + (whole((2,) + block, F32),) * 2 + (whole((2,) + tile, F32),),
            in_specs=[IN_VMEM] * 7 + [ANYWHERE] + [IN_VMEM] * 3 + [ANYWHERE] * 8,
            out_specs=(IN_VMEM,) * 5,
            scratch_shapes=rows_scratch
            + sums
            + [pltpu.VMEM((2, 2 * chips, 2) + tile, F32), pltpu.VMEM((2 * chips, 2) + tile, F32)]
            + [pltpu.VMEM((padded, 2 * width), BF16)]
            + ([pltpu.VMEM((2, 2 * length) + block, BF16)] + reduce_room(length, block, BF16)) * 2
            + reduce_room(length, tile, F32)
            + (reduce_sems(length) + [pltpu.SemaphoreType.DMA((2, 2 * length))]) * 2
            + reduce_sems(length)
            + [pltpu.SemaphoreType.DMA((2, 3))],
            compiler_params=pltpu.CompilerParams(
                vmem_limit_bytes=VMEM_LIMIT, collective_id=2, has_side_effects=True
            ),
            cost_estimate=estimate,
            name="attention_backward",
        )(*saved, part_sib, wqkv, wout, par, early[0], early[2], *got, late[0], late[2], late[1], late[3])
        mine = mine.transpose(1, 0, 2).reshape(part, 1024)
        grad_shard = jnp.concatenate([early_grad, late_grad], 0).reshape(number, 2 * units, width)
    else:
        part_other = lax.ppermute(part_sib, "core", SWAP)
        output, grad_tokens, gqkv, gout, gpar = pl.pallas_call(
            functools.partial(attention_backward, False),
            out_shape=shapes + tuple(whole(ref.shape, F32) for ref in sums),
            in_specs=[IN_VMEM] * 11,
            out_specs=(IN_VMEM,) * 5,
            scratch_shapes=rows_scratch,
            compiler_params=pltpu.CompilerParams(vmem_limit_bytes=VMEM_LIMIT),
            cost_estimate=estimate,
            name="attention_backward",
        )(*saved, part_other, wqkv, wout, par)
        grads = jnp.stack(early + late).reshape(4, 2, quarter, 2, shards // 2, units, width)
        grads = grads.transpose(1, 4, 0, 2, 3, 5, 6).reshape(shards, number, 2 * units, width)
        grad_shard = lax.psum_scatter(grads, RING, scatter_dimension=0, tiled=False).astype(F32)
        owed = jnp.concatenate([gqkv.reshape(width, 3, width), gout[:, None]], 1)
        owed = owed.reshape(groups, part, 4, span, wide).transpose(0, 3, 1, 2, 4)
        owed = owed.reshape(groups, span, part, 4 * wide)
        own_vectors = jnp.broadcast_to(gpar[:8].T.reshape(groups, 1, part, 8), (groups, span, part, 8))
        owed = jnp.concatenate([owed, own_vectors], -1).reshape(groups * span, part, 4 * wide + 8)
        mine = lax.psum_scatter(owed, ALL, scatter_dimension=0, tiled=False)
    vectors = mine[:, 4 * wide : 4 * wide + 4]
    return (
        output,
        grad_tokens,
        mine[:, : 3 * wide].reshape(part, 3, wide),
        mine[:, 3 * wide : 4 * wide].T,
        vectors[:, 0],
        vectors[:, 1],
        vectors[:, 2],
        vectors[:, 3],
        grad_shard[:, :units].transpose(0, 2, 1),
        grad_shard[:, units:],
    )


def solution(mesh):
    groups, span = mesh.devices.shape
    split = Mesh(mesh.devices.reshape(groups // 2, 2, span), ALL)
    return jax.shard_map(
        on_device,
        mesh=split,
        in_specs=(
            P(ALL, None),
            P(DP, None, "tensor"),
            P("tensor", DP),
            P(DP),
            P(DP),
            P(DP),
            P(DP),
            P(None, None, ALL),
            P(None, ALL, None),
            P(DP, None),
            P(DP, None),
            P(ALL, None),
        ),
        out_specs=(
            P(ALL, None),
            P(ALL, None),
            P(DP, None, "tensor"),
            P("tensor", DP),
            P(DP),
            P(DP),
            P(DP),
            P(DP),
            P(None, None, ALL),
            P(None, ALL, None),
        ),
        check_vma=False,
    )
```
